512 devices in a mesh: seq: 64 (over z, x), head: 8 (over y, core).
Axes of the slice: x: 4, y: 4, z: 16, core: 2. Of those that a mesh axis runs over, the one named last changes fastest.
Arguments:
- x_proj: bfloat16 [16384, 8192], P(('seq', 'head')), may hold values from -6 to 6
- z_proj: bfloat16 [16384, 8192], P(('seq', 'head')), may hold values from -6 to 6
- b_proj: bfloat16 [16384, 1024], P(('seq', 'head')), may hold values from -6 to 6
- c_proj: bfloat16 [16384, 1024], P(('seq', 'head')), may hold values from -6 to 6
- dt_raw: bfloat16 [16384, 128], P(('seq', 'head')), may hold values from -3.2 to 3.2, as said below
- dt_bias: float32 [128], P('head'), may hold values from -6.3 to -1.2, as said below
- a_log: float32 [128], P('head'), as said below
- d_skip: float32 [128], P('head'), may hold values from 0.5 to 2
- conv_x: float32 [4, 8192], P(None, 'head'), may hold values from -3 to 3
- conv_bias_x: float32 [8192], P('head'), may hold values from -3 to 3
- conv_bc: float32 [4, 2, 1024], P(None, None, 'head'), may hold values from -3 to 3
- conv_bias_bc: float32 [2, 1024], P(None, 'head'), may hold values from -3 to 3
- norm_weight: float32 [8192], P('head'), may hold values from 0.25 to 1.75
- out_weight: bfloat16 [8192, 4096], P('head', 'seq'), may hold values from -0.0625 to 0.0625
Outputs:
- mixed: bfloat16 [16384, 4096], P(('seq', 'head'))
The draws below stay inside these ranges and needn't reach their ends.
Inputs may be any that keep to these rules, and one draw needn't show every extreme that they name: `dt_raw`: A normal draw times 0.7 plus an offset common to each head and each aligned run of 256 tokens. `dt_bias`: the inverse softplus of a per-head step size between 0.002 and 0.25. Finite; exp(a_log) lies above 0.0 and at most 0.3.
All inputs are finite; a program needn't handle non-finite values.
Results may differ from the reference program's by a relative error of at most 0.014.
Values may be sent and summed in bfloat16 or wider, within the bound.
No kernel may reach another device: no remote copies, remote signals or barrier semaphores. Data moves between devices by JAX's collectives and lax.ppermute only.
A program may use at most 128 MiB of HBM per device.

```python
import jax
import jax.numpy as jnp
from jax import lax

D = 4096
HEADS = 128
HEAD_DIM = 64
STATE = 128
GROUPS = 8
CONV = 4
TOK_DEV = 256
SPAN = 128
DI = 8192
TOKENS = 16384
N_HEAD = 8


def head_kinds(key):
    order = jax.random.permutation(jax.random.fold_in(key, 101), HEADS)
    return order < HEADS // 2


def draw_dt_bias(key, part):
    slow_heads = head_kinds(key)
    uniform_draw = jax.random.uniform(jax.random.fold_in(key, 102), (HEADS,), jnp.float32)
    lower_log = jnp.where(slow_heads, jnp.log(0.002), jnp.log(0.08))
    upper_log = jnp.where(slow_heads, jnp.log(0.006), jnp.log(0.25))
    step_value = jnp.exp(lower_log + uniform_draw * (upper_log - lower_log))
    return jnp.log(jnp.expm1(step_value)).astype(jnp.float32)


def draw_a_log(key, part):
    slow_heads = head_kinds(key)
    uniform_draw = jax.random.uniform(jax.random.fold_in(key, 105), (HEADS,), jnp.float32)
    slow_log = jnp.log(0.1) + uniform_draw * (jnp.log(0.6) - jnp.log(0.1)) - jnp.log(0.004 * TOKENS)
    fast_log = jnp.log(0.15) + uniform_draw * (jnp.log(0.3) - jnp.log(0.15))
    return jnp.where(slow_heads, slow_log, fast_log).astype(jnp.float32)


def draw_dt_raw(key, part):
    noise_part = jax.random.truncated_normal(jax.random.fold_in(key, 103), -3.0, 3.0, (TOKENS, HEADS), jnp.float32) * 0.7
    offsets = jax.random.uniform(jax.random.fold_in(key, 104), (TOKENS // TOK_DEV, HEADS), jnp.float32, minval=-1.0, maxval=1.0)
    return (noise_part + jnp.repeat(offsets, TOK_DEV, axis=0)).astype(jnp.bfloat16)


def block_levels(own_key, shape, pieces, smallest, high):
    loudness = 1.0
    for axis_at, shards_of in pieces:
        steps = jax.random.uniform(jax.random.fold_in(jax.random.fold_in(own_key, 6), axis_at), (shards_of,), jnp.float32, smallest / len(pieces), high / len(pieces))
        loudness = loudness * jnp.repeat(jnp.exp(steps), shape[axis_at] // shards_of).reshape((-1,) + (1,) * (len(shape) - 1 - axis_at))
    return loudness


def normal_values(stream_key, extent, scale, most, split=(), held_as=jnp.bfloat16):
    gain = block_levels(stream_key, extent, split, -0.22, 0.18) if split else 1.0
    array = jax.random.normal(stream_key, extent, jnp.float32) * scale * gain
    return jnp.minimum(jnp.maximum(array, -most), most).astype(held_as)


def setup_inputs(seed: int = 0) -> dict:
    key_of = jax.random.split(jax.random.key(seed), 15)
    x_proj = normal_values(key_of[0], (TOKENS, DI), 1.0, 6.0, ((0, 512),))
    z_proj = normal_values(key_of[1], (TOKENS, DI), 1.0, 6.0, ((0, 512),))
    b_proj = normal_values(key_of[2], (TOKENS, GROUPS * STATE), 1.0, 6.0, ((0, 512),))
    c_proj = normal_values(key_of[3], (TOKENS, GROUPS * STATE), 1.0, 6.0, ((0, 512),))
    dt_raw = draw_dt_raw(jax.random.fold_in(key_of[14], 71), 0)
    dt_bias = draw_dt_bias(jax.random.fold_in(key_of[14], 71), 0)
    a_log = draw_a_log(jax.random.fold_in(key_of[14], 71), 0)
    d_skip = jnp.clip(0.5 + 1.5 * jax.random.uniform(key_of[7], (HEADS,), jnp.float32) ** block_levels(key_of[7], (HEADS,), ((0, 8),), -0.2, 0.2), 0.5, 2.0)
    conv_x = normal_values(key_of[8], (CONV, DI), CONV ** -0.5, 3.0, ((1, 8),), jnp.float32)
    conv_bias_x = normal_values(key_of[9], (DI,), 0.5, 3.0, ((0, 8),), jnp.float32)
    conv_bc = normal_values(key_of[10], (CONV, 2, GROUPS * STATE), CONV ** -0.5, 3.0, ((2, 8),), jnp.float32)
    conv_bias_bc = normal_values(key_of[11], (2, GROUPS * STATE), 0.5, 3.0, ((1, 8),), jnp.float32)
    norm_weight = jnp.clip(1.0 + 0.15 * jax.random.normal(key_of[12], (DI,), jnp.float32), 0.25, 1.75)
    out_weight = normal_values(key_of[13], (DI, D), DI ** -0.5, 0.0625, ((0, 8), (1, 64)))
    return {"x_proj": x_proj, "z_proj": z_proj, "b_proj": b_proj, "c_proj": c_proj, "dt_raw": dt_raw, "dt_bias": dt_bias, "a_log": a_log, "d_skip": d_skip, "conv_x": conv_x, "conv_bias_x": conv_bias_x, "conv_bc": conv_bc, "conv_bias_bc": conv_bias_bc, "norm_weight": norm_weight, "out_weight": out_weight}


def conv_silu(inputs, weight, bias_row):
    taps = weight.shape[0]
    padded = jnp.pad(inputs.astype(jnp.float32), ((taps - 1, 0), (0, 0)))
    length = inputs.shape[0]
    summed = jnp.broadcast_to(bias_row, inputs.shape).astype(jnp.float32)
    for offset in range(taps):
        summed = summed + weight[offset] * padded[offset:offset + length]
    return jax.nn.silu(summed).astype(jnp.bfloat16)

def to_bf16_f32(value):
    rounded = lax.optimization_barrier(value.astype(jnp.bfloat16))
    return rounded.astype(jnp.float32)

def reference(x_proj, z_proj, b_proj, c_proj, dt_raw, dt_bias, a_log, d_skip, conv_x, conv_bias_x, conv_bc, conv_bias_bc, norm_weight, out_weight):
    high = lax.Precision.HIGHEST
    x_conv = conv_silu(x_proj, conv_x, conv_bias_x)
    b_conv = conv_silu(b_proj, conv_bc[:, 0], conv_bias_bc[0])
    c_conv = conv_silu(c_proj, conv_bc[:, 1], conv_bias_bc[1])
    step_size = jax.nn.softplus(dt_raw.astype(jnp.float32) + dt_bias)
    coeff = -jnp.exp(a_log)
    blocks = TOKENS // SPAN
    per_group = HEADS // GROUPS
    x_blocks = x_conv.reshape(blocks, SPAN, HEADS, HEAD_DIM)
    b_blocks = b_conv.reshape(blocks, SPAN, GROUPS, STATE)
    c_blocks = c_conv.reshape(blocks, SPAN, GROUPS, STATE)
    step_blocks = step_size.reshape(blocks, SPAN, HEADS)
    causal = jnp.arange(SPAN)[:, None] >= jnp.arange(SPAN)[None, :]

    def span_step(state, inputs):
        x_span, b_span, c_span, step_span = inputs
        x_float = x_span.astype(jnp.float32)
        b_float = b_span.astype(jnp.float32)
        c_float = c_span.astype(jnp.float32)
        cumulative = jnp.cumsum(coeff * step_span, axis=0)
        scores = jnp.einsum('tgn,sgn->gts', c_float, b_float, precision=high)
        by_head = cumulative.T
        spread = by_head[:, :, None] - by_head[:, None, :]
        decays = jnp.exp(jnp.where(causal, spread, -jnp.inf))
        scaled = decays * step_span.T[:, None, :]
        mix_weights = (scaled.reshape(GROUPS, per_group, SPAN, SPAN) * scores[:, None]).reshape(HEADS, SPAN, SPAN)
        mix_weights = to_bf16_f32(mix_weights)
        y_local = jnp.einsum('hts,shp->thp', mix_weights, x_float, precision=high)
        state_scale = step_span * jnp.exp(cumulative[-1:] - cumulative)
        x_weighted = to_bf16_f32(x_float * state_scale[:, :, None])
        piece = jnp.einsum('sgqp,sgn->gqpn', x_weighted.reshape(SPAN, GROUPS, per_group, HEAD_DIM), b_float, precision=high)
        piece = piece.reshape(HEADS, HEAD_DIM, STATE)
        start_state = to_bf16_f32(state).reshape(GROUPS, per_group, HEAD_DIM, STATE)
        y_carry = jnp.einsum('tgn,gqpn->tgqp', c_float, start_state, precision=high).reshape(SPAN, HEADS, HEAD_DIM)
        y_carry = y_carry * jnp.exp(cumulative)[:, :, None]
        outputs = y_local + y_carry + d_skip[:, None] * x_float
        new_state = jnp.exp(cumulative[-1])[:, None, None] * state + piece
        return (new_state, outputs)
    initial = jnp.zeros((HEADS, HEAD_DIM, STATE), jnp.float32)
    final_state, outputs = lax.scan(span_step, initial, (x_blocks, b_blocks, c_blocks, step_blocks))
    outputs = outputs.reshape(TOKENS, DI)
    gated = outputs * jax.nn.silu(z_proj.astype(jnp.float32))
    grouped = gated.reshape(TOKENS, GROUPS, DI // GROUPS)
    normed = grouped / jnp.sqrt(lax.optimization_barrier(jnp.mean(grouped * grouped, axis=-1, keepdims=True)) + 1.0)
    normed = (normed.reshape(TOKENS, DI) * norm_weight).astype(jnp.bfloat16)
    block_rows = DI // N_HEAD
    summed = jnp.zeros((TOKENS, D), jnp.float32)
    for block_idx in range(N_HEAD):
        rows_lo = block_idx * block_rows
        partial_sum = jnp.dot(normed[:, rows_lo:rows_lo + block_rows], out_weight[rows_lo:rows_lo + block_rows], preferred_element_type=jnp.float32)
        summed = summed + to_bf16_f32(partial_sum)
    return summed.astype(jnp.bfloat16)
```

```python
import jax
import jax.numpy as jnp
from jax import lax
from jax.experimental import pallas as pl
from jax.experimental.pallas import tpu as pltpu
from jax.sharding import Mesh
from jax.sharding import PartitionSpec as P

HEAD_DIM = 64
STATE = 128
SPAN = 128
LANES = 128
F32 = jnp.float32
BF16 = jnp.bfloat16
SEQ = ("z", "x")
HEAD = ("y", "c")
PLANE = ("x", "y", "c")
ALL = ("z", "x", "y", "c")
VMEM = pl.BlockSpec(memory_space=pltpu.VMEM)


def call(kernel, outs, inputs, scratch=(), flops=1 << 22, limit=16):
    return pl.pallas_call(
        kernel,
        out_shape=outs,
        in_specs=[VMEM] * len(inputs),
        out_specs=jax.tree.map(lambda _: VMEM, outs),
        scratch_shapes=list(scratch),
        compiler_params=pltpu.CompilerParams(vmem_limit_bytes=limit << 20),
        cost_estimate=pl.CostEstimate(flops=flops, bytes_accessed=1 << 20, transcendentals=0),
    )(*inputs)


def shape(dims, dtype):
    return jax.ShapeDtypeStruct(dims, dtype)


def silu(v):
    return v * (1.0 / (1.0 + jnp.exp(-v)))


def nt(a, b):
    return lax.dot_general(a, b, (((1,), (1,)), ((), ())), preferred_element_type=F32)


def tn(a, b):
    return lax.dot_general(a, b, (((0,), (0,)), ((), ())), preferred_element_type=F32)


def by_head(values, chunk, first):
    return jnp.where(first, values[:, 2 * chunk : 2 * chunk + 1], values[:, 2 * chunk + 1 : 2 * chunk + 2])


def left_half():
    return lax.broadcasted_iota(jnp.int32, (1, LANES), 1) < HEAD_DIM


def top_half():
    return lax.broadcasted_iota(jnp.int32, (LANES, 1), 0) < HEAD_DIM


def spread_out(out_ref, wide_ref, group_ref):
    count, _, _ = out_ref.shape
    groups = group_ref.shape[1] // LANES
    cols = wide_ref.shape[1] // count
    for d in range(count):
        part, group = divmod(d, groups)
        lo = (group * (count // groups) + part) * cols
        out_ref[d, :, :cols] = wide_ref[:, lo : lo + cols]
        out_ref[d, :, cols : cols + LANES] = group_ref[:, group * LANES : (group + 1) * LANES]


def pack_first(x_ref, b_ref, dt_ref, out_ref):
    spread_out(out_ref, x_ref, b_ref)
    count, _, width = out_ref.shape
    groups = b_ref.shape[1] // LANES
    heads = dt_ref.shape[1] // count
    dt = dt_ref[...].astype(F32)
    for d in range(count):
        part, group = divmod(d, groups)
        lo = (group * (count // groups) + part) * heads
        mine = dt if lo == 0 else pltpu.roll(dt, LANES - lo, 1)
        out_ref[d, :, width - LANES :] = mine.astype(BF16)


def pack_second(z_ref, c_ref, out_ref):
    spread_out(out_ref, z_ref, c_ref)


def steps(packed_ref, heads_ref, dt_ref, cum_ref, sum_ref):
    tokens = dt_ref.shape[0]
    rows = lax.broadcasted_iota(jnp.int32, (SPAN, SPAN), 0)
    cols = lax.broadcasted_iota(jnp.int32, (SPAN, SPAN), 1)
    ones = (rows >= cols).astype(F32)
    total = jnp.zeros((1, LANES), F32)
    for k in range(tokens // SPAN):
        part = slice(k * SPAN, (k + 1) * SPAN)
        raw = packed_ref[part, packed_ref.shape[1] - LANES :].astype(F32) + heads_ref[0:1]
        dt = jnp.maximum(raw, 0.0) + jnp.log1p(jnp.exp(-jnp.abs(raw)))
        dt_ref[part] = dt
        cum = lax.dot(
            ones, heads_ref[1:2] * dt, precision=lax.Precision.HIGHEST, preferred_element_type=F32
        )
        cum_ref[part] = cum
        sum_ref[part] = cum + total
        total = total + cum[SPAN - 1 :]


def fill_padded(padded, halo_ref, packed_ref, width):
    padded[:8] = halo_ref[:, :width].astype(F32)
    padded[8:] = packed_ref[:, :width].astype(F32)


def conv(padded, taps, bias, k, lo):
    first = 8 + k * SPAN - 3
    total = bias + taps[0] * padded[first : first + SPAN, lo : lo + LANES]
    for j in range(1, 4):
        total = total + taps[j] * padded[first + j : first + j + SPAN, lo : lo + LANES]
    return silu(total).astype(BF16)


def scan_in(
    packed_ref, halo_ref, taps_ref, group_taps_ref, dt_ref, cum_ref, sum_ref,
    xs_ref, b_ref, held_ref, sent_ref, padded,
):
    tokens, cols = xs_ref.shape
    blocks = tokens // SPAN
    fill_padded(padded, halo_ref, packed_ref, cols + LANES)
    left, top = left_half(), top_half()
    group_taps = [group_taps_ref[j : j + 1] for j in range(4)]
    states = [jnp.zeros((LANES, STATE), F32) for _ in range(cols // LANES)]
    for k in range(blocks):
        part = slice(k * SPAN, (k + 1) * SPAN)
        b = conv(padded, group_taps, group_taps_ref[4:5], k, cols)
        b_ref[part] = b
        cum = cum_ref[part]
        last = cum[SPAN - 1 :]
        scale = dt_ref[part] * jnp.exp(last - cum)
        decay = jnp.exp(last)
        for chunk in range(cols // LANES):
            lo = chunk * LANES
            taps = [taps_ref[j : j + 1, lo : lo + LANES] for j in range(4)]
            xs = conv(padded, taps, taps_ref[4:5, lo : lo + LANES], k, lo)
            xs_ref[part, lo : lo + LANES] = xs
            weighted = (xs.astype(F32) * by_head(scale, chunk, left)).astype(BF16)
            held_ref[k, lo : lo + LANES] = states[chunk].astype(BF16)
            states[chunk] = by_head(decay, chunk, top) * states[chunk] + tn(weighted, b)
    count, extra = sent_ref.shape[0], sent_ref.shape[1]
    rows = cols // count
    for chunk in range(cols // LANES):
        final = states[chunk].astype(BF16)
        for i in range(LANES // rows):
            sent_ref[chunk * (LANES // rows) + i, :rows] = final[i * rows : (i + 1) * rows]
    total = sum_ref[tokens - 1 :]
    high = total.astype(BF16).astype(F32)
    middle = (total - high).astype(BF16).astype(F32)
    low = total - high - middle
    at = lax.broadcasted_iota(jnp.int32, (extra - rows, LANES), 0)
    tail = jnp.where(at == 0, high, jnp.where(at == 1, middle, jnp.where(at == 2, low, 0.0)))
    for d in range(count):
        sent_ref[d, rows:] = tail.astype(BF16)


def scan_all(inbox_ref, starts_ref, decays):
    count, rows, _ = starts_ref.shape
    tail = inbox_ref[:, rows:].astype(F32)
    logs = tail[:, 0] + tail[:, 1] + tail[:, 2]
    lanes = lax.broadcasted_iota(jnp.int32, logs.shape, 1)
    head = lax.axis_index("z") * rows // HEAD_DIM
    column = jnp.sum(jnp.where(lanes == head, logs, 0.0), axis=1, keepdims=True)
    decays[...] = jnp.broadcast_to(jnp.exp(column), decays.shape)
    state = jnp.zeros((rows, STATE), F32)
    for i in range(count):
        starts_ref[i] = state.astype(BF16)
        state = decays[i : i + 1] * state + inbox_ref[i, :rows].astype(F32)


def local(
    xs_ref, b_ref, packed_ref, halo_ref, group_taps_ref, dt_ref, cum_ref, held_ref, heads_ref,
    c_ref, y_ref, padded,
):
    tokens, cols = xs_ref.shape
    padded[:8] = halo_ref[...].astype(F32)
    padded[8:] = packed_ref[:, cols:].astype(F32)
    rows = lax.broadcasted_iota(jnp.int32, (SPAN, SPAN), 0)
    lanes = lax.broadcasted_iota(jnp.int32, (SPAN, SPAN), 1)
    causal = rows >= lanes
    left = left_half()
    taps = [group_taps_ref[8 + j : 9 + j] for j in range(4)]
    for k in range(tokens // SPAN):
        part = slice(k * SPAN, (k + 1) * SPAN)
        c = conv(padded, taps, group_taps_ref[12:13], k, 0)
        c_ref[part] = c
        scores = nt(c, b_ref[part])
        cum = cum_ref[part]
        grown = jnp.exp(cum)
        cum_t = cum.T
        dt_t = dt_ref[part].T

        def mix(h):
            spread = cum[:, h : h + 1] - cum_t[h : h + 1]
            decays = jnp.exp(jnp.where(causal, spread, -jnp.inf))
            return (decays * dt_t[h : h + 1] * scores).astype(BF16)

        for chunk in range(cols // LANES):
            lo = chunk * LANES
            xs = xs_ref[part, lo : lo + LANES]
            y0 = jnp.dot(mix(2 * chunk), xs, preferred_element_type=F32)
            y1 = jnp.dot(mix(2 * chunk + 1), xs, preferred_element_type=F32)
            y = jnp.where(left, y0, y1) + by_head(heads_ref[2:3], chunk, left) * xs.astype(F32)
            if k > 0:
                y = y + nt(c, held_ref[k, lo : lo + LANES]) * by_head(grown, chunk, left)
            y_ref[part, lo : lo + LANES] = y


def finish(start_ref, c_ref, sum_ref, y_ref, packed_ref, theirs_ref, ours_ref):
    tokens, cols = y_ref.shape
    rows = tokens // 32
    left = left_half()
    first = lax.axis_index("c") == 0
    for k in range(tokens // SPAN):
        part = slice(k * SPAN, (k + 1) * SPAN)
        grown = jnp.exp(sum_ref[part])
        for chunk in range(cols // LANES):
            lo = chunk * LANES
            carry = nt(c_ref[part], start_ref[lo : lo + LANES]) * by_head(grown, chunk, left)
            z = packed_ref[part, lo : lo + LANES].astype(F32)
            gated = ((y_ref[part, lo : lo + LANES] + carry) * silu(z)).astype(BF16)
            for i in range(SPAN // (2 * rows)):
                even = gated[2 * i * rows : (2 * i + 1) * rows]
                odd = gated[(2 * i + 1) * rows : (2 * i + 2) * rows]
                at = k * (SPAN // 2) + i * rows
                theirs_ref[at : at + rows, lo : lo + LANES] = jnp.where(first, odd, even)
                ours_ref[at : at + rows, lo : lo + LANES] = jnp.where(first, even, odd)


def multiply(parts, weights_ref, out_ref, other_ref):
    rows, cols = parts[0].shape
    width = weights_ref.shape[1]
    me = lax.axis_index("x")
    step = 128
    for lo in range(0, rows, step):
        squares = jnp.zeros((step, 1), F32)
        total = jnp.zeros((step, weights_ref.shape[0]), F32)
        middle = rows // 2
        for i, offset in enumerate((0, 3, 1, 2)):
            at = pl.multiple_of(lax.rem(me + offset, 4) * cols, cols)
            if i < 3:
                gated = parts[i][lo : lo + step]
            elif lo < middle:
                gated = parts[3][lo : lo + step]
            else:
                gated = parts[4][lo - middle : lo - middle + step]
            total = total + nt(gated, weights_ref[:, pl.ds(at, cols)])
            value = gated.astype(F32)
            squares = squares + jnp.sum(value * value, axis=1, keepdims=True)
        total = total * (1.0 / jnp.sqrt(squares / width + 1.0))
        if other_ref is not None:
            total = total + other_ref[lo : lo + step].astype(F32)
        out_ref[lo : lo + step] = total.astype(BF16)


def stack(*refs):
    out_ref = refs[-1]
    at = 0
    for ref in refs[:-1]:
        out_ref[at : at + ref.shape[0]] = ref[...]
        at += ref.shape[0]


def project(own_ref, before_ref, after_ref, low_ref, high_ref, weights_ref, out_ref):
    multiply((own_ref, before_ref, after_ref, low_ref, high_ref), weights_ref, out_ref, None)


def project_add(own_ref, before_ref, after_ref, low_ref, high_ref, weights_ref, other_ref, out_ref):
    multiply((own_ref, before_ref, after_ref, low_ref, high_ref), weights_ref, out_ref, other_ref)


def tail(array_ref, out_ref):
    rows, cols = array_ref.shape
    out_ref[...] = array_ref[rows - out_ref.shape[0] :, cols - out_ref.shape[1] :]


def collect(shares_ref, out_ref, *, ys):
    count, _, width = shares_ref.shape
    xs = count // ys
    zs = width // HEAD_DIM
    me = lax.axis_index("z")
    left = left_half()
    order = ring_order(zs)
    for pair in range(width // LANES):
        lo = pair * LANES
        sums = []
        for i in range(xs):
            total = shares_ref[i * ys, :, lo : lo + LANES].astype(F32)
            for j in range(1, ys):
                total = total + shares_ref[i * ys + j, :, lo : lo + LANES].astype(F32)
            sums.append(total)
        rolled = [pltpu.roll(total, HEAD_DIM, 1) for total in sums]
        for side in range(2):
            z = lax.rem(me + order[2 * pair + side] + zs, zs)
            for i in range(0, xs, 2):
                if side == 0:
                    value = jnp.where(left, sums[i], rolled[i + 1])
                else:
                    value = jnp.where(left, rolled[i], sums[i + 1])
                at = pl.multiple_of(z * (xs * HEAD_DIM) + i * HEAD_DIM, LANES)
                out_ref[:, pl.ds(at, LANES)] = value.astype(BF16)


def ring_order(count):
    order = [0]
    for t in range(1, count // 2):
        order += [-t, t]
    return order + [count // 2]


def shift(array, axis, by, wrap=True):
    count = lax.axis_size(axis)
    pairs = [(i, (i + by) % count) for i in range(count) if wrap or 0 <= i + by < count]
    return lax.ppermute(array, axis, pairs)


class Ring:
    def __init__(self, block):
        self.blocks = [block]
        self.up = self.down = block
        self.t = 0
        self.half = lax.axis_size("z") // 2

    def step(self):
        self.t += 1
        self.move()

    def move(self):
        if self.t < self.half:
            self.up = shift(self.up, "z", 1)
            self.down = shift(self.down, "z", -1)
            self.blocks += [self.up, self.down]
        elif self.t == self.half:
            self.blocks += [shift(self.up, "z", 1)]

    def tie(self, value):
        value, self.up, self.down = lax.optimization_barrier((value, self.up, self.down))
        if self.t and self.t < self.half:
            self.blocks[-2:] = [self.up, self.down]
        return value


def sent(array, axes):
    return lax.all_to_all(array, axes, 0, 0, tiled=True)


def gather_x(block):
    before = shift(block, "x", 1)
    after = shift(block, "x", -1)
    middle = block.shape[0] // 2
    across = (shift(before[:middle], "x", 1), shift(after[middle:], "x", -1))
    return block, before, after, *across


def per_device(
    x_proj, z_proj, b_proj, c_proj, dt_raw, dt_bias, a_log, d_skip,
    conv_x, conv_bias_x, conv_bc, conv_bias_bc, norm_weight, out_weight,
):
    xs, ys, cs = (lax.axis_size(a) for a in PLANE)
    zs = lax.axis_size("z")
    plane = xs * ys * cs
    rows, inner = x_proj.shape
    cols = inner // plane
    tokens = rows * plane
    part = lax.axis_index("x")
    heads = dt_bias.shape[0] // xs

    def own(values, axis):
        size = values.shape[axis] // xs
        return lax.dynamic_slice_in_dim(values, part * size, size, axis)

    ring = Ring((out_weight.T.astype(F32) * norm_weight[None]).astype(BF16))
    first_out = call(
        pack_first, shape((plane, rows, cols + 2 * LANES), BF16), (x_proj, b_proj, dt_raw)
    )
    first_out = ring.tie(first_out)
    first_in = sent(first_out, PLANE)
    ring.step()
    ring.step()
    second_out = call(pack_second, shape((plane, rows, cols + LANES), BF16), (z_proj, c_proj))
    per_head = jnp.stack([own(dt_bias, 0), own(-jnp.exp(a_log), 0), own(d_skip, 0)])
    per_head = jnp.pad(per_head, ((0, 5), (0, LANES - heads)))
    taps = jnp.pad(jnp.concatenate([own(conv_x, 1), own(conv_bias_x, 0)[None]]), ((0, 3), (0, 0)))
    group_taps = jnp.pad(
        jnp.concatenate([jnp.moveaxis(conv_bc, 0, 1), conv_bias_bc[:, None]], axis=1),
        ((0, 0), (0, 3), (0, 0)),
    ).reshape(16, LANES)
    first_in, second_out, per_head, taps, group_taps = ring.tie(
        (first_in, second_out, per_head, taps, group_taps)
    )
    packed = first_in.reshape(tokens, cols + 2 * LANES)
    halo = call(tail, shape((8, cols + 2 * LANES), BF16), (packed,), (), 1 << 16, 4)
    halo = shift(halo, "z", 1, wrap=False)
    second = sent(second_out, PLANE).reshape(tokens, cols + LANES)
    lanes = shape((tokens, LANES), F32)
    dt, cum, sums = call(steps, (lanes, lanes, lanes), (packed, per_head))
    x_conv, b_conv, held, states_out = call(
        scan_in,
        (
            shape((tokens, cols), BF16),
            shape((tokens, LANES), BF16),
            shape((tokens // SPAN, cols, STATE), BF16),
            shape((zs, cols // zs + 8, STATE), BF16),
        ),
        (packed, halo, taps, group_taps, dt, cum, sums),
        [pltpu.VMEM((tokens + 8, cols + LANES), F32)],
        1 << 25,
    )
    states_out, second = ring.tie((states_out, second))
    states_in = sent(states_out, "z")
    c_halo = call(tail, shape((8, LANES), BF16), (second,), (), 1 << 16, 4)
    c_halo = shift(c_halo, "z", 1, wrap=False)
    ring.step()
    ring.step()
    ring.step()
    states_in = ring.tie(states_in)
    starts = call(
        scan_all,
        shape((zs, cols // zs, STATE), BF16),
        (states_in,),
        [pltpu.VMEM((zs, LANES), F32)],
    )
    starts = ring.tie(starts)
    start = sent(starts, "z").reshape(cols, STATE)
    ring.step()
    ring.step()
    ring.step()
    c_conv, y = call(
        local,
        (shape((tokens, LANES), BF16), shape((tokens, cols), F32)),
        (x_conv, b_conv, second, c_halo, group_taps, dt, cum, held, per_head),
        [pltpu.VMEM((tokens + 8, LANES), F32)],
        1 << 27,
    )
    width = sum(block.shape[0] for block in ring.blocks)
    weights = call(stack, shape((width, inner // (ys * cs)), BF16), tuple(ring.blocks), (), 1 << 22, 8)
    start, weights = lax.optimization_barrier((start, weights))
    half = shape((tokens // 2, cols), BF16)
    theirs, ours = call(finish, (half, half), (start, c_conv, sums, y, second), (), 1 << 25)
    product = shape((tokens // 2, weights.shape[0]), BF16)
    theirs = gather_x(theirs)
    ours = gather_x(ours)
    away = call(project, product, (*theirs, weights), (), 1 << 29, 24)
    other = shift(away, "c", 1)
    both = call(project_add, product, (*ours, weights, other), (), 1 << 29, 24)
    shares = sent(both.reshape(xs * ys, rows, weights.shape[0]), ("x", "y"))

    def collect_all(shares_ref, out_ref):
        collect(shares_ref, out_ref, ys=ys)

    return call(collect_all, shape((rows, xs * weights.shape[0]), BF16), (shares,))


def solution(mesh):
    split = Mesh(mesh.devices.reshape(16, 4, 4, 2), ALL)
    return jax.shard_map(
        per_device,
        mesh=split,
        in_specs=(
            P(ALL, None),
            P(ALL, None),
            P(ALL, None),
            P(ALL, None),
            P(ALL, None),
            P(HEAD),
            P(HEAD),
            P(HEAD),
            P(None, HEAD),
            P(HEAD),
            P(None, None, HEAD),
            P(None, HEAD),
            P(HEAD),
            P(HEAD, SEQ),
        ),
        out_specs=P(ALL, None),
        check_vma=False,
    )
```

```python
import jax
import jax.numpy as jnp
from jax import lax
from jax.experimental import pallas as pl
from jax.experimental.pallas import tpu as pltpu
from jax.sharding import Mesh
from jax.sharding import PartitionSpec as P

HEAD_DIM = 64
STATE = 128
SPAN = 128
LANES = 128
F32 = jnp.float32
BF16 = jnp.bfloat16
SEQ = ("z", "x")
HEAD = ("y", "c")
PLANE = ("x", "y", "c")
ALL = ("z", "x", "y", "c")
VMEM = pl.BlockSpec(memory_space=pltpu.VMEM)
HBM = pl.BlockSpec(memory_space=pltpu.HBM)


def call(kernel, outs, inputs, scratch=(), flops=1 << 22, limit=16, far=(), far_out=False):
    return pl.pallas_call(
        kernel,
        out_shape=outs,
        in_specs=[HBM if i in far else VMEM for i in range(len(inputs))],
        out_specs=jax.tree.map(lambda _: HBM if far_out else VMEM, outs),
        scratch_shapes=list(scratch),
        compiler_params=pltpu.CompilerParams(vmem_limit_bytes=limit << 20),
        cost_estimate=pl.CostEstimate(flops=flops, bytes_accessed=1 << 20, transcendentals=0),
        name=kernel.__name__,
    )(*inputs)


def shape(dims, dtype):
    return jax.ShapeDtypeStruct(dims, dtype)


def silu(v):
    return v * (1.0 / (1.0 + jnp.exp(-v)))


def nt(a, b):
    return lax.dot_general(a, b, (((1,), (1,)), ((), ())), preferred_element_type=F32)


def tn(a, b):
    return lax.dot_general(a, b, (((0,), (0,)), ((), ())), preferred_element_type=F32)


def by_head(values, chunk, first):
    return jnp.where(first, values[:, 2 * chunk : 2 * chunk + 1], values[:, 2 * chunk + 1 : 2 * chunk + 2])


def left_half():
    return lax.broadcasted_iota(jnp.int32, (1, LANES), 1) < HEAD_DIM


def top_half():
    return lax.broadcasted_iota(jnp.int32, (LANES, 1), 0) < HEAD_DIM


def pack(
    x_far, z_far, b_far, c_far, dt_far, out_far,
    x_ref, z_ref, b_ref, c_ref, dt_ref, out_ref, in_sems, out_sems,
):
    pairs = ((dt_far, dt_ref), (b_far, b_ref), (c_far, c_ref), (x_far, x_ref), (z_far, z_ref))
    loads = [pltpu.make_async_copy(*pair, in_sems.at[i]) for i, pair in enumerate(pairs)]
    for load in loads:
        load.start()
    for load in loads:
        load.wait()
    count, _, width = out_ref.shape
    groups = b_ref.shape[1] // LANES
    parts = count // groups
    cols = x_ref.shape[1] // count
    heads = dt_ref.shape[1] // count
    dt = dt_ref[...].astype(F32)
    stores = [
        pltpu.make_async_copy(out_ref.at[d], out_far.at[d], out_sems.at[d]) for d in range(count)
    ]
    for d in range(count):
        part, group = divmod(d, groups)
        at = group * parts + part
        mine = dt if at == 0 else pltpu.roll(dt, LANES - at * heads, 1)
        side = slice(group * LANES, (group + 1) * LANES)
        out_ref[d, :, :cols] = x_ref[:, at * cols : (at + 1) * cols]
        out_ref[d, :, cols : cols + LANES] = b_ref[:, side]
        out_ref[d, :, cols + LANES : cols + 2 * LANES] = c_ref[:, side]
        out_ref[d, :, cols + 2 * LANES : width - LANES] = z_ref[:, at * cols : (at + 1) * cols]
        out_ref[d, :, width - LANES :] = mine.astype(BF16)
        if d > 0:
            stores[d - 1].start()
    stores[-1].start()
    for store in stores:
        store.wait()


def steps(packed_ref, heads_ref, dt_ref, cum_ref, sum_ref):
    rows, tokens = dt_ref.shape
    before = lax.broadcasted_iota(jnp.int32, (SPAN, SPAN), 0)
    after = lax.broadcasted_iota(jnp.int32, (SPAN, SPAN), 1)
    ones = (before <= after).astype(F32)
    bias, coeff = heads_ref[:, 0:1], heads_ref[:, 1:2]
    total = jnp.zeros((rows, 1), F32)
    for k in range(tokens // SPAN):
        part = slice(k * SPAN, (k + 1) * SPAN)
        raw = packed_ref[part, packed_ref.shape[1] - LANES :].astype(F32).T[:rows] + bias
        dt = jnp.maximum(raw, 0.0) + jnp.log1p(jnp.exp(-jnp.abs(raw)))
        dt_ref[:, part] = dt
        cum = lax.dot(
            coeff * dt, ones, precision=lax.Precision.HIGHEST, preferred_element_type=F32
        )
        cum_ref[:, part] = cum
        sum_ref[:, part] = cum + total
        total = total + cum[:, SPAN - 1 :]


def columns(rows):
    filled = jnp.concatenate([rows, jnp.zeros((SPAN - rows.shape[0], SPAN), F32)])
    return filled.T


def fill_padded(padded, halo_ref, packed_ref, width):
    padded[:8] = halo_ref[:, :width].astype(F32)
    padded[8:] = packed_ref[:, :width].astype(F32)


def conv(padded, taps, bias, k, lo):
    first = 8 + k * SPAN - 3
    total = bias + taps[0] * padded[first : first + SPAN, lo : lo + LANES]
    for j in range(1, 4):
        total = total + taps[j] * padded[first + j : first + j + SPAN, lo : lo + LANES]
    return silu(total).astype(BF16)


def scan_in(
    packed_ref, halo_ref, taps_ref, group_taps_ref, dt_ref, cum_ref, sum_ref,
    xs_ref, b_ref, held_ref, sent_ref, padded,
):
    tokens, cols = xs_ref.shape
    blocks = tokens // SPAN
    fill_padded(padded, halo_ref, packed_ref, cols + LANES)
    left, top = left_half(), top_half()
    group_taps = [group_taps_ref[j : j + 1] for j in range(4)]
    states = [jnp.zeros((LANES, STATE), F32) for _ in range(cols // LANES)]
    for k in range(blocks):
        part = slice(k * SPAN, (k + 1) * SPAN)
        b = conv(padded, group_taps, group_taps_ref[4:5], k, cols)
        b_ref[part] = b
        cum = cum_ref[:, part]
        scale = columns(dt_ref[:, part] * jnp.exp(cum[:, SPAN - 1 :] - cum))
        decay = columns(jnp.broadcast_to(jnp.exp(cum[:, SPAN - 1 :]), cum.shape))
        for chunk in range(cols // LANES):
            lo = chunk * LANES
            taps = [taps_ref[j : j + 1, lo : lo + LANES] for j in range(4)]
            xs = conv(padded, taps, taps_ref[4:5, lo : lo + LANES], k, lo)
            xs_ref[part, lo : lo + LANES] = xs
            weighted = (xs.astype(F32) * by_head(scale, chunk, left)).astype(BF16)
            held_ref[k, lo : lo + LANES] = states[chunk].astype(BF16)
            states[chunk] = by_head(decay, chunk, top) * states[chunk] + tn(weighted, b)
    count, extra = sent_ref.shape[0], sent_ref.shape[1]
    rows = cols // count
    for chunk in range(cols // LANES):
        final = states[chunk].astype(BF16)
        for i in range(LANES // rows):
            sent_ref[chunk * (LANES // rows) + i, :rows] = final[i * rows : (i + 1) * rows]
    total = columns(jnp.broadcast_to(sum_ref[:, tokens - 1 :], (sum_ref.shape[0], SPAN)))[:1]
    high = total.astype(BF16).astype(F32)
    middle = (total - high).astype(BF16).astype(F32)
    low = total - high - middle
    at = lax.broadcasted_iota(jnp.int32, (extra - rows, LANES), 0)
    tail = jnp.where(at == 0, high, jnp.where(at == 1, middle, jnp.where(at == 2, low, 0.0)))
    for d in range(count):
        sent_ref[d, rows:] = tail.astype(BF16)


def scan_all(inbox_ref, starts_ref, decays):
    count, rows, _ = starts_ref.shape
    tail = inbox_ref[:, rows:].astype(F32)
    logs = tail[:, 0] + tail[:, 1] + tail[:, 2]
    lanes = lax.broadcasted_iota(jnp.int32, logs.shape, 1)
    head = lax.axis_index("z") * rows // HEAD_DIM
    column = jnp.sum(jnp.where(lanes == head, logs, 0.0), axis=1, keepdims=True)
    decays[...] = jnp.broadcast_to(jnp.exp(column), decays.shape)
    state = jnp.zeros((rows, STATE), F32)
    for i in range(count):
        starts_ref[i] = state.astype(BF16)
        state = decays[i : i + 1] * state + inbox_ref[i, :rows].astype(F32)


def local(
    xs_ref, b_ref, packed_ref, halo_ref, group_taps_ref, dt_ref, cum_ref, held_ref, skip_ref,
    c_ref, y_ref, padded,
):
    tokens, cols = xs_ref.shape
    padded[:8] = halo_ref[:, cols + LANES : cols + 2 * LANES].astype(F32)
    padded[8:] = packed_ref[:, cols + LANES : cols + 2 * LANES].astype(F32)
    rows = lax.broadcasted_iota(jnp.int32, (SPAN, SPAN), 0)
    lanes = lax.broadcasted_iota(jnp.int32, (SPAN, SPAN), 1)
    causal = rows >= lanes
    left = left_half()
    taps = [group_taps_ref[8 + j : 9 + j] for j in range(4)]
    for k in range(tokens // SPAN):
        part = slice(k * SPAN, (k + 1) * SPAN)
        c = conv(padded, taps, group_taps_ref[12:13], k, 0)
        c_ref[part] = c
        scores = nt(c, b_ref[part])
        cum_t = cum_ref[:, part]
        dt_t = dt_ref[:, part]
        cum = columns(cum_t)
        grown = jnp.exp(cum)

        def mix(h):
            spread = cum[:, h : h + 1] - cum_t[h : h + 1]
            decays = jnp.exp(jnp.where(causal, spread, -jnp.inf))
            return (decays * dt_t[h : h + 1] * scores).astype(BF16)

        for chunk in range(cols // LANES):
            lo = chunk * LANES
            xs = xs_ref[part, lo : lo + LANES]
            y0 = jnp.dot(mix(2 * chunk), xs, preferred_element_type=F32)
            y1 = jnp.dot(mix(2 * chunk + 1), xs, preferred_element_type=F32)
            y = jnp.where(left, y0, y1) + by_head(skip_ref[...], chunk, left) * xs.astype(F32)
            if k > 0:
                y = y + nt(c, held_ref[k, lo : lo + LANES]) * by_head(grown, chunk, left)
            y_ref[part, lo : lo + LANES] = y


def finish(start_ref, c_ref, sum_ref, y_ref, packed_ref, out_ref):
    tokens, cols = y_ref.shape
    copies = out_ref.shape[0]
    rows = tokens // 32
    left = left_half()
    first = lax.axis_index("c") == 0
    for k in range(tokens // SPAN):
        part = slice(k * SPAN, (k + 1) * SPAN)
        grown = jnp.exp(columns(sum_ref[:, part]))
        for chunk in range(cols // LANES):
            lo = chunk * LANES
            carry = nt(c_ref[part], start_ref[lo : lo + LANES]) * by_head(grown, chunk, left)
            at = cols + 2 * LANES + lo
            z = packed_ref[part, at : at + LANES].astype(F32)
            gated = ((y_ref[part, lo : lo + LANES] + carry) * silu(z)).astype(BF16)
            for i in range(SPAN // (2 * rows)):
                even = gated[2 * i * rows : (2 * i + 1) * rows]
                odd = gated[(2 * i + 1) * rows : (2 * i + 2) * rows]
                theirs = jnp.where(first, odd, even)
                ours = jnp.where(first, even, odd)
                at = k * (SPAN // 2) + i * rows
                for d in range(copies):
                    out_ref[d, at : at + rows, lo : lo + LANES] = theirs
                    out_ref[d, tokens // 2 + at : tokens // 2 + at + rows, lo : lo + LANES] = ours


def multiply(gated_ref, first, weights_ref, out_ref, other_ref):
    parts, _, cols = gated_ref.shape
    rows, width = out_ref.shape
    squares = jnp.zeros((rows, 1), F32)
    for i in range(parts):
        value = gated_ref[i, first : first + rows].astype(F32)
        squares = squares + jnp.sum(value * value, axis=1, keepdims=True)
    scale = 1.0 / jnp.sqrt(squares / weights_ref.shape[1] + 1.0)
    step = 2 * LANES
    for lo in range(0, width, step):
        total = jnp.zeros((rows, step), F32)
        for i in range(parts):
            weights = weights_ref[lo : lo + step, i * cols : (i + 1) * cols]
            total = total + nt(gated_ref[i, first : first + rows], weights)
        total = total * scale
        if other_ref is not None:
            total = total + other_ref[:, lo : lo + step].astype(F32)
        out_ref[:, lo : lo + step] = total.astype(BF16)


def rescale(weights_ref, gain_ref, out_ref):
    for lo in range(0, out_ref.shape[0], SPAN):
        part = slice(lo, lo + SPAN)
        out_ref[part] = (weights_ref[part].astype(F32) * gain_ref[...]).astype(BF16)


def project(gated_ref, weights_ref, out_ref):
    multiply(gated_ref, 0, weights_ref, out_ref, None)


def project_add(gated_ref, weights_ref, other_ref, out_ref):
    multiply(gated_ref, out_ref.shape[0], weights_ref, out_ref, other_ref)


def tail(array_ref, out_ref):
    out_ref[...] = array_ref[array_ref.shape[0] - out_ref.shape[0] :, : out_ref.shape[1]]


def collect(shares_ref, out_ref, *, ys):
    count, rows, width = shares_ref.shape
    xs = count // ys
    left = left_half()
    for pair in range(width // LANES):
        lo = pair * LANES
        sums = []
        for i in range(xs):
            total = shares_ref[i * ys, :, lo : lo + LANES].astype(F32)
            for j in range(1, ys):
                total = total + shares_ref[i * ys + j, :, lo : lo + LANES].astype(F32)
            sums.append(total)
        rolled = [pltpu.roll(total, HEAD_DIM, 1) for total in sums]
        for side in range(2):
            for i in range(0, xs, 2):
                if side == 0:
                    value = jnp.where(left, sums[i], rolled[i + 1])
                else:
                    value = jnp.where(left, rolled[i], sums[i + 1])
                at = (2 * pair + side) * (xs * HEAD_DIM) + i * HEAD_DIM
                out_ref[:, at : at + LANES] = value.astype(BF16)


def shift(array, axis, by, wrap=True):
    count = lax.axis_size(axis)
    pairs = [(i, (i + by) % count) for i in range(count) if wrap or 0 <= i + by < count]
    return lax.ppermute(array, axis, pairs)


def sent(array, axes, name):
    with jax.named_scope(name):
        return lax.all_to_all(array, axes, 0, 0, tiled=True)


def per_device(
    x_proj, z_proj, b_proj, c_proj, dt_raw, dt_bias, a_log, d_skip,
    conv_x, conv_bias_x, conv_bc, conv_bias_bc, norm_weight, out_weight,
):
    xs, ys, cs = (lax.axis_size(a) for a in PLANE)
    zs = lax.axis_size("z")
    plane = xs * ys * cs
    rows, inner = x_proj.shape
    cols = inner // plane
    tokens = rows * plane
    part = lax.axis_index("x")
    heads = dt_bias.shape[0] // xs

    def own(values, axis):
        size = values.shape[axis] // xs
        return lax.dynamic_slice_in_dim(values, part * size, size, axis)

    weights = lax.all_gather(out_weight.T, "z", axis=0, tiled=True)
    out = call(
        pack,
        shape((plane, rows, 2 * cols + 3 * LANES), BF16),
        (x_proj, z_proj, b_proj, c_proj, dt_raw),
        [pltpu.VMEM(a.shape, BF16) for a in (x_proj, z_proj, b_proj, c_proj, dt_raw)]
        + [
            pltpu.VMEM((plane, rows, 2 * cols + 3 * LANES), BF16),
            pltpu.SemaphoreType.DMA((5,)),
            pltpu.SemaphoreType.DMA((plane,)),
        ],
        limit=60,
        far=range(5),
        far_out=True,
    )
    per_head = jnp.stack([own(dt_bias, 0), own(-jnp.exp(a_log), 0)], axis=1)
    per_head = jnp.pad(per_head, ((0, 8 - heads), (0, LANES - 2)))
    skip = jnp.pad(own(d_skip, 0), (0, LANES - heads))[None]
    taps = jnp.pad(jnp.concatenate([own(conv_x, 1), own(conv_bias_x, 0)[None]]), ((0, 3), (0, 0)))
    group_taps = jnp.pad(
        jnp.concatenate([jnp.moveaxis(conv_bc, 0, 1), conv_bias_bc[:, None]], axis=1),
        ((0, 0), (0, 3), (0, 0)),
    ).reshape(16, LANES)
    packed, per_head, skip, taps, group_taps = lax.optimization_barrier(
        (sent(out, PLANE, "entry"), per_head, skip, taps, group_taps)
    )
    packed = packed.reshape(tokens, 2 * cols + 3 * LANES)
    halo = call(tail, shape((8, cols + 2 * LANES), BF16), (packed,), (), 1 << 16, 4)
    halo = shift(halo, "z", 1, wrap=False)
    by_token = shape((8, tokens), F32)
    dt, cum, sums = call(steps, (by_token, by_token, by_token), (packed, per_head))
    x_conv, b_conv, held, states_out = call(
        scan_in,
        (
            shape((tokens, cols), BF16),
            shape((tokens, LANES), BF16),
            shape((tokens // SPAN, cols, STATE), BF16),
            shape((zs, cols // zs + 8, STATE), BF16),
        ),
        (packed, halo, taps, group_taps, dt, cum, sums),
        [pltpu.VMEM((tokens + 8, cols + LANES), F32)],
        1 << 25,
    )
    states_in = sent(states_out, "z", "pieces")
    c_conv, y = call(
        local,
        (shape((tokens, LANES), BF16), shape((tokens, cols), F32)),
        (x_conv, b_conv, packed, halo, group_taps, dt, cum, held, skip),
        [pltpu.VMEM((tokens + 8, LANES), F32)],
        1 << 27,
    )
    states_in, y = lax.optimization_barrier((states_in, y))
    starts = call(
        scan_all,
        shape((zs, cols // zs, STATE), BF16),
        (states_in,),
        [pltpu.VMEM((zs, LANES), F32)],
    )
    start = sent(starts, "z", "starts").reshape(cols, STATE)
    copies = call(
        finish, shape((xs, tokens, cols), BF16), (start, c_conv, sums, y, packed), (), 1 << 25
    )
    gated = sent(copies, "x", "gather")
    weights = call(rescale, shape(weights.shape, BF16), (weights, norm_weight[None]))
    product = shape((tokens // 2, weights.shape[0]), BF16)
    away = call(project, product, (gated, weights), (), 1 << 29, 24)
    other = shift(away, "c", 1)
    both = call(project_add, product, (gated, weights, other), (), 1 << 29, 24)
    shares = sent(both.reshape(xs * ys, rows, weights.shape[0]), ("x", "y"), "exit")

    def collect_all(shares_ref, out_ref):
        collect(shares_ref, out_ref, ys=ys)

    return call(collect_all, shape((rows, xs * weights.shape[0]), BF16), (shares,))


def solution(mesh):
    split = Mesh(mesh.devices.reshape(16, 4, 4, 2), ALL)
    return jax.shard_map(
        per_device,
        mesh=split,
        in_specs=(
            P(ALL, None),
            P(ALL, None),
            P(ALL, None),
            P(ALL, None),
            P(ALL, None),
            P(HEAD),
            P(HEAD),
            P(HEAD),
            P(None, HEAD),
            P(HEAD),
            P(None, None, HEAD),
            P(None, HEAD),
            P(HEAD),
            P(HEAD, SEQ),
        ),
        out_specs=P(ALL, None),
        check_vma=False,
    )
```

```python
import jax
import jax.numpy as jnp
from jax import lax
from jax.experimental import pallas as pl
from jax.experimental.pallas import tpu as pltpu
from jax.sharding import Mesh
from jax.sharding import PartitionSpec as P

HEAD_DIM = 64
STATE = 128
SPAN = 128
LANES = 128
F32 = jnp.float32
BF16 = jnp.bfloat16
Z = ("zh", "zl")
SEQ = ("zh", "zl", "x")
HEAD = ("y", "c")
PLANE = ("x", "y", "c")
ALL = ("zh", "zl", "x", "y", "c")
VMEM = pl.BlockSpec(memory_space=pltpu.VMEM)
HBM = pl.BlockSpec(memory_space=pltpu.HBM)


def call(kernel, outs, inputs, scratch=(), flops=1 << 22, limit=16, far=(), far_out=False):
    return pl.pallas_call(
        kernel,
        out_shape=outs,
        in_specs=[HBM if i in far else VMEM for i in range(len(inputs))],
        out_specs=jax.tree.map(lambda _: HBM if far_out else VMEM, outs),
        scratch_shapes=list(scratch),
        compiler_params=pltpu.CompilerParams(vmem_limit_bytes=limit << 20),
        cost_estimate=pl.CostEstimate(flops=flops, bytes_accessed=1 << 20, transcendentals=0),
    )(*inputs)


def shape(dims, dtype):
    return jax.ShapeDtypeStruct(dims, dtype)


def silu(v):
    return v * (1.0 / (1.0 + jnp.exp(-v)))


def nt(a, b):
    return lax.dot_general(a, b, (((1,), (1,)), ((), ())), preferred_element_type=F32)


def tn(a, b):
    return lax.dot_general(a, b, (((0,), (0,)), ((), ())), preferred_element_type=F32)


def by_head(values, chunk, first):
    return jnp.where(first, values[:, 2 * chunk : 2 * chunk + 1], values[:, 2 * chunk + 1 : 2 * chunk + 2])


def left_half():
    return lax.broadcasted_iota(jnp.int32, (1, LANES), 1) < HEAD_DIM


def top_half():
    return lax.broadcasted_iota(jnp.int32, (LANES, 1), 0) < HEAD_DIM


def pack(
    x_far, z_far, b_far, c_far, dt_far, out_far,
    x_ref, z_ref, b_ref, c_ref, dt_ref, out_ref, in_sems, out_sems,
):
    pairs = ((dt_far, dt_ref), (b_far, b_ref), (c_far, c_ref), (x_far, x_ref), (z_far, z_ref))
    loads = [pltpu.make_async_copy(*pair, in_sems.at[i]) for i, pair in enumerate(pairs)]
    for load in loads:
        load.start()
    for load in loads:
        load.wait()
    count, _, width = out_ref.shape
    groups = b_ref.shape[1] // LANES
    parts = count // groups
    cols = x_ref.shape[1] // count
    heads = dt_ref.shape[1] // count
    dt = dt_ref[...].astype(F32)
    stores = [
        pltpu.make_async_copy(out_ref.at[d], out_far.at[d], out_sems.at[d]) for d in range(count)
    ]
    for d in range(count):
        part, group = divmod(d, groups)
        at = group * parts + part
        mine = dt if at == 0 else pltpu.roll(dt, LANES - at * heads, 1)
        side = slice(group * LANES, (group + 1) * LANES)
        out_ref[d, :, :cols] = x_ref[:, at * cols : (at + 1) * cols]
        out_ref[d, :, cols : cols + LANES] = b_ref[:, side]
        out_ref[d, :, cols + LANES : cols + 2 * LANES] = c_ref[:, side]
        out_ref[d, :, cols + 2 * LANES : width - LANES] = z_ref[:, at * cols : (at + 1) * cols]
        out_ref[d, :, width - LANES :] = mine.astype(BF16)
        if d > 0:
            stores[d - 1].start()
    stores[-1].start()
    for store in stores:
        store.wait()


def steps(packed_ref, heads_ref, dt_ref, cum_ref, sum_ref):
    rows, tokens = dt_ref.shape
    before = lax.broadcasted_iota(jnp.int32, (SPAN, SPAN), 0)
    after = lax.broadcasted_iota(jnp.int32, (SPAN, SPAN), 1)
    ones = (before <= after).astype(F32)
    bias, coeff = heads_ref[:, 0:1], heads_ref[:, 1:2]
    total = jnp.zeros((rows, 1), F32)
    for k in range(tokens // SPAN):
        part = slice(k * SPAN, (k + 1) * SPAN)
        raw = packed_ref[part, packed_ref.shape[1] - LANES :].astype(F32).T[:rows] + bias
        dt = jnp.maximum(raw, 0.0) + jnp.log1p(jnp.exp(-jnp.abs(raw)))
        dt_ref[:, part] = dt
        cum = lax.dot(
            coeff * dt, ones, precision=lax.Precision.HIGHEST, preferred_element_type=F32
        )
        cum_ref[:, part] = cum
        sum_ref[:, part] = cum + total
        total = total + cum[:, SPAN - 1 :]


def columns(rows):
    filled = jnp.concatenate([rows, jnp.zeros((SPAN - rows.shape[0], SPAN), F32)])
    return filled.T


def fill_padded(padded, halo_ref, packed_ref, width):
    padded[:8] = halo_ref[:, :width].astype(F32)
    padded[8:] = packed_ref[:, :width].astype(F32)


def conv(padded, taps, bias, k, lo):
    first = 8 + k * SPAN - 3
    total = bias + taps[0] * padded[first : first + SPAN, lo : lo + LANES]
    for j in range(1, 4):
        total = total + taps[j] * padded[first + j : first + j + SPAN, lo : lo + LANES]
    return silu(total).astype(BF16)


def scan_in(
    packed_ref, halo_ref, taps_ref, group_taps_ref, dt_ref, cum_ref, sum_ref,
    xs_ref, b_ref, held_ref, sent_ref, padded,
):
    tokens, cols = xs_ref.shape
    blocks = tokens // SPAN
    fill_padded(padded, halo_ref, packed_ref, cols + LANES)
    left, top = left_half(), top_half()
    group_taps = [group_taps_ref[j : j + 1] for j in range(4)]
    states = [jnp.zeros((LANES, STATE), F32) for _ in range(cols // LANES)]
    for k in range(blocks):
        part = slice(k * SPAN, (k + 1) * SPAN)
        b = conv(padded, group_taps, group_taps_ref[4:5], k, cols)
        b_ref[part] = b
        cum = cum_ref[:, part]
        scale = columns(dt_ref[:, part] * jnp.exp(cum[:, SPAN - 1 :] - cum))
        decay = columns(jnp.broadcast_to(jnp.exp(cum[:, SPAN - 1 :]), cum.shape))
        for chunk in range(cols // LANES):
            lo = chunk * LANES
            taps = [taps_ref[j : j + 1, lo : lo + LANES] for j in range(4)]
            xs = conv(padded, taps, taps_ref[4:5, lo : lo + LANES], k, lo)
            xs_ref[part, lo : lo + LANES] = xs
            weighted = (xs.astype(F32) * by_head(scale, chunk, left)).astype(BF16)
            held_ref[k, lo : lo + LANES] = states[chunk].astype(BF16)
            states[chunk] = by_head(decay, chunk, top) * states[chunk] + tn(weighted, b)
    count = sent_ref.shape[0]
    rows = cols // count
    total = columns(jnp.broadcast_to(sum_ref[:, tokens - 1 :], (sum_ref.shape[0], SPAN)))[:1]
    for d in range(count):
        chunk, lo = divmod(d * rows, LANES)
        sent_ref[d, :rows] = states[chunk][lo : lo + rows].astype(BF16)
        sent_ref[d, rows:] = in_terms(total[:, d : d + 1])


def in_terms(value):
    high = value.astype(BF16).astype(F32)
    middle = (value - high).astype(BF16).astype(F32)
    low = value - high - middle
    at = lax.broadcasted_iota(jnp.int32, (8, LANES), 0)
    terms = jnp.where(at == 0, high, jnp.where(at == 1, middle, jnp.where(at == 2, low, 0.0)))
    return terms.astype(BF16)


def from_terms(terms):
    terms = terms.astype(F32)
    return terms[0:1] + terms[1:2] + terms[2:3]


def scan_near(inbox_ref, inner_ref, before_ref, sent_ref):
    count, rows, _ = inner_ref.shape
    state = jnp.zeros((rows, STATE), F32)
    log = jnp.zeros((1, LANES), F32)
    for i in range(count):
        inner_ref[i] = state
        before_ref[8 * i : 8 * i + 8] = jnp.broadcast_to(log, (8, LANES))
        mine = from_terms(inbox_ref[i, rows:])
        state = jnp.exp(mine) * state + inbox_ref[i, :rows].astype(F32)
        log = log + mine
    for d in range(sent_ref.shape[0]):
        sent_ref[d, :rows] = state.astype(BF16)
        sent_ref[d, rows:] = in_terms(log)


def scan_far(inbox_ref, inner_ref, before_ref, starts_ref):
    count, rows, _ = inner_ref.shape
    me = lax.axis_index("zh")
    state = jnp.zeros((rows, STATE), F32)
    for j in range(inbox_ref.shape[0]):
        later = jnp.exp(from_terms(inbox_ref[j, rows:])) * state + inbox_ref[j, :rows].astype(F32)
        state = jnp.where(j < me, later, state)
    for i in range(count):
        grown = jnp.exp(before_ref[8 * i : 8 * i + 1])
        starts_ref[i] = (grown * state + inner_ref[i]).astype(BF16)


def local(
    xs_ref, b_ref, packed_ref, halo_ref, group_taps_ref, dt_ref, cum_ref, held_ref, skip_ref,
    c_ref, y_ref, padded,
):
    tokens, cols = xs_ref.shape
    padded[:8] = halo_ref[:, cols + LANES : cols + 2 * LANES].astype(F32)
    padded[8:] = packed_ref[:, cols + LANES : cols + 2 * LANES].astype(F32)
    rows = lax.broadcasted_iota(jnp.int32, (SPAN, SPAN), 0)
    lanes = lax.broadcasted_iota(jnp.int32, (SPAN, SPAN), 1)
    causal = rows >= lanes
    left = left_half()
    taps = [group_taps_ref[8 + j : 9 + j] for j in range(4)]
    for k in range(tokens // SPAN):
        part = slice(k * SPAN, (k + 1) * SPAN)
        c = conv(padded, taps, group_taps_ref[12:13], k, 0)
        c_ref[part] = c
        scores = nt(c, b_ref[part])
        cum_t = cum_ref[:, part]
        dt_t = dt_ref[:, part]
        cum = columns(cum_t)
        grown = jnp.exp(cum)

        def mix(h):
            spread = cum[:, h : h + 1] - cum_t[h : h + 1]
            decays = jnp.exp(jnp.where(causal, spread, -jnp.inf))
            return (decays * dt_t[h : h + 1] * scores).astype(BF16)

        for chunk in range(cols // LANES):
            lo = chunk * LANES
            xs = xs_ref[part, lo : lo + LANES]
            y0 = jnp.dot(mix(2 * chunk), xs, preferred_element_type=F32)
            y1 = jnp.dot(mix(2 * chunk + 1), xs, preferred_element_type=F32)
            y = jnp.where(left, y0, y1) + by_head(skip_ref[...], chunk, left) * xs.astype(F32)
            if k > 0:
                y = y + nt(c, held_ref[k, lo : lo + LANES]) * by_head(grown, chunk, left)
            y_ref[part, lo : lo + LANES] = y


def finish(start_ref, c_ref, sum_ref, y_ref, packed_ref, out_ref):
    tokens, cols = y_ref.shape
    copies = out_ref.shape[0]
    rows = tokens // 32
    left = left_half()
    first = lax.axis_index("c") == 0
    for k in range(tokens // SPAN):
        part = slice(k * SPAN, (k + 1) * SPAN)
        grown = jnp.exp(columns(sum_ref[:, part]))
        for chunk in range(cols // LANES):
            lo = chunk * LANES
            carry = nt(c_ref[part], start_ref[lo : lo + LANES]) * by_head(grown, chunk, left)
            at = cols + 2 * LANES + lo
            z = packed_ref[part, at : at + LANES].astype(F32)
            gated = ((y_ref[part, lo : lo + LANES] + carry) * silu(z)).astype(BF16)
            for i in range(SPAN // (2 * rows)):
                even = gated[2 * i * rows : (2 * i + 1) * rows]
                odd = gated[(2 * i + 1) * rows : (2 * i + 2) * rows]
                theirs = jnp.where(first, odd, even)
                ours = jnp.where(first, even, odd)
                at = k * (SPAN // 2) + i * rows
                for d in range(copies):
                    out_ref[d, at : at + rows, lo : lo + LANES] = theirs
                    out_ref[d, tokens // 2 + at : tokens // 2 + at + rows, lo : lo + LANES] = ours


def multiply(gated_ref, first, weights_ref, out_ref, other_ref):
    parts, _, cols = gated_ref.shape
    rows, width = out_ref.shape
    squares = jnp.zeros((rows, 1), F32)
    for i in range(parts):
        value = gated_ref[i, first : first + rows].astype(F32)
        squares = squares + jnp.sum(value * value, axis=1, keepdims=True)
    scale = 1.0 / jnp.sqrt(squares / weights_ref.shape[1] + 1.0)
    step = 2 * LANES
    for lo in range(0, width, step):
        total = jnp.zeros((rows, step), F32)
        for i in range(parts):
            weights = weights_ref[lo : lo + step, i * cols : (i + 1) * cols]
            total = total + nt(gated_ref[i, first : first + rows], weights)
        total = total * scale
        if other_ref is not None:
            total = total + other_ref[:, lo : lo + step].astype(F32)
        out_ref[:, lo : lo + step] = total.astype(BF16)


def rescale(weights_ref, gain_ref, out_ref):
    for lo in range(0, out_ref.shape[0], SPAN):
        part = slice(lo, lo + SPAN)
        out_ref[part] = (weights_ref[part].astype(F32) * gain_ref[...]).astype(BF16)


def project(gated_ref, weights_ref, out_ref):
    multiply(gated_ref, 0, weights_ref, out_ref, None)


def project_add(gated_ref, weights_ref, other_ref, out_ref):
    multiply(gated_ref, out_ref.shape[0], weights_ref, out_ref, other_ref)


def tail(array_ref, out_ref):
    out_ref[...] = array_ref[array_ref.shape[0] - out_ref.shape[0] :, : out_ref.shape[1]]


def collect(shares_ref, out_ref, *, ys):
    count, _, width = shares_ref.shape
    xs = count // ys
    left = left_half()
    for pair in range(width // LANES):
        lo = pair * LANES
        sums = []
        for i in range(xs):
            total = shares_ref[i * ys, :, lo : lo + LANES].astype(F32)
            for j in range(1, ys):
                total = total + shares_ref[i * ys + j, :, lo : lo + LANES].astype(F32)
            sums.append(total)
        rolled = [pltpu.roll(total, HEAD_DIM, 1) for total in sums]
        for side in range(2):
            for i in range(0, xs, 2):
                if side == 0:
                    value = jnp.where(left, sums[i], rolled[i + 1])
                else:
                    value = jnp.where(left, rolled[i], sums[i + 1])
                at = (2 * pair + side) * (xs * HEAD_DIM) + i * HEAD_DIM
                out_ref[:, at : at + LANES] = value.astype(BF16)


def shift(array, axis, by, wrap=True):
    count = lax.axis_size(axis)
    pairs = [(i, (i + by) % count) for i in range(count) if wrap or 0 <= i + by < count]
    return lax.ppermute(array, axis, pairs)


def sent(array, axes):
    return lax.all_to_all(array, axes, 0, 0, tiled=True)


def per_device(
    x_proj, z_proj, b_proj, c_proj, dt_raw, dt_bias, a_log, d_skip,
    conv_x, conv_bias_x, conv_bc, conv_bias_bc, norm_weight, out_weight,
):
    xs, ys, cs = (lax.axis_size(a) for a in PLANE)
    zh, zl = (lax.axis_size(a) for a in Z)
    plane = xs * ys * cs
    rows, inner = x_proj.shape
    cols = inner // plane
    tokens = rows * plane
    part = lax.axis_index("x")
    heads = dt_bias.shape[0] // xs

    def own(values, axis):
        size = values.shape[axis] // xs
        return lax.dynamic_slice_in_dim(values, part * size, size, axis)

    weights = lax.all_gather(out_weight.T, Z, axis=0, tiled=True)
    out = call(
        pack,
        shape((plane, rows, 2 * cols + 3 * LANES), BF16),
        (x_proj, z_proj, b_proj, c_proj, dt_raw),
        [pltpu.VMEM(a.shape, BF16) for a in (x_proj, z_proj, b_proj, c_proj, dt_raw)]
        + [
            pltpu.VMEM((plane, rows, 2 * cols + 3 * LANES), BF16),
            pltpu.SemaphoreType.DMA((5,)),
            pltpu.SemaphoreType.DMA((plane,)),
        ],
        limit=60,
        far=range(5),
        far_out=True,
    )
    per_head = jnp.stack([own(dt_bias, 0), own(-jnp.exp(a_log), 0)], axis=1)
    per_head = jnp.pad(per_head, ((0, 8 - heads), (0, LANES - 2)))
    skip = jnp.pad(own(d_skip, 0), (0, LANES - heads))[None]
    taps = jnp.pad(jnp.concatenate([own(conv_x, 1), own(conv_bias_x, 0)[None]]), ((0, 3), (0, 0)))
    group_taps = jnp.pad(
        jnp.concatenate([jnp.moveaxis(conv_bc, 0, 1), conv_bias_bc[:, None]], axis=1),
        ((0, 0), (0, 3), (0, 0)),
    ).reshape(16, LANES)
    packed, per_head, skip, taps, group_taps = lax.optimization_barrier(
        (sent(out, PLANE), per_head, skip, taps, group_taps)
    )
    packed = packed.reshape(tokens, 2 * cols + 3 * LANES)
    halo = call(tail, shape((8, cols + 2 * LANES), BF16), (packed,), (), 1 << 16, 4)
    halo = shift(halo, Z, 1, wrap=False)
    by_token = shape((8, tokens), F32)
    dt, cum, sums = call(steps, (by_token, by_token, by_token), (packed, per_head))
    x_conv, b_conv, held, states_out = call(
        scan_in,
        (
            shape((tokens, cols), BF16),
            shape((tokens, LANES), BF16),
            shape((tokens // SPAN, cols, STATE), BF16),
            shape((zl, cols // zl + 8, STATE), BF16),
        ),
        (packed, halo, taps, group_taps, dt, cum, sums),
        [pltpu.VMEM((tokens + 8, cols + LANES), F32)],
        1 << 25,
    )
    near_in = sent(states_out, "zl")
    near = zl, cols // zl, STATE
    inner, before, far_out = call(
        scan_near,
        (shape(near, F32), shape((8 * zl, LANES), F32), shape((zh, cols // zl + 8, STATE), BF16)),
        (near_in,),
    )
    far_in = sent(far_out, "zh")
    starts = call(scan_far, shape(near, BF16), (far_in, inner, before))
    start = sent(starts, "zl").reshape(cols, STATE)
    c_conv, y = call(
        local,
        (shape((tokens, LANES), BF16), shape((tokens, cols), F32)),
        (x_conv, b_conv, packed, halo, group_taps, dt, cum, held, skip),
        [pltpu.VMEM((tokens + 8, LANES), F32)],
        1 << 27,
    )
    copies = call(
        finish, shape((xs, tokens, cols), BF16), (start, c_conv, sums, y, packed), (), 1 << 25
    )
    gated = sent(copies, "x")
    weights = call(rescale, shape(weights.shape, BF16), (weights, norm_weight[None]))
    product = shape((tokens // 2, weights.shape[0]), BF16)
    away = call(project, product, (gated, weights), (), 1 << 29, 24)
    other = shift(away, "c", 1)
    both = call(project_add, product, (gated, weights, other), (), 1 << 29, 24)
    shares = sent(both.reshape(xs * ys, rows, weights.shape[0]), ("x", "y"))

    def collect_all(shares_ref, out_ref):
        collect(shares_ref, out_ref, ys=ys)

    return call(collect_all, shape((rows, xs * weights.shape[0]), BF16), (shares,))


def solution(mesh):
    split = Mesh(mesh.devices.reshape(4, 4, 4, 4, 2), ALL)
    return jax.shard_map(
        per_device,
        mesh=split,
        in_specs=(
            P(ALL, None),
            P(ALL, None),
            P(ALL, None),
            P(ALL, None),
            P(ALL, None),
            P(HEAD),
            P(HEAD),
            P(HEAD),
            P(None, HEAD),
            P(HEAD),
            P(None, None, HEAD),
            P(None, HEAD),
            P(HEAD),
            P(HEAD, SEQ),
        ),
        out_specs=P(ALL, None),
        check_vma=False,
    )
```

```python
import jax
import jax.numpy as jnp
from jax import lax
from jax.experimental import pallas as pl
from jax.experimental.pallas import tpu as pltpu
from jax.sharding import Mesh
from jax.sharding import PartitionSpec as P

HEAD_DIM = 64
STATE = 128
SPAN = 128
LANES = 128
F32 = jnp.float32
BF16 = jnp.bfloat16
Z = ("zh", "zl")
X = ("xh", "xl")
SEQ = ("zh", "zl", "xh", "xl")
HEAD = ("y", "c")
PLANE = ("xh", "xl", "y", "c")
ALL = ("zh", "zl", "xh", "xl", "y", "c")
VMEM = pl.BlockSpec(memory_space=pltpu.VMEM)
HBM = pl.BlockSpec(memory_space=pltpu.HBM)


def call(kernel, outs, inputs, scratch=(), flops=1 << 22, limit=16, far=(), far_out=False):
    return pl.pallas_call(
        kernel,
        out_shape=outs,
        in_specs=[HBM if i in far else VMEM for i in range(len(inputs))],
        out_specs=jax.tree.map(lambda _: HBM if far_out else VMEM, outs),
        scratch_shapes=list(scratch),
        compiler_params=pltpu.CompilerParams(vmem_limit_bytes=limit << 20),
        cost_estimate=pl.CostEstimate(flops=flops, bytes_accessed=1 << 20, transcendentals=0),
    )(*inputs)


def shape(dims, dtype):
    return jax.ShapeDtypeStruct(dims, dtype)


def silu(v):
    return v * (1.0 / (1.0 + jnp.exp(-v)))


def nt(a, b):
    return lax.dot_general(a, b, (((1,), (1,)), ((), ())), preferred_element_type=F32)


def tn(a, b):
    return lax.dot_general(a, b, (((0,), (0,)), ((), ())), preferred_element_type=F32)


def by_head(values, chunk, first):
    return jnp.where(first, values[:, 2 * chunk : 2 * chunk + 1], values[:, 2 * chunk + 1 : 2 * chunk + 2])


def left_half():
    return lax.broadcasted_iota(jnp.int32, (1, LANES), 1) < HEAD_DIM


def top_half():
    return lax.broadcasted_iota(jnp.int32, (LANES, 1), 0) < HEAD_DIM


def pack(
    x_far, z_far, b_far, c_far, dt_far, out_far,
    x_ref, z_ref, b_ref, c_ref, dt_ref, out_ref, in_sems, out_sems,
):
    pairs = ((dt_far, dt_ref), (b_far, b_ref), (c_far, c_ref), (x_far, x_ref), (z_far, z_ref))
    loads = [pltpu.make_async_copy(*pair, in_sems.at[i]) for i, pair in enumerate(pairs)]
    for load in loads:
        load.start()
    for load in loads:
        load.wait()
    count, _, width = out_ref.shape
    groups = b_ref.shape[1] // LANES
    parts = count // groups
    cols = x_ref.shape[1] // count
    heads = dt_ref.shape[1] // count
    dt = dt_ref[...].astype(F32)
    stores = [
        pltpu.make_async_copy(out_ref.at[d], out_far.at[d], out_sems.at[d]) for d in range(count)
    ]
    for d in range(count):
        part, group = divmod(d, groups)
        at = group * parts + part
        mine = dt if at == 0 else pltpu.roll(dt, LANES - at * heads, 1)
        side = slice(group * LANES, (group + 1) * LANES)
        out_ref[d, :, :cols] = x_ref[:, at * cols : (at + 1) * cols]
        out_ref[d, :, cols : cols + LANES] = b_ref[:, side]
        out_ref[d, :, cols + LANES : cols + 2 * LANES] = c_ref[:, side]
        out_ref[d, :, cols + 2 * LANES : width - LANES] = z_ref[:, at * cols : (at + 1) * cols]
        out_ref[d, :, width - LANES :] = mine.astype(BF16)
        if d > 0:
            stores[d - 1].start()
    stores[-1].start()
    for store in stores:
        store.wait()


def steps(packed_ref, heads_ref, dt_ref, cum_ref, sum_ref, late_ref):
    rows, tokens = dt_ref.shape
    width = late_ref.shape[1]
    late_ref[...] = packed_ref[:, packed_ref.shape[1] - LANES - width : packed_ref.shape[1] - LANES]
    before = lax.broadcasted_iota(jnp.int32, (SPAN, SPAN), 0)
    after = lax.broadcasted_iota(jnp.int32, (SPAN, SPAN), 1)
    ones = (before <= after).astype(F32)
    bias, coeff = heads_ref[:, 0:1], heads_ref[:, 1:2]
    total = jnp.zeros((rows, 1), F32)
    for k in range(tokens // SPAN):
        part = slice(k * SPAN, (k + 1) * SPAN)
        raw = packed_ref[part, packed_ref.shape[1] - LANES :].astype(F32).T[:rows] + bias
        dt = jnp.maximum(raw, 0.0) + jnp.log1p(jnp.exp(-jnp.abs(raw)))
        dt_ref[:, part] = dt
        cum = lax.dot(
            coeff * dt, ones, precision=lax.Precision.HIGHEST, preferred_element_type=F32
        )
        cum_ref[:, part] = cum
        sum_ref[:, part] = cum + total
        total = total + cum[:, SPAN - 1 :]


def columns(rows):
    filled = jnp.concatenate([rows, jnp.zeros((SPAN - rows.shape[0], SPAN), F32)])
    return filled.T


def fill_padded(padded, halo_ref, packed_ref, width):
    padded[:8] = halo_ref[:, :width].astype(F32)
    padded[8:] = packed_ref[:, :width].astype(F32)


def conv(padded, taps, bias, k, lo):
    first = 8 + k * SPAN - 3
    total = bias + taps[0] * padded[first : first + SPAN, lo : lo + LANES]
    for j in range(1, 4):
        total = total + taps[j] * padded[first + j : first + j + SPAN, lo : lo + LANES]
    return silu(total).astype(BF16)


def scan_in(
    packed_ref, halo_ref, taps_ref, group_taps_ref, dt_ref, cum_ref, sum_ref,
    xs_ref, b_ref, held_ref, sent_ref, padded,
):
    tokens, cols = xs_ref.shape
    blocks = tokens // SPAN
    fill_padded(padded, halo_ref, packed_ref, cols + LANES)
    left, top = left_half(), top_half()
    group_taps = [group_taps_ref[j : j + 1] for j in range(4)]
    states = [jnp.zeros((LANES, STATE), F32) for _ in range(cols // LANES)]
    for k in range(blocks):
        part = slice(k * SPAN, (k + 1) * SPAN)
        b = conv(padded, group_taps, group_taps_ref[4:5], k, cols)
        b_ref[part] = b
        cum = cum_ref[:, part]
        scale = columns(dt_ref[:, part] * jnp.exp(cum[:, SPAN - 1 :] - cum))
        decay = columns(jnp.broadcast_to(jnp.exp(cum[:, SPAN - 1 :]), cum.shape))
        for chunk in range(cols // LANES):
            lo = chunk * LANES
            taps = [taps_ref[j : j + 1, lo : lo + LANES] for j in range(4)]
            xs = conv(padded, taps, taps_ref[4:5, lo : lo + LANES], k, lo)
            xs_ref[part, lo : lo + LANES] = xs
            weighted = (xs.astype(F32) * by_head(scale, chunk, left)).astype(BF16)
            held_ref[k, lo : lo + LANES] = states[chunk].astype(BF16)
            states[chunk] = by_head(decay, chunk, top) * states[chunk] + tn(weighted, b)
    count = sent_ref.shape[0]
    rows = cols // count
    total = columns(jnp.broadcast_to(sum_ref[:, tokens - 1 :], (sum_ref.shape[0], SPAN)))[:1]
    for d in range(count):
        chunk, lo = divmod(d * rows, LANES)
        sent_ref[d, :rows] = states[chunk][lo : lo + rows].astype(BF16)
        sent_ref[d, rows:] = in_terms(total[:, d : d + 1])


def in_terms(value):
    high = value.astype(BF16).astype(F32)
    middle = (value - high).astype(BF16).astype(F32)
    low = value - high - middle
    at = lax.broadcasted_iota(jnp.int32, (8, LANES), 0)
    terms = jnp.where(at == 0, high, jnp.where(at == 1, middle, jnp.where(at == 2, low, 0.0)))
    return terms.astype(BF16)


def from_terms(terms):
    terms = terms.astype(F32)
    return terms[0:1] + terms[1:2] + terms[2:3]


def scan_near(inbox_ref, inner_ref, before_ref, sent_ref):
    count, rows, _ = inner_ref.shape
    state = jnp.zeros((rows, STATE), F32)
    log = jnp.zeros((1, LANES), F32)
    for i in range(count):
        inner_ref[i] = state
        before_ref[8 * i : 8 * i + 8] = jnp.broadcast_to(log, (8, LANES))
        mine = from_terms(inbox_ref[i, rows:])
        state = jnp.exp(mine) * state + inbox_ref[i, :rows].astype(F32)
        log = log + mine
    for d in range(sent_ref.shape[0]):
        sent_ref[d, :rows] = state.astype(BF16)
        sent_ref[d, rows:] = in_terms(log)


def scan_far(inbox_ref, inner_ref, before_ref, starts_ref):
    count, rows, _ = inner_ref.shape
    me = lax.axis_index("zh")
    state = jnp.zeros((rows, STATE), F32)
    for j in range(inbox_ref.shape[0]):
        later = jnp.exp(from_terms(inbox_ref[j, rows:])) * state + inbox_ref[j, :rows].astype(F32)
        state = jnp.where(j < me, later, state)
    for i in range(count):
        grown = jnp.exp(before_ref[8 * i : 8 * i + 1])
        starts_ref[i] = (grown * state + inner_ref[i]).astype(BF16)


def local(
    xs_ref, b_ref, late_ref, halo_ref, group_taps_ref, dt_ref, cum_ref, held_ref, skip_ref,
    c_ref, y_ref, padded,
):
    tokens, cols = xs_ref.shape
    padded[:8] = halo_ref[:, cols + LANES : cols + 2 * LANES].astype(F32)
    padded[8:] = late_ref[:, :LANES].astype(F32)
    rows = lax.broadcasted_iota(jnp.int32, (SPAN, SPAN), 0)
    lanes = lax.broadcasted_iota(jnp.int32, (SPAN, SPAN), 1)
    causal = rows >= lanes
    left = left_half()
    taps = [group_taps_ref[8 + j : 9 + j] for j in range(4)]
    for k in range(tokens // SPAN):
        part = slice(k * SPAN, (k + 1) * SPAN)
        c = conv(padded, taps, group_taps_ref[12:13], k, 0)
        c_ref[part] = c
        scores = nt(c, b_ref[part])
        cum_t = cum_ref[:, part]
        dt_t = dt_ref[:, part]
        cum = columns(cum_t)
        grown = jnp.exp(cum)

        def mix(h):
            spread = cum[:, h : h + 1] - cum_t[h : h + 1]
            decays = jnp.exp(jnp.where(causal, spread, -jnp.inf))
            return (decays * dt_t[h : h + 1] * scores).astype(BF16)

        for chunk in range(cols // LANES):
            lo = chunk * LANES
            xs = xs_ref[part, lo : lo + LANES]
            y0 = jnp.dot(mix(2 * chunk), xs, preferred_element_type=F32)
            y1 = jnp.dot(mix(2 * chunk + 1), xs, preferred_element_type=F32)
            y = jnp.where(left, y0, y1) + by_head(skip_ref[...], chunk, left) * xs.astype(F32)
            if k > 0:
                y = y + nt(c, held_ref[k, lo : lo + LANES]) * by_head(grown, chunk, left)
            y_ref[part, lo : lo + LANES] = y


def finish(start_ref, c_ref, sum_ref, y_ref, late_ref, out_ref, *, ys):
    tokens, cols = y_ref.shape
    rows = tokens // 32
    half = out_ref.shape[1] // 2
    left = left_half()
    first = lax.axis_index("c") == 0
    for k in range(tokens // SPAN):
        part = slice(k * SPAN, (k + 1) * SPAN)
        grown = jnp.exp(columns(sum_ref[:, part]))
        for chunk in range(cols // LANES):
            lo = chunk * LANES
            carry = nt(c_ref[part], start_ref[lo : lo + LANES]) * by_head(grown, chunk, left)
            z = late_ref[part, LANES + lo : 2 * LANES + lo].astype(F32)
            gated = ((y_ref[part, lo : lo + LANES] + carry) * silu(z)).astype(BF16)
            for i in range(SPAN // (2 * rows)):
                even = gated[2 * i * rows : (2 * i + 1) * rows]
                odd = gated[(2 * i + 1) * rows : (2 * i + 2) * rows]
                theirs = jnp.where(first, odd, even)
                ours = jnp.where(first, even, odd)
                x, y = divmod(k * (SPAN // (2 * rows)) + i, ys)
                at = (x // 2 * ys + y) * rows
                for d in range(x % 2, out_ref.shape[0], 2):
                    out_ref[d, at : at + rows, lo : lo + LANES] = theirs
                    out_ref[d, half + at : half + at + rows, lo : lo + LANES] = ours


def rescale(weights_ref, gain_ref, out_ref):
    for lo in range(0, out_ref.shape[0], SPAN):
        part = slice(lo, lo + SPAN)
        out_ref[part] = (weights_ref[part].astype(F32) * gain_ref[...]).astype(BF16)


def multiply(first, gated_ref, weights_far, out_ref, weights_ref, sems):
    parts, _, cols = gated_ref.shape
    rows, width = out_ref.shape
    step = width // sems.shape[0]
    loads = []
    for j in range(sems.shape[0]):
        span = pl.ds(j * step, step)
        loads.append(pltpu.make_async_copy(weights_far.at[span], weights_ref.at[span], sems.at[j]))
        loads[-1].start()
    squares = jnp.zeros((rows, 1), F32)
    for i in range(parts):
        value = gated_ref[i, first : first + rows].astype(F32)
        squares = squares + jnp.sum(value * value, axis=1, keepdims=True)
    scale = 1.0 / jnp.sqrt(squares / weights_ref.shape[1] + 1.0)
    for j, load in enumerate(loads):
        lo = j * step
        load.wait()
        total = jnp.zeros((rows, step), F32)
        for i in range(parts):
            weights = weights_ref[lo : lo + step, i * cols : (i + 1) * cols]
            total = total + nt(gated_ref[i, first : first + rows], weights)
        out_ref[:, lo : lo + step] = (total * scale).astype(BF16)


def project_theirs(*refs):
    multiply(0, *refs)


def project_ours(gated_ref, weights_far, out_ref, *refs):
    multiply(out_ref.shape[0], gated_ref, weights_far, out_ref, *refs)


def add(ours_ref, other_ref, out_ref):
    out_ref[...] = (ours_ref[...].astype(F32) + other_ref[...].astype(F32)).astype(BF16)


def tail(array_ref, out_ref):
    out_ref[...] = array_ref[array_ref.shape[0] - out_ref.shape[0] :, : out_ref.shape[1]]


def collect(shares_ref, out_ref, *, ys):
    count, _, width = shares_ref.shape
    halves = count // ys
    for k in range(width // LANES):
        for i in range(halves):
            total = shares_ref[i * ys, :, k * LANES : (k + 1) * LANES].astype(F32)
            for j in range(1, ys):
                total = total + shares_ref[i * ys + j, :, k * LANES : (k + 1) * LANES].astype(F32)
            at = (k * halves + i) * LANES
            out_ref[:, at : at + LANES] = total.astype(BF16)


def shift(array, axis, by, wrap=True):
    count = lax.axis_size(axis)
    pairs = [(i, (i + by) % count) for i in range(count) if wrap or 0 <= i + by < count]
    return lax.ppermute(array, axis, pairs)


def sent(array, axes):
    return lax.all_to_all(array, axes, 0, 0, tiled=True)


def per_device(
    x_proj, z_proj, b_proj, c_proj, dt_raw, dt_bias, a_log, d_skip,
    conv_x, conv_bias_x, conv_bc, conv_bias_bc, norm_weight, out_weight,
):
    xh, xl, ys, cs = (lax.axis_size(a) for a in PLANE)
    xs = xh * xl
    zh, zl = (lax.axis_size(a) for a in Z)
    plane = xs * ys * cs
    rows, inner = x_proj.shape
    cols = inner // plane
    tokens = rows * plane
    part = lax.axis_index("xh") * xl + lax.axis_index("xl")
    heads = dt_bias.shape[0] // xs

    def own(values, axis):
        size = values.shape[axis] // xs
        return lax.dynamic_slice_in_dim(values, part * size, size, axis)

    mine = out_weight.T
    other = shift(mine, "xl", 1)
    even = lax.axis_index("xl") == 0
    pair = jnp.concatenate([jnp.where(even, mine, other), jnp.where(even, other, mine)])
    weights = lax.all_gather(pair, Z, axis=0, tiled=True)
    out = call(
        pack,
        shape((plane, rows, 2 * cols + 3 * LANES), BF16),
        (x_proj, z_proj, b_proj, c_proj, dt_raw),
        [pltpu.VMEM(a.shape, BF16) for a in (x_proj, z_proj, b_proj, c_proj, dt_raw)]
        + [
            pltpu.VMEM((plane, rows, 2 * cols + 3 * LANES), BF16),
            pltpu.SemaphoreType.DMA((5,)),
            pltpu.SemaphoreType.DMA((plane,)),
        ],
        limit=60,
        far=range(5),
        far_out=True,
    )
    per_head = jnp.stack([own(dt_bias, 0), own(-jnp.exp(a_log), 0)], axis=1)
    per_head = jnp.pad(per_head, ((0, 8 - heads), (0, LANES - 2)))
    skip = jnp.pad(own(d_skip, 0), (0, LANES - heads))[None]
    taps = jnp.pad(jnp.concatenate([own(conv_x, 1), own(conv_bias_x, 0)[None]]), ((0, 3), (0, 0)))
    group_taps = jnp.pad(
        jnp.concatenate([jnp.moveaxis(conv_bc, 0, 1), conv_bias_bc[:, None]], axis=1),
        ((0, 0), (0, 3), (0, 0)),
    ).reshape(16, LANES)
    packed, per_head, skip, taps, group_taps = lax.optimization_barrier(
        (sent(out, PLANE), per_head, skip, taps, group_taps)
    )
    packed = packed.reshape(tokens, 2 * cols + 3 * LANES)
    halo = call(tail, shape((8, cols + 2 * LANES), BF16), (packed,), (), 1 << 16, 4)
    halo = shift(halo, Z, 1, wrap=False)
    by_token = shape((8, tokens), F32)
    late = shape((tokens, cols + LANES), BF16)
    dt, cum, sums, late = call(steps, (by_token, by_token, by_token, late), (packed, per_head))
    x_conv, b_conv, held, states_out = call(
        scan_in,
        (
            shape((tokens, cols), BF16),
            shape((tokens, LANES), BF16),
            shape((tokens // SPAN, cols, STATE), BF16),
            shape((zl, cols // zl + 8, STATE), BF16),
        ),
        (packed, halo, taps, group_taps, dt, cum, sums),
        [pltpu.VMEM((tokens + 8, cols + LANES), F32)],
        1 << 25,
    )
    near_in = sent(states_out, "zl")
    near = zl, cols // zl, STATE
    inner, before, far_out = call(
        scan_near,
        (shape(near, F32), shape((8 * zl, LANES), F32), shape((zh, cols // zl + 8, STATE), BF16)),
        (near_in,),
    )
    c_conv, y = call(
        local,
        (shape((tokens, LANES), BF16), shape((tokens, cols), F32)),
        (x_conv, b_conv, late, halo, group_taps, dt, cum, held, skip),
        [pltpu.VMEM((tokens + 8, LANES), F32)],
        1 << 27,
    )
    far_in, c_conv, y = lax.optimization_barrier((sent(far_out, "zh"), c_conv, y))
    starts = call(scan_far, shape(near, BF16), (far_in, inner, before))
    start = sent(starts, "zl").reshape(cols, STATE)

    def finish_all(*refs):
        finish(*refs, ys=ys)

    def collect_all(*refs):
        collect(*refs, ys=ys)

    copies = call(
        finish_all,
        shape((xs, tokens // xl, cols), BF16),
        (start, c_conv, sums, y, late),
        (),
        1 << 25,
    )
    gated = sent(copies, X)
    weights = call(rescale, shape(weights.shape, BF16), (weights, norm_weight[None]), (), 1 << 22, 60)
    count = tokens // (2 * xl)
    product = shape((count, weights.shape[0]), BF16)
    room = [pltpu.VMEM(weights.shape, BF16), pltpu.SemaphoreType.DMA((8,))]
    theirs = call(project_theirs, product, (gated, weights), room, 1 << 30, 50, (1,))
    ours = call(project_ours, product, (gated, weights), room, 1 << 30, 50, (1,))
    both = call(add, product, (ours, shift(theirs, "c", 1)))
    shares = sent(both.reshape(xh * ys, rows, weights.shape[0]), ("xh", "y"))
    return call(collect_all, shape((rows, xh * weights.shape[0]), BF16), (shares,))


def solution(mesh):
    split = Mesh(mesh.devices.reshape(4, 4, 2, 2, 4, 2), ALL)
    return jax.shard_map(
        per_device,
        mesh=split,
        in_specs=(
            P(ALL, None),
            P(ALL, None),
            P(ALL, None),
            P(ALL, None),
            P(ALL, None),
            P(HEAD),
            P(HEAD),
            P(HEAD),
            P(None, HEAD),
            P(HEAD),
            P(None, None, HEAD),
            P(None, HEAD),
            P(HEAD),
            P(HEAD, SEQ),
        ),
        out_specs=P(ALL, None),
        check_vma=False,
    )
```

```python
import jax
import jax.numpy as jnp
from jax import lax
from jax.experimental import pallas as pl
from jax.experimental.pallas import tpu as pltpu
from jax.sharding import Mesh
from jax.sharding import PartitionSpec as P

HEAD_DIM = 64
STATE = 128
SPAN = 128
LANES = 128
F32 = jnp.float32
BF16 = jnp.bfloat16
Z = ("zh", "zl")
X = ("xh", "xl")
SEQ = ("zh", "zl", "xh", "xl")
HEAD = ("y", "c")
PLANE = ("xh", "xl", "y", "c")
ALL = ("zh", "zl", "xh", "xl", "y", "c")
VMEM = pl.BlockSpec(memory_space=pltpu.VMEM)
HBM = pl.BlockSpec(memory_space=pltpu.HBM)


def call(kernel, outs, inputs, scratch=(), flops=1 << 22, limit=16, far=(), far_out=False):
    return pl.pallas_call(
        kernel,
        out_shape=outs,
        in_specs=[HBM if i in far else VMEM for i in range(len(inputs))],
        out_specs=jax.tree.map(lambda _: HBM if far_out else VMEM, outs),
        scratch_shapes=list(scratch),
        compiler_params=pltpu.CompilerParams(vmem_limit_bytes=limit << 20),
        cost_estimate=pl.CostEstimate(flops=flops, bytes_accessed=1 << 20, transcendentals=0),
    )(*inputs)


def shape(dims, dtype):
    return jax.ShapeDtypeStruct(dims, dtype)


def silu(v):
    return v * (1.0 / (1.0 + jnp.exp(-v)))


def nt(a, b):
    return lax.dot_general(a, b, (((1,), (1,)), ((), ())), preferred_element_type=F32)


def tn(a, b):
    return lax.dot_general(a, b, (((0,), (0,)), ((), ())), preferred_element_type=F32)


def by_head(values, chunk, first):
    return jnp.where(first, values[:, 2 * chunk : 2 * chunk + 1], values[:, 2 * chunk + 1 : 2 * chunk + 2])


def left_half():
    return lax.broadcasted_iota(jnp.int32, (1, LANES), 1) < HEAD_DIM


def top_half():
    return lax.broadcasted_iota(jnp.int32, (LANES, 1), 0) < HEAD_DIM


def pack(
    x_far, z_far, b_far, c_far, dt_far, out_far,
    x_ref, z_ref, b_ref, c_ref, dt_ref, out_ref, in_sems, out_sems,
):
    pairs = ((dt_far, dt_ref), (b_far, b_ref), (c_far, c_ref), (x_far, x_ref), (z_far, z_ref))
    loads = [pltpu.make_async_copy(*pair, in_sems.at[i]) for i, pair in enumerate(pairs)]
    for load in loads:
        load.start()
    for load in loads:
        load.wait()
    count, _, width = out_ref.shape
    groups = b_ref.shape[1] // LANES
    parts = count // groups
    cols = x_ref.shape[1] // count
    heads = dt_ref.shape[1] // count
    dt = dt_ref[...].astype(F32)
    stores = [
        pltpu.make_async_copy(out_ref.at[d], out_far.at[d], out_sems.at[d]) for d in range(count)
    ]
    for d in range(count):
        part, group = divmod(d, groups)
        at = group * parts + part
        mine = dt if at == 0 else pltpu.roll(dt, LANES - at * heads, 1)
        side = slice(group * LANES, (group + 1) * LANES)
        out_ref[d, :, :cols] = x_ref[:, at * cols : (at + 1) * cols]
        out_ref[d, :, cols : cols + LANES] = b_ref[:, side]
        out_ref[d, :, cols + LANES : cols + 2 * LANES] = c_ref[:, side]
        out_ref[d, :, cols + 2 * LANES : width - LANES] = z_ref[:, at * cols : (at + 1) * cols]
        out_ref[d, :, width - LANES :] = mine.astype(BF16)
        if d > 0:
            stores[d - 1].start()
    stores[-1].start()
    for store in stores:
        store.wait()


def steps(packed_ref, heads_ref, dt_ref, cum_ref, sum_ref, late_ref):
    rows, tokens = dt_ref.shape
    width = late_ref.shape[1]
    late_ref[...] = packed_ref[:, packed_ref.shape[1] - LANES - width : packed_ref.shape[1] - LANES]
    before = lax.broadcasted_iota(jnp.int32, (SPAN, SPAN), 0)
    after = lax.broadcasted_iota(jnp.int32, (SPAN, SPAN), 1)
    ones = (before <= after).astype(F32)
    bias, coeff = heads_ref[:, 0:1], heads_ref[:, 1:2]
    total = jnp.zeros((rows, 1), F32)
    for k in range(tokens // SPAN):
        part = slice(k * SPAN, (k + 1) * SPAN)
        raw = packed_ref[part, packed_ref.shape[1] - LANES :].astype(F32).T[:rows] + bias
        dt = jnp.maximum(raw, 0.0) + jnp.log1p(jnp.exp(-jnp.abs(raw)))
        dt_ref[:, part] = dt
        cum = lax.dot(
            coeff * dt, ones, precision=lax.Precision.HIGHEST, preferred_element_type=F32
        )
        cum_ref[:, part] = cum
        sum_ref[:, part] = cum + total
        total = total + cum[:, SPAN - 1 :]


def columns(rows):
    filled = jnp.concatenate([rows, jnp.zeros((SPAN - rows.shape[0], SPAN), F32)])
    return filled.T


def fill_padded(padded, halo_ref, packed_ref, width):
    padded[:8] = halo_ref[:, :width].astype(F32)
    padded[8:] = packed_ref[:, :width].astype(F32)


def conv(padded, taps, bias, k, lo):
    first = 8 + k * SPAN - 3
    total = bias + taps[0] * padded[first : first + SPAN, lo : lo + LANES]
    for j in range(1, 4):
        total = total + taps[j] * padded[first + j : first + j + SPAN, lo : lo + LANES]
    return silu(total).astype(BF16)


def scan_in(
    packed_ref, halo_ref, taps_ref, group_taps_ref, dt_ref, cum_ref, sum_ref,
    xs_ref, b_ref, held_ref, sent_ref, padded,
):
    tokens, cols = xs_ref.shape
    blocks = tokens // SPAN
    fill_padded(padded, halo_ref, packed_ref, cols + LANES)
    left, top = left_half(), top_half()
    group_taps = [group_taps_ref[j : j + 1] for j in range(4)]
    states = [jnp.zeros((LANES, STATE), F32) for _ in range(cols // LANES)]
    for k in range(blocks):
        part = slice(k * SPAN, (k + 1) * SPAN)
        b = conv(padded, group_taps, group_taps_ref[4:5], k, cols)
        b_ref[part] = b
        cum = cum_ref[:, part]
        scale = columns(dt_ref[:, part] * jnp.exp(cum[:, SPAN - 1 :] - cum))
        decay = columns(jnp.broadcast_to(jnp.exp(cum[:, SPAN - 1 :]), cum.shape))
        for chunk in range(cols // LANES):
            lo = chunk * LANES
            taps = [taps_ref[j : j + 1, lo : lo + LANES] for j in range(4)]
            xs = conv(padded, taps, taps_ref[4:5, lo : lo + LANES], k, lo)
            xs_ref[part, lo : lo + LANES] = xs
            weighted = (xs.astype(F32) * by_head(scale, chunk, left)).astype(BF16)
            held_ref[k, lo : lo + LANES] = states[chunk].astype(BF16)
            states[chunk] = by_head(decay, chunk, top) * states[chunk] + tn(weighted, b)
    count = sent_ref.shape[0]
    rows = cols // count
    total = columns(jnp.broadcast_to(sum_ref[:, tokens - 1 :], (sum_ref.shape[0], SPAN)))[:1]
    for d in range(count):
        chunk, lo = divmod(d * rows, LANES)
        sent_ref[d, :rows] = states[chunk][lo : lo + rows].astype(BF16)
        sent_ref[d, rows:] = in_terms(total[:, d : d + 1])


def in_terms(value):
    high = value.astype(BF16).astype(F32)
    middle = (value - high).astype(BF16).astype(F32)
    low = value - high - middle
    at = lax.broadcasted_iota(jnp.int32, (8, LANES), 0)
    terms = jnp.where(at == 0, high, jnp.where(at == 1, middle, jnp.where(at == 2, low, 0.0)))
    return terms.astype(BF16)


def from_terms(terms):
    terms = terms.astype(F32)
    return terms[0:1] + terms[1:2] + terms[2:3]


def scan_near(inbox_ref, inner_ref, before_ref, group_ref, sent_ref):
    count, rows, _ = inner_ref.shape
    state = jnp.zeros((rows, STATE), F32)
    log = jnp.zeros((1, LANES), F32)
    for i in range(count):
        inner_ref[i] = state
        before_ref[8 * i : 8 * i + 8] = jnp.broadcast_to(log, (8, LANES))
        mine = from_terms(inbox_ref[i, rows:])
        state = jnp.exp(mine) * state + inbox_ref[i, :rows].astype(F32)
        log = log + mine
    before_ref[8 * count :] = jnp.broadcast_to(log, (8, LANES))
    group_ref[...] = state
    sent_ref[...] = state.astype(BF16)


def extend(inbox_ref, before_ref, group_ref, sent_ref):
    grown = jnp.exp(before_ref[before_ref.shape[0] - 1 :])
    sent_ref[...] = (grown * inbox_ref[...].astype(F32) + group_ref[...]).astype(BF16)


def scan_far(inner_ref, before_ref, *refs):
    starts_ref = refs[-1]
    state = refs[0][...].astype(F32)
    for ref in refs[1:-1]:
        state = state + ref[...].astype(F32)
    for i in range(inner_ref.shape[0]):
        grown = jnp.exp(before_ref[8 * i : 8 * i + 1])
        starts_ref[i] = (grown * state + inner_ref[i]).astype(BF16)


def local(
    xs_ref, b_ref, late_ref, halo_ref, group_taps_ref, dt_ref, cum_ref, held_ref, skip_ref,
    c_ref, y_ref, padded,
):
    tokens, cols = xs_ref.shape
    padded[:8] = halo_ref[:, cols + LANES : cols + 2 * LANES].astype(F32)
    padded[8:] = late_ref[:, :LANES].astype(F32)
    rows = lax.broadcasted_iota(jnp.int32, (SPAN, SPAN), 0)
    lanes = lax.broadcasted_iota(jnp.int32, (SPAN, SPAN), 1)
    causal = rows >= lanes
    left = left_half()
    taps = [group_taps_ref[8 + j : 9 + j] for j in range(4)]
    for k in range(tokens // SPAN):
        part = slice(k * SPAN, (k + 1) * SPAN)
        c = conv(padded, taps, group_taps_ref[12:13], k, 0)
        c_ref[part] = c
        scores = nt(c, b_ref[part])
        cum_t = cum_ref[:, part]
        dt_t = dt_ref[:, part]
        cum = columns(cum_t)
        grown = jnp.exp(cum)

        def mix(h):
            spread = cum[:, h : h + 1] - cum_t[h : h + 1]
            decays = jnp.exp(jnp.where(causal, spread, -jnp.inf))
            return (decays * dt_t[h : h + 1] * scores).astype(BF16)

        for chunk in range(cols // LANES):
            lo = chunk * LANES
            xs = xs_ref[part, lo : lo + LANES]
            y0 = jnp.dot(mix(2 * chunk), xs, preferred_element_type=F32)
            y1 = jnp.dot(mix(2 * chunk + 1), xs, preferred_element_type=F32)
            y = jnp.where(left, y0, y1) + by_head(skip_ref[...], chunk, left) * xs.astype(F32)
            if k > 0:
                y = y + nt(c, held_ref[k, lo : lo + LANES]) * by_head(grown, chunk, left)
            y_ref[part, lo : lo + LANES] = y


def finish(start_ref, c_ref, sum_ref, y_ref, late_ref, out_ref, *, ys):
    tokens, cols = y_ref.shape
    rows = tokens // 32
    half = out_ref.shape[1] // 2
    left = left_half()
    first = lax.axis_index("c") == 0
    for k in range(tokens // SPAN):
        part = slice(k * SPAN, (k + 1) * SPAN)
        grown = jnp.exp(columns(sum_ref[:, part]))
        for chunk in range(cols // LANES):
            lo = chunk * LANES
            carry = nt(c_ref[part], start_ref[lo : lo + LANES]) * by_head(grown, chunk, left)
            z = late_ref[part, LANES + lo : 2 * LANES + lo].astype(F32)
            gated = ((y_ref[part, lo : lo + LANES] + carry) * silu(z)).astype(BF16)
            for i in range(SPAN // (2 * rows)):
                even = gated[2 * i * rows : (2 * i + 1) * rows]
                odd = gated[(2 * i + 1) * rows : (2 * i + 2) * rows]
                theirs = jnp.where(first, odd, even)
                ours = jnp.where(first, even, odd)
                x, y = divmod(k * (SPAN // (2 * rows)) + i, ys)
                at = (x // 2 * ys + y) * rows
                for d in range(x % 2, out_ref.shape[0], 2):
                    out_ref[d, at : at + rows, lo : lo + LANES] = theirs
                    out_ref[d, half + at : half + at + rows, lo : lo + LANES] = ours


def project(gated_ref, weights_far, theirs_ref, ours_ref, weights_ref, sems):
    parts, rows, cols = gated_ref.shape
    half, width = ours_ref.shape
    step = width // sems.shape[0]
    loads = []
    for j in range(sems.shape[0]):
        span = pl.ds(j * step, step)
        loads.append(pltpu.make_async_copy(weights_far.at[span], weights_ref.at[span], sems.at[j]))
        loads[-1].start()
    squares = jnp.zeros((rows, 1), F32)
    for i in range(parts):
        value = gated_ref[i].astype(F32)
        squares = squares + jnp.sum(value * value, axis=1, keepdims=True)
    scale = 1.0 / jnp.sqrt(squares / weights_ref.shape[1] + 1.0)
    for j, load in enumerate(loads):
        lo = j * step
        load.wait()
        total = jnp.zeros((rows, step), F32)
        for i in range(parts):
            weights = weights_ref[lo : lo + step, i * cols : (i + 1) * cols]
            total = total + nt(gated_ref[i], weights)
        total = (total * scale).astype(BF16)
        theirs_ref[:, lo : lo + step] = total[:half]
        ours_ref[:, lo : lo + step] = total[half:]


def add(ours_ref, other_ref, out_ref):
    out_ref[...] = (ours_ref[...].astype(F32) + other_ref[...].astype(F32)).astype(BF16)


def tail(array_ref, out_ref):
    out_ref[...] = array_ref[array_ref.shape[0] - out_ref.shape[0] :, : out_ref.shape[1]]


def collect(shares_ref, out_ref, *, ys):
    count, _, width = shares_ref.shape
    halves = count // ys
    for k in range(width // LANES):
        for i in range(halves):
            total = shares_ref[i * ys, :, k * LANES : (k + 1) * LANES].astype(F32)
            for j in range(1, ys):
                total = total + shares_ref[i * ys + j, :, k * LANES : (k + 1) * LANES].astype(F32)
            at = (k * halves + i) * LANES
            out_ref[:, at : at + LANES] = total.astype(BF16)


def shift(array, axis, by, wrap=True):
    count = lax.axis_size(axis)
    pairs = [(i, (i + by) % count) for i in range(count) if wrap or 0 <= i + by < count]
    return lax.ppermute(array, axis, pairs)


def sent(array, axes):
    return lax.all_to_all(array, axes, 0, 0, tiled=True)


def per_device(
    x_proj, z_proj, b_proj, c_proj, dt_raw, dt_bias, a_log, d_skip,
    conv_x, conv_bias_x, conv_bc, conv_bias_bc, norm_weight, out_weight,
):
    xh, xl, ys, cs = (lax.axis_size(a) for a in PLANE)
    xs = xh * xl
    zh, zl = (lax.axis_size(a) for a in Z)
    plane = xs * ys * cs
    rows, inner = x_proj.shape
    cols = inner // plane
    tokens = rows * plane
    part = lax.axis_index("xh") * xl + lax.axis_index("xl")
    heads = dt_bias.shape[0] // xs

    def own(values, axis):
        size = values.shape[axis] // xs
        return lax.dynamic_slice_in_dim(values, part * size, size, axis)

    scaled = (out_weight.T.astype(F32) * norm_weight[None]).astype(BF16)
    weights = lax.all_gather(scaled, (*Z, "xl"), axis=0, tiled=True)
    out = call(
        pack,
        shape((plane, rows, 2 * cols + 3 * LANES), BF16),
        (x_proj, z_proj, b_proj, c_proj, dt_raw),
        [pltpu.VMEM(a.shape, BF16) for a in (x_proj, z_proj, b_proj, c_proj, dt_raw)]
        + [
            pltpu.VMEM((plane, rows, 2 * cols + 3 * LANES), BF16),
            pltpu.SemaphoreType.DMA((5,)),
            pltpu.SemaphoreType.DMA((plane,)),
        ],
        limit=60,
        far=range(5),
        far_out=True,
    )
    per_head = jnp.stack([own(dt_bias, 0), own(-jnp.exp(a_log), 0)], axis=1)
    per_head = jnp.pad(per_head, ((0, 8 - heads), (0, LANES - 2)))
    skip = jnp.pad(own(d_skip, 0), (0, LANES - heads))[None]
    taps = jnp.pad(jnp.concatenate([own(conv_x, 1), own(conv_bias_x, 0)[None]]), ((0, 3), (0, 0)))
    group_taps = jnp.pad(
        jnp.concatenate([jnp.moveaxis(conv_bc, 0, 1), conv_bias_bc[:, None]], axis=1),
        ((0, 0), (0, 3), (0, 0)),
    ).reshape(16, LANES)
    packed, per_head, skip, taps, group_taps = lax.optimization_barrier(
        (sent(out, PLANE), per_head, skip, taps, group_taps)
    )
    packed = packed.reshape(tokens, 2 * cols + 3 * LANES)
    halo = call(tail, shape((8, cols + 2 * LANES), BF16), (packed,), (), 1 << 16, 4)
    halo = shift(halo, Z, 1, wrap=False)
    by_token = shape((8, tokens), F32)
    late = shape((tokens, cols + LANES), BF16)
    dt, cum, sums, late = call(steps, (by_token, by_token, by_token, late), (packed, per_head))
    x_conv, b_conv, held, states_out = call(
        scan_in,
        (
            shape((tokens, cols), BF16),
            shape((tokens, LANES), BF16),
            shape((tokens // SPAN, cols, STATE), BF16),
            shape((zl, cols // zl + 8, STATE), BF16),
        ),
        (packed, halo, taps, group_taps, dt, cum, sums),
        [pltpu.VMEM((tokens + 8, cols + LANES), F32)],
        1 << 25,
    )
    c_conv, y = call(
        local,
        (shape((tokens, LANES), BF16), shape((tokens, cols), F32)),
        (x_conv, b_conv, late, halo, group_taps, dt, cum, held, skip),
        [pltpu.VMEM((tokens + 8, LANES), F32)],
        1 << 27,
    )
    near_in, c_conv, y = lax.optimization_barrier((sent(states_out, "zl"), c_conv, y))
    near = zl, cols // zl, STATE
    inner, before, group, ahead = call(
        scan_near,
        (
            shape(near, F32),
            shape((8 * zl + 8, LANES), F32),
            shape(near[1:], F32),
            shape(near[1:], BF16),
        ),
        (near_in,),
    )
    inboxes = []
    for hop in range(zh - 1):
        if hop:
            ahead = call(extend, shape(near[1:], BF16), (inboxes[-1], before, group))
        inboxes.append(lax.ppermute(ahead, "zh", [(hop, hop + 1)]))
    starts = call(scan_far, shape(near, BF16), (inner, before, *inboxes))
    start = sent(starts, "zl").reshape(cols, STATE)

    def finish_all(*refs):
        finish(*refs, ys=ys)

    def collect_all(*refs):
        collect(*refs, ys=ys)

    copies = call(
        finish_all,
        shape((xs, tokens // xl, cols), BF16),
        (start, c_conv, sums, y, late),
        (),
        1 << 25,
    )
    gated = sent(copies, X)
    count = tokens // (2 * xl)
    product = shape((count, weights.shape[0]), BF16)
    room = [pltpu.VMEM(weights.shape, BF16), pltpu.SemaphoreType.DMA((8,))]
    theirs, ours = call(project, (product, product), (gated, weights), room, 1 << 30, 50, (1,))
    both = call(add, product, (ours, shift(theirs, "c", 1)))
    shares = sent(both.reshape(xh * ys, rows, weights.shape[0]), ("xh", "y"))
    return call(collect_all, shape((rows, xh * weights.shape[0]), BF16), (shares,))


def solution(mesh):
    split = Mesh(mesh.devices.reshape(4, 4, 2, 2, 4, 2), ALL)
    return jax.shard_map(
        per_device,
        mesh=split,
        in_specs=(
            P(ALL, None),
            P(ALL, None),
            P(ALL, None),
            P(ALL, None),
            P(ALL, None),
            P(HEAD),
            P(HEAD),
            P(HEAD),
            P(None, HEAD),
            P(HEAD),
            P(None, None, HEAD),
            P(None, HEAD),
            P(HEAD),
            P(HEAD, SEQ),
        ),
        out_specs=P(ALL, None),
        check_vma=False,
    )
```

```python
import jax
import jax.numpy as jnp
from jax import lax
from jax.experimental import pallas as pl
from jax.experimental.pallas import tpu as pltpu
from jax.sharding import Mesh
from jax.sharding import PartitionSpec as P

HEAD_DIM = 64
STATE = 128
SPAN = 128
LANES = 128
F32 = jnp.float32
BF16 = jnp.bfloat16
Z = ("zh", "zl")
X = ("xh", "xl")
SEQ = ("zh", "zl", "xh", "xl")
HEAD = ("y", "c")
PLANE = ("xh", "xl", "y", "c")
ALL = ("zh", "zl", "xh", "xl", "y", "c")
VMEM = pl.BlockSpec(memory_space=pltpu.VMEM)
HBM = pl.BlockSpec(memory_space=pltpu.HBM)


def call(kernel, outs, inputs, scratch=(), flops=1 << 22, limit=16, far=(), far_out=False):
    return pl.pallas_call(
        kernel,
        out_shape=outs,
        in_specs=[HBM if i in far else VMEM for i in range(len(inputs))],
        out_specs=jax.tree.map(lambda _: HBM if far_out else VMEM, outs),
        scratch_shapes=list(scratch),
        compiler_params=pltpu.CompilerParams(vmem_limit_bytes=limit << 20),
        cost_estimate=pl.CostEstimate(flops=flops, bytes_accessed=1 << 20, transcendentals=0),
    )(*inputs)


def shape(dims, dtype):
    return jax.ShapeDtypeStruct(dims, dtype)


def silu(v):
    return v * (1.0 / (1.0 + jnp.exp(-v)))


def nt(a, b):
    return lax.dot_general(a, b, (((1,), (1,)), ((), ())), preferred_element_type=F32)


def tn(a, b):
    return lax.dot_general(a, b, (((0,), (0,)), ((), ())), preferred_element_type=F32)


def by_head(values, chunk, first):
    return jnp.where(first, values[:, 2 * chunk : 2 * chunk + 1], values[:, 2 * chunk + 1 : 2 * chunk + 2])


def left_half():
    return lax.broadcasted_iota(jnp.int32, (1, LANES), 1) < HEAD_DIM


def top_half():
    return lax.broadcasted_iota(jnp.int32, (LANES, 1), 0) < HEAD_DIM


def pack(
    x_far, z_far, b_far, c_far, dt_far, out_far,
    x_ref, z_ref, b_ref, c_ref, dt_ref, out_ref, in_sems, out_sems,
):
    pairs = ((dt_far, dt_ref), (b_far, b_ref), (c_far, c_ref), (x_far, x_ref), (z_far, z_ref))
    loads = [pltpu.make_async_copy(*pair, in_sems.at[i]) for i, pair in enumerate(pairs)]
    for load in loads:
        load.start()
    for load in loads:
        load.wait()
    count, _, width = out_ref.shape
    groups = b_ref.shape[1] // LANES
    parts = count // groups
    cols = x_ref.shape[1] // count
    heads = dt_ref.shape[1] // count
    dt = dt_ref[...].astype(F32)
    stores = [
        pltpu.make_async_copy(out_ref.at[d], out_far.at[d], out_sems.at[d]) for d in range(count)
    ]
    for d in range(count):
        part, group = divmod(d, groups)
        at = group * parts + part
        mine = dt if at == 0 else pltpu.roll(dt, LANES - at * heads, 1)
        side = slice(group * LANES, (group + 1) * LANES)
        out_ref[d, :, :cols] = x_ref[:, at * cols : (at + 1) * cols]
        out_ref[d, :, cols : cols + LANES] = b_ref[:, side]
        out_ref[d, :, cols + LANES : cols + 2 * LANES] = c_ref[:, side]
        out_ref[d, :, cols + 2 * LANES : width - LANES] = z_ref[:, at * cols : (at + 1) * cols]
        out_ref[d, :, width - LANES :] = mine.astype(BF16)
        if d > 0:
            stores[d - 1].start()
    stores[-1].start()
    for store in stores:
        store.wait()


def steps(packed_ref, heads_ref, dt_ref, cum_ref, sum_ref, late_ref):
    rows, tokens = dt_ref.shape
    width = late_ref.shape[1]
    late_ref[...] = packed_ref[:, packed_ref.shape[1] - LANES - width : packed_ref.shape[1] - LANES]
    before = lax.broadcasted_iota(jnp.int32, (SPAN, SPAN), 0)
    after = lax.broadcasted_iota(jnp.int32, (SPAN, SPAN), 1)
    ones = (before <= after).astype(F32)
    bias, coeff = heads_ref[:, 0:1], heads_ref[:, 1:2]
    total = jnp.zeros((rows, 1), F32)
    for k in range(tokens // SPAN):
        part = slice(k * SPAN, (k + 1) * SPAN)
        raw = packed_ref[part, packed_ref.shape[1] - LANES :].astype(F32).T[:rows] + bias
        dt = jnp.maximum(raw, 0.0) + jnp.log1p(jnp.exp(-jnp.abs(raw)))
        dt_ref[:, part] = dt
        cum = lax.dot(
            coeff * dt, ones, precision=lax.Precision.HIGHEST, preferred_element_type=F32
        )
        cum_ref[:, part] = cum
        sum_ref[:, part] = cum + total
        total = total + cum[:, SPAN - 1 :]


def columns(rows):
    filled = jnp.concatenate([rows, jnp.zeros((SPAN - rows.shape[0], SPAN), F32)])
    return filled.T


def fill_padded(padded, halo_ref, packed_ref, width):
    padded[:8] = halo_ref[:, :width].astype(F32)
    padded[8:] = packed_ref[:, :width].astype(F32)


def conv(padded, taps, bias, k, lo):
    first = 8 + k * SPAN - 3
    total = bias + taps[0] * padded[first : first + SPAN, lo : lo + LANES]
    for j in range(1, 4):
        total = total + taps[j] * padded[first + j : first + j + SPAN, lo : lo + LANES]
    return silu(total).astype(BF16)


def scan_in(
    packed_ref, halo_ref, taps_ref, group_taps_ref, dt_ref, cum_ref, sum_ref,
    xs_ref, b_ref, held_ref, sent_ref, padded,
):
    tokens, cols = xs_ref.shape
    blocks = tokens // SPAN
    fill_padded(padded, halo_ref, packed_ref, cols + LANES)
    left, top = left_half(), top_half()
    group_taps = [group_taps_ref[j : j + 1] for j in range(4)]
    states = [jnp.zeros((LANES, STATE), F32) for _ in range(cols // LANES)]
    for k in range(blocks):
        part = slice(k * SPAN, (k + 1) * SPAN)
        b = conv(padded, group_taps, group_taps_ref[4:5], k, cols)
        b_ref[part] = b
        cum = cum_ref[:, part]
        scale = columns(dt_ref[:, part] * jnp.exp(cum[:, SPAN - 1 :] - cum))
        decay = columns(jnp.broadcast_to(jnp.exp(cum[:, SPAN - 1 :]), cum.shape))
        for chunk in range(cols // LANES):
            lo = chunk * LANES
            taps = [taps_ref[j : j + 1, lo : lo + LANES] for j in range(4)]
            xs = conv(padded, taps, taps_ref[4:5, lo : lo + LANES], k, lo)
            xs_ref[part, lo : lo + LANES] = xs
            weighted = (xs.astype(F32) * by_head(scale, chunk, left)).astype(BF16)
            held_ref[k, lo : lo + LANES] = states[chunk].astype(BF16)
            states[chunk] = by_head(decay, chunk, top) * states[chunk] + tn(weighted, b)
    count = sent_ref.shape[0]
    rows = cols // count
    total = columns(jnp.broadcast_to(sum_ref[:, tokens - 1 :], (sum_ref.shape[0], SPAN)))[:1]
    for d in range(count):
        chunk, lo = divmod(d * rows, LANES)
        sent_ref[d, :rows] = states[chunk][lo : lo + rows].astype(BF16)
        sent_ref[d, rows:] = in_terms(total[:, d : d + 1])


def in_terms(value):
    high = value.astype(BF16).astype(F32)
    middle = (value - high).astype(BF16).astype(F32)
    low = value - high - middle
    at = lax.broadcasted_iota(jnp.int32, (8, LANES), 0)
    terms = jnp.where(at == 0, high, jnp.where(at == 1, middle, jnp.where(at == 2, low, 0.0)))
    return terms.astype(BF16)


def from_terms(terms):
    terms = terms.astype(F32)
    return terms[0:1] + terms[1:2] + terms[2:3]


def scan_near(inbox_ref, inner_ref, before_ref, group_ref, sent_ref):
    count, rows, _ = inner_ref.shape
    state = jnp.zeros((rows, STATE), F32)
    log = jnp.zeros((1, LANES), F32)
    for i in range(count):
        inner_ref[i] = state
        before_ref[8 * i : 8 * i + 8] = jnp.broadcast_to(log, (8, LANES))
        mine = from_terms(inbox_ref[i, rows:])
        state = jnp.exp(mine) * state + inbox_ref[i, :rows].astype(F32)
        log = log + mine
    before_ref[8 * count :] = jnp.broadcast_to(log, (8, LANES))
    group_ref[...] = state
    sent_ref[...] = state.astype(BF16)


def extend(inbox_ref, before_ref, group_ref, sent_ref):
    grown = jnp.exp(before_ref[before_ref.shape[0] - 1 :])
    sent_ref[...] = (grown * inbox_ref[...].astype(F32) + group_ref[...]).astype(BF16)


def scan_far(inner_ref, before_ref, *refs):
    starts_ref = refs[-1]
    state = refs[0][...].astype(F32)
    for ref in refs[1:-1]:
        state = state + ref[...].astype(F32)
    for i in range(inner_ref.shape[0]):
        grown = jnp.exp(before_ref[8 * i : 8 * i + 1])
        starts_ref[i] = (grown * state + inner_ref[i]).astype(BF16)


def local(
    xs_ref, b_ref, late_ref, halo_ref, group_taps_ref, dt_ref, cum_ref, held_ref, skip_ref,
    c_ref, y_ref, padded,
):
    tokens, cols = xs_ref.shape
    padded[:8] = halo_ref[:, cols + LANES : cols + 2 * LANES].astype(F32)
    padded[8:] = late_ref[:, :LANES].astype(F32)
    rows = lax.broadcasted_iota(jnp.int32, (SPAN, SPAN), 0)
    lanes = lax.broadcasted_iota(jnp.int32, (SPAN, SPAN), 1)
    causal = rows >= lanes
    left = left_half()
    taps = [group_taps_ref[8 + j : 9 + j] for j in range(4)]
    for k in range(tokens // SPAN):
        part = slice(k * SPAN, (k + 1) * SPAN)
        c = conv(padded, taps, group_taps_ref[12:13], k, 0)
        c_ref[part] = c
        scores = nt(c, b_ref[part])
        cum_t = cum_ref[:, part]
        dt_t = dt_ref[:, part]
        cum = columns(cum_t)
        grown = jnp.exp(cum)

        def mix(h):
            spread = cum[:, h : h + 1] - cum_t[h : h + 1]
            decays = jnp.exp(jnp.where(causal, spread, -jnp.inf))
            return (decays * dt_t[h : h + 1] * scores).astype(BF16)

        for chunk in range(cols // LANES):
            lo = chunk * LANES
            xs = xs_ref[part, lo : lo + LANES]
            y0 = jnp.dot(mix(2 * chunk), xs, preferred_element_type=F32)
            y1 = jnp.dot(mix(2 * chunk + 1), xs, preferred_element_type=F32)
            y = jnp.where(left, y0, y1) + by_head(skip_ref[...], chunk, left) * xs.astype(F32)
            if k > 0:
                y = y + nt(c, held_ref[k, lo : lo + LANES]) * by_head(grown, chunk, left)
            y_ref[part, lo : lo + LANES] = y


def finish(start_ref, c_ref, sum_ref, y_ref, late_ref, out_ref, *, ys):
    tokens, cols = y_ref.shape
    rows = tokens // 32
    half = out_ref.shape[1] // 2
    left = left_half()
    first = lax.axis_index("c") == 0
    for k in range(tokens // SPAN):
        part = slice(k * SPAN, (k + 1) * SPAN)
        grown = jnp.exp(columns(sum_ref[:, part]))
        for chunk in range(cols // LANES):
            lo = chunk * LANES
            carry = nt(c_ref[part], start_ref[lo : lo + LANES]) * by_head(grown, chunk, left)
            z = late_ref[part, LANES + lo : 2 * LANES + lo].astype(F32)
            gated = ((y_ref[part, lo : lo + LANES] + carry) * silu(z)).astype(BF16)
            for i in range(SPAN // (2 * rows)):
                even = gated[2 * i * rows : (2 * i + 1) * rows]
                odd = gated[(2 * i + 1) * rows : (2 * i + 2) * rows]
                theirs = jnp.where(first, odd, even)
                ours = jnp.where(first, even, odd)
                x, y = divmod(k * (SPAN // (2 * rows)) + i, ys)
                at = (x // 2 * ys + y) * rows
                for d in range(x % 2, out_ref.shape[0], 2):
                    out_ref[d, at : at + rows, lo : lo + LANES] = theirs
                    out_ref[d, half + at : half + at + rows, lo : lo + LANES] = ours


def join(mine_ref, other_ref, gain_ref, out_ref):
    rows = mine_ref.shape[0]
    mine = mine_ref[...].astype(F32) * gain_ref[...]
    other = other_ref[...].astype(F32) * gain_ref[...]
    even = lax.axis_index("xl") == 0
    out_ref[:rows] = jnp.where(even, mine, other).astype(BF16)
    out_ref[rows:] = jnp.where(even, other, mine).astype(BF16)


def project(gated_ref, weights_far, theirs_ref, ours_ref, weights_ref, wide_ref, sems):
    parts, rows, cols = gated_ref.shape
    half, width = ours_ref.shape
    step = width // sems.shape[0]
    loads = []
    for j in range(sems.shape[0]):
        span = pl.ds(j * step, step)
        loads.append(pltpu.make_async_copy(weights_far.at[span], weights_ref.at[span], sems.at[j]))
        loads[-1].start()
    squares = jnp.zeros((rows, 1), F32)
    for i in range(parts):
        wide_ref[:, i * cols : (i + 1) * cols] = gated_ref[i]
        value = gated_ref[i].astype(F32)
        squares = squares + jnp.sum(value * value, axis=1, keepdims=True)
    scale = 1.0 / jnp.sqrt(squares / weights_ref.shape[1] + 1.0)
    for j, load in enumerate(loads):
        lo = j * step
        load.wait()
        total = (nt(wide_ref[...], weights_ref[lo : lo + step]) * scale).astype(BF16)
        theirs_ref[:, lo : lo + step] = total[:half]
        ours_ref[:, lo : lo + step] = total[half:]


def add(ours_ref, other_ref, out_ref):
    out_ref[...] = (ours_ref[...].astype(F32) + other_ref[...].astype(F32)).astype(BF16)


def tail(array_ref, out_ref):
    out_ref[...] = array_ref[array_ref.shape[0] - out_ref.shape[0] :, : out_ref.shape[1]]


def collect(shares_ref, out_ref, *, ys):
    count, _, width = shares_ref.shape
    halves = count // ys
    for k in range(width // LANES):
        for i in range(halves):
            total = shares_ref[i * ys, :, k * LANES : (k + 1) * LANES].astype(F32)
            for j in range(1, ys):
                total = total + shares_ref[i * ys + j, :, k * LANES : (k + 1) * LANES].astype(F32)
            at = (k * halves + i) * LANES
            out_ref[:, at : at + LANES] = total.astype(BF16)


def shift(array, axis, by, wrap=True):
    count = lax.axis_size(axis)
    pairs = [(i, (i + by) % count) for i in range(count) if wrap or 0 <= i + by < count]
    return lax.ppermute(array, axis, pairs)


def sent(array, axes):
    return lax.all_to_all(array, axes, 0, 0, tiled=True)


def per_device(
    x_proj, z_proj, b_proj, c_proj, dt_raw, dt_bias, a_log, d_skip,
    conv_x, conv_bias_x, conv_bc, conv_bias_bc, norm_weight, out_weight,
):
    xh, xl, ys, cs = (lax.axis_size(a) for a in PLANE)
    xs = xh * xl
    zh, zl = (lax.axis_size(a) for a in Z)
    plane = xs * ys * cs
    rows, inner = x_proj.shape
    cols = inner // plane
    tokens = rows * plane
    part = lax.axis_index("xh") * xl + lax.axis_index("xl")
    heads = dt_bias.shape[0] // xs

    def own(values, axis):
        size = values.shape[axis] // xs
        return lax.dynamic_slice_in_dim(values, part * size, size, axis)

    mine = out_weight.T
    other = shift(mine, "xl", 1)
    pair = call(
        join,
        shape((2 * mine.shape[0], mine.shape[1]), BF16),
        (mine, other, norm_weight[None]),
    )
    weights = lax.all_gather(pair, Z, axis=0, tiled=True)
    out = call(
        pack,
        shape((plane, rows, 2 * cols + 3 * LANES), BF16),
        (x_proj, z_proj, b_proj, c_proj, dt_raw),
        [pltpu.VMEM(a.shape, BF16) for a in (x_proj, z_proj, b_proj, c_proj, dt_raw)]
        + [
            pltpu.VMEM((plane, rows, 2 * cols + 3 * LANES), BF16),
            pltpu.SemaphoreType.DMA((5,)),
            pltpu.SemaphoreType.DMA((plane,)),
        ],
        limit=60,
        far=range(5),
        far_out=True,
    )
    per_head = jnp.stack([own(dt_bias, 0), own(-jnp.exp(a_log), 0)], axis=1)
    per_head = jnp.pad(per_head, ((0, 8 - heads), (0, LANES - 2)))
    skip = jnp.pad(own(d_skip, 0), (0, LANES - heads))[None]
    taps = jnp.pad(jnp.concatenate([own(conv_x, 1), own(conv_bias_x, 0)[None]]), ((0, 3), (0, 0)))
    group_taps = jnp.pad(
        jnp.concatenate([jnp.moveaxis(conv_bc, 0, 1), conv_bias_bc[:, None]], axis=1),
        ((0, 0), (0, 3), (0, 0)),
    ).reshape(16, LANES)
    packed, per_head, skip, taps, group_taps = lax.optimization_barrier(
        (sent(out, PLANE), per_head, skip, taps, group_taps)
    )
    packed = packed.reshape(tokens, 2 * cols + 3 * LANES)
    halo = call(tail, shape((8, cols + 2 * LANES), BF16), (packed,), (), 1 << 16, 4)
    halo = shift(halo, Z, 1, wrap=False)
    by_token = shape((8, tokens), F32)
    late = shape((tokens, cols + LANES), BF16)
    dt, cum, sums, late = call(steps, (by_token, by_token, by_token, late), (packed, per_head))
    x_conv, b_conv, held, states_out = call(
        scan_in,
        (
            shape((tokens, cols), BF16),
            shape((tokens, LANES), BF16),
            shape((tokens // SPAN, cols, STATE), BF16),
            shape((zl, cols // zl + 8, STATE), BF16),
        ),
        (packed, halo, taps, group_taps, dt, cum, sums),
        [pltpu.VMEM((tokens + 8, cols + LANES), F32)],
        1 << 25,
    )
    c_conv, y = call(
        local,
        (shape((tokens, LANES), BF16), shape((tokens, cols), F32)),
        (x_conv, b_conv, late, halo, group_taps, dt, cum, held, skip),
        [pltpu.VMEM((tokens + 8, LANES), F32)],
        1 << 27,
    )
    near_in, c_conv, y = lax.optimization_barrier((sent(states_out, "zl"), c_conv, y))
    near = zl, cols // zl, STATE
    inner, before, group, ahead = call(
        scan_near,
        (
            shape(near, F32),
            shape((8 * zl + 8, LANES), F32),
            shape(near[1:], F32),
            shape(near[1:], BF16),
        ),
        (near_in,),
    )
    inboxes = []
    for hop in range(zh - 1):
        if hop:
            ahead = call(extend, shape(near[1:], BF16), (inboxes[-1], before, group))
        inboxes.append(lax.ppermute(ahead, "zh", [(hop, hop + 1)]))
    starts = call(scan_far, shape(near, BF16), (inner, before, *inboxes))
    start = sent(starts, "zl").reshape(cols, STATE)

    def finish_all(*refs):
        finish(*refs, ys=ys)

    def collect_all(*refs):
        collect(*refs, ys=ys)

    copies = call(
        finish_all,
        shape((xs, tokens // xl, cols), BF16),
        (start, c_conv, sums, y, late),
        (),
        1 << 25,
    )
    gated = sent(copies, X)
    count = tokens // (2 * xl)
    product = shape((count, weights.shape[0]), BF16)
    room = [
        pltpu.VMEM(weights.shape, BF16),
        pltpu.VMEM((2 * count, weights.shape[1]), BF16),
        pltpu.SemaphoreType.DMA((8,)),
    ]
    theirs, ours = call(project, (product, product), (gated, weights), room, 1 << 30, 50, (1,))
    both = call(add, product, (ours, shift(theirs, "c", 1)))
    shares = sent(both.reshape(xh * ys, rows, weights.shape[0]), ("xh", "y"))
    return call(collect_all, shape((rows, xh * weights.shape[0]), BF16), (shares,))


def solution(mesh):
    split = Mesh(mesh.devices.reshape(4, 4, 2, 2, 4, 2), ALL)
    return jax.shard_map(
        per_device,
        mesh=split,
        in_specs=(
            P(ALL, None),
            P(ALL, None),
            P(ALL, None),
            P(ALL, None),
            P(ALL, None),
            P(HEAD),
            P(HEAD),
            P(HEAD),
            P(None, HEAD),
            P(HEAD),
            P(None, None, HEAD),
            P(None, HEAD),
            P(HEAD),
            P(HEAD, SEQ),
        ),
        out_specs=P(ALL, None),
        check_vma=False,
    )
```

```python
import jax
import jax.numpy as jnp
from jax import lax
from jax.experimental import pallas as pl
from jax.experimental.pallas import tpu as pltpu
from jax.sharding import Mesh
from jax.sharding import PartitionSpec as P

HEAD_DIM = 64
STATE = 128
SPAN = 128
LANES = 128
F32 = jnp.float32
BF16 = jnp.bfloat16
Z = ("zh", "zl")
X = ("xh", "xl")
SEQ = ("zh", "zl", "xh", "xl")
HEAD = ("y", "c")
PLANE = ("xh", "xl", "y", "c")
ALL = ("zh", "zl", "xh", "xl", "y", "c")
VMEM = pl.BlockSpec(memory_space=pltpu.VMEM)
HBM = pl.BlockSpec(memory_space=pltpu.HBM)


def call(kernel, outs, inputs, scratch=(), flops=1 << 22, limit=16, far=(), far_out=False):
    return pl.pallas_call(
        kernel,
        out_shape=outs,
        in_specs=[HBM if i in far else VMEM for i in range(len(inputs))],
        out_specs=jax.tree.map(lambda _: HBM if far_out else VMEM, outs),
        scratch_shapes=list(scratch),
        compiler_params=pltpu.CompilerParams(vmem_limit_bytes=limit << 20),
        cost_estimate=pl.CostEstimate(flops=flops, bytes_accessed=1 << 20, transcendentals=0),
    )(*inputs)


def shape(dims, dtype):
    return jax.ShapeDtypeStruct(dims, dtype)


def silu(v):
    return v * (1.0 / (1.0 + jnp.exp(-v)))


def nt(a, b):
    return lax.dot_general(a, b, (((1,), (1,)), ((), ())), preferred_element_type=F32)


def tn(a, b):
    return lax.dot_general(a, b, (((0,), (0,)), ((), ())), preferred_element_type=F32)


def by_head(values, chunk, first):
    return jnp.where(first, values[:, 2 * chunk : 2 * chunk + 1], values[:, 2 * chunk + 1 : 2 * chunk + 2])


def left_half():
    return lax.broadcasted_iota(jnp.int32, (1, LANES), 1) < HEAD_DIM


def top_half():
    return lax.broadcasted_iota(jnp.int32, (LANES, 1), 0) < HEAD_DIM


def pack(
    x_far, z_far, b_far, c_far, dt_far, out_far,
    x_ref, z_ref, b_ref, c_ref, dt_ref, out_ref, in_sems, out_sems,
):
    pairs = ((dt_far, dt_ref), (b_far, b_ref), (c_far, c_ref), (x_far, x_ref), (z_far, z_ref))
    loads = [pltpu.make_async_copy(*pair, in_sems.at[i]) for i, pair in enumerate(pairs)]
    for load in loads:
        load.start()
    for load in loads:
        load.wait()
    count, _, width = out_ref.shape
    groups = b_ref.shape[1] // LANES
    parts = count // groups
    cols = x_ref.shape[1] // count
    heads = dt_ref.shape[1] // count
    dt = dt_ref[...].astype(F32)
    stores = [
        pltpu.make_async_copy(out_ref.at[d], out_far.at[d], out_sems.at[d]) for d in range(count)
    ]
    for d in range(count):
        part, group = divmod(d, groups)
        at = group * parts + part
        mine = dt if at == 0 else pltpu.roll(dt, LANES - at * heads, 1)
        side = slice(group * LANES, (group + 1) * LANES)
        out_ref[d, :, :cols] = x_ref[:, at * cols : (at + 1) * cols]
        out_ref[d, :, cols : cols + LANES] = b_ref[:, side]
        out_ref[d, :, cols + LANES : cols + 2 * LANES] = c_ref[:, side]
        out_ref[d, :, cols + 2 * LANES : width - LANES] = z_ref[:, at * cols : (at + 1) * cols]
        out_ref[d, :, width - LANES :] = mine.astype(BF16)
        if d > 0:
            stores[d - 1].start()
    stores[-1].start()
    for store in stores:
        store.wait()


def steps(packed_ref, heads_ref, dt_ref, cum_ref, sum_ref, c_ref, z_ref):
    rows, tokens = dt_ref.shape
    last = packed_ref.shape[1] - LANES
    first = last - z_ref.shape[1]
    c_ref[...] = packed_ref[:, first - LANES : first]
    z_ref[...] = packed_ref[:, first:last]
    before = lax.broadcasted_iota(jnp.int32, (SPAN, SPAN), 0)
    after = lax.broadcasted_iota(jnp.int32, (SPAN, SPAN), 1)
    ones = (before <= after).astype(F32)
    bias, coeff = heads_ref[:, 0:1], heads_ref[:, 1:2]
    total = jnp.zeros((rows, 1), F32)
    for k in range(tokens // SPAN):
        part = slice(k * SPAN, (k + 1) * SPAN)
        raw = packed_ref[part, packed_ref.shape[1] - LANES :].astype(F32).T[:rows] + bias
        dt = jnp.maximum(raw, 0.0) + jnp.log1p(jnp.exp(-jnp.abs(raw)))
        dt_ref[:, part] = dt
        cum = lax.dot(
            coeff * dt, ones, precision=lax.Precision.HIGHEST, preferred_element_type=F32
        )
        cum_ref[:, part] = cum
        sum_ref[:, part] = cum + total
        total = total + cum[:, SPAN - 1 :]


def columns(rows):
    filled = jnp.concatenate([rows, jnp.zeros((SPAN - rows.shape[0], SPAN), F32)])
    return filled.T


def fill_padded(padded, halo_ref, packed_ref, width):
    padded[:8] = halo_ref[:, :width].astype(F32)
    padded[8:] = packed_ref[:, :width].astype(F32)


def conv(padded, taps, bias, k, lo):
    first = 8 + k * SPAN - 3
    total = bias + taps[0] * padded[first : first + SPAN, lo : lo + LANES]
    for j in range(1, 4):
        total = total + taps[j] * padded[first + j : first + j + SPAN, lo : lo + LANES]
    return silu(total).astype(BF16)


def scan_in(
    packed_ref, halo_ref, taps_ref, group_taps_ref, dt_ref, cum_ref, sum_ref,
    xs_ref, b_ref, held_ref, sent_ref, padded,
):
    tokens, cols = xs_ref.shape
    blocks = tokens // SPAN
    fill_padded(padded, halo_ref, packed_ref, cols + LANES)
    left, top = left_half(), top_half()
    group_taps = [group_taps_ref[j : j + 1] for j in range(4)]
    states = [jnp.zeros((LANES, STATE), F32) for _ in range(cols // LANES)]
    for k in range(blocks):
        part = slice(k * SPAN, (k + 1) * SPAN)
        b = conv(padded, group_taps, group_taps_ref[4:5], k, cols)
        b_ref[part] = b
        cum = cum_ref[:, part]
        scale = columns(dt_ref[:, part] * jnp.exp(cum[:, SPAN - 1 :] - cum))
        decay = columns(jnp.broadcast_to(jnp.exp(cum[:, SPAN - 1 :]), cum.shape))
        for chunk in range(cols // LANES):
            lo = chunk * LANES
            taps = [taps_ref[j : j + 1, lo : lo + LANES] for j in range(4)]
            xs = conv(padded, taps, taps_ref[4:5, lo : lo + LANES], k, lo)
            xs_ref[part, lo : lo + LANES] = xs
            weighted = (xs.astype(F32) * by_head(scale, chunk, left)).astype(BF16)
            held_ref[k, lo : lo + LANES] = states[chunk].astype(BF16)
            states[chunk] = by_head(decay, chunk, top) * states[chunk] + tn(weighted, b)
    count = sent_ref.shape[0]
    rows = cols // count
    total = columns(jnp.broadcast_to(sum_ref[:, tokens - 1 :], (sum_ref.shape[0], SPAN)))[:1]
    for d in range(count):
        chunk, lo = divmod(d * rows, LANES)
        sent_ref[d, :rows] = states[chunk][lo : lo + rows].astype(BF16)
        sent_ref[d, rows:] = in_terms(total[:, d : d + 1])


def in_terms(value):
    high = value.astype(BF16).astype(F32)
    middle = (value - high).astype(BF16).astype(F32)
    low = value - high - middle
    at = lax.broadcasted_iota(jnp.int32, (8, LANES), 0)
    terms = jnp.where(at == 0, high, jnp.where(at == 1, middle, jnp.where(at == 2, low, 0.0)))
    return terms.astype(BF16)


def from_terms(terms):
    terms = terms.astype(F32)
    return terms[0:1] + terms[1:2] + terms[2:3]


def scan_near(inbox_ref, inner_ref, before_ref, group_ref, sent_ref):
    count, rows, _ = inner_ref.shape
    state = jnp.zeros((rows, STATE), F32)
    log = jnp.zeros((1, LANES), F32)
    for i in range(count):
        inner_ref[i] = state
        before_ref[8 * i : 8 * i + 8] = jnp.broadcast_to(log, (8, LANES))
        mine = from_terms(inbox_ref[i, rows:])
        state = jnp.exp(mine) * state + inbox_ref[i, :rows].astype(F32)
        log = log + mine
    before_ref[8 * count :] = jnp.broadcast_to(log, (8, LANES))
    group_ref[...] = state
    sent_ref[...] = state.astype(BF16)


def extend(inbox_ref, before_ref, group_ref, sent_ref):
    grown = jnp.exp(before_ref[before_ref.shape[0] - 1 :])
    sent_ref[...] = (grown * inbox_ref[...].astype(F32) + group_ref[...]).astype(BF16)


def scan_far(inner_ref, before_ref, *refs):
    starts_ref = refs[-1]
    state = refs[0][...].astype(F32)
    for ref in refs[1:-1]:
        state = state + ref[...].astype(F32)
    for i in range(inner_ref.shape[0]):
        grown = jnp.exp(before_ref[8 * i : 8 * i + 1])
        starts_ref[i] = (grown * state + inner_ref[i]).astype(BF16)


def local(
    xs_ref, b_ref, raw_ref, halo_ref, group_taps_ref, dt_ref, cum_ref, held_ref, skip_ref,
    c_ref, y_ref, padded,
):
    tokens, cols = xs_ref.shape
    padded[:8] = halo_ref[:, cols + LANES : cols + 2 * LANES].astype(F32)
    padded[8:] = raw_ref[...].astype(F32)
    rows = lax.broadcasted_iota(jnp.int32, (SPAN, SPAN), 0)
    lanes = lax.broadcasted_iota(jnp.int32, (SPAN, SPAN), 1)
    causal = rows >= lanes
    left = left_half()
    taps = [group_taps_ref[8 + j : 9 + j] for j in range(4)]
    for k in range(tokens // SPAN):
        part = slice(k * SPAN, (k + 1) * SPAN)
        c = conv(padded, taps, group_taps_ref[12:13], k, 0)
        c_ref[part] = c
        scores = nt(c, b_ref[part])
        cum_t = cum_ref[:, part]
        dt_t = dt_ref[:, part]
        cum = columns(cum_t)
        grown = jnp.exp(cum)

        def mix(h):
            spread = cum[:, h : h + 1] - cum_t[h : h + 1]
            decays = jnp.exp(jnp.where(causal, spread, -jnp.inf))
            return (decays * dt_t[h : h + 1] * scores).astype(BF16)

        for chunk in range(cols // LANES):
            lo = chunk * LANES
            xs = xs_ref[part, lo : lo + LANES]
            y0 = jnp.dot(mix(2 * chunk), xs, preferred_element_type=F32)
            y1 = jnp.dot(mix(2 * chunk + 1), xs, preferred_element_type=F32)
            y = jnp.where(left, y0, y1) + by_head(skip_ref[...], chunk, left) * xs.astype(F32)
            if k > 0:
                y = y + nt(c, held_ref[k, lo : lo + LANES]) * by_head(grown, chunk, left)
            y_ref[part, lo : lo + LANES] = y.astype(BF16)


def finish(start_ref, c_ref, sum_ref, y_ref, z_ref, out_ref, *, ys):
    tokens, cols = y_ref.shape
    rows = tokens // 32
    half = out_ref.shape[1] // 2
    left = left_half()
    first = lax.axis_index("c") == 0
    for k in range(tokens // SPAN):
        part = slice(k * SPAN, (k + 1) * SPAN)
        grown = jnp.exp(columns(sum_ref[:, part]))
        for chunk in range(cols // LANES):
            lo = chunk * LANES
            carry = nt(c_ref[part], start_ref[lo : lo + LANES]) * by_head(grown, chunk, left)
            z = z_ref[part, lo : lo + LANES].astype(F32)
            gated = ((y_ref[part, lo : lo + LANES].astype(F32) + carry) * silu(z)).astype(BF16)
            for i in range(SPAN // (2 * rows)):
                even = gated[2 * i * rows : (2 * i + 1) * rows]
                odd = gated[(2 * i + 1) * rows : (2 * i + 2) * rows]
                theirs = jnp.where(first, odd, even)
                ours = jnp.where(first, even, odd)
                x, y = divmod(k * (SPAN // (2 * rows)) + i, ys)
                at = (x // 2 * ys + y) * rows
                for d in range(x % 2, out_ref.shape[0], 2):
                    out_ref[d, at : at + rows, lo : lo + LANES] = theirs
                    out_ref[d, half + at : half + at + rows, lo : lo + LANES] = ours


def join(mine_ref, other_ref, gain_ref, out_ref):
    rows = mine_ref.shape[0]
    mine = mine_ref[...].astype(F32) * gain_ref[...]
    other = other_ref[...].astype(F32) * gain_ref[...]
    even = lax.axis_index("xl") == 0
    out_ref[:rows] = jnp.where(even, mine, other).astype(BF16)
    out_ref[rows:] = jnp.where(even, other, mine).astype(BF16)


def project(gated_ref, weights_far, theirs_ref, ours_ref, weights_ref, wide_ref, sems):
    parts, rows, cols = gated_ref.shape
    half, width = ours_ref.shape
    step = width // sems.shape[0]
    loads = []
    for j in range(sems.shape[0]):
        span = pl.ds(j * step, step)
        loads.append(pltpu.make_async_copy(weights_far.at[span], weights_ref.at[span], sems.at[j]))
        loads[-1].start()
    squares = jnp.zeros((rows, 1), F32)
    for i in range(parts):
        wide_ref[:, i * cols : (i + 1) * cols] = gated_ref[i]
        value = gated_ref[i].astype(F32)
        squares = squares + jnp.sum(value * value, axis=1, keepdims=True)
    scale = 1.0 / jnp.sqrt(squares / weights_ref.shape[1] + 1.0)
    for j, load in enumerate(loads):
        lo = j * step
        load.wait()
        total = (nt(wide_ref[...], weights_ref[lo : lo + step]) * scale).astype(BF16)
        theirs_ref[:, lo : lo + step] = total[:half]
        ours_ref[:, lo : lo + step] = total[half:]


def add(ours_ref, other_ref, out_ref):
    out_ref[...] = (ours_ref[...].astype(F32) + other_ref[...].astype(F32)).astype(BF16)


def tail(array_ref, out_ref):
    out_ref[...] = array_ref[array_ref.shape[0] - out_ref.shape[0] :, : out_ref.shape[1]]


def collect(shares_ref, out_ref, *, ys):
    count, _, width = shares_ref.shape
    halves = count // ys
    for k in range(width // LANES):
        for i in range(halves):
            total = shares_ref[i * ys, :, k * LANES : (k + 1) * LANES].astype(F32)
            for j in range(1, ys):
                total = total + shares_ref[i * ys + j, :, k * LANES : (k + 1) * LANES].astype(F32)
            at = (k * halves + i) * LANES
            out_ref[:, at : at + LANES] = total.astype(BF16)


def shift(array, axis, by, wrap=True):
    count = lax.axis_size(axis)
    pairs = [(i, (i + by) % count) for i in range(count) if wrap or 0 <= i + by < count]
    return lax.ppermute(array, axis, pairs)


def sent(array, axes):
    return lax.all_to_all(array, axes, 0, 0, tiled=True)


def per_device(
    x_proj, z_proj, b_proj, c_proj, dt_raw, dt_bias, a_log, d_skip,
    conv_x, conv_bias_x, conv_bc, conv_bias_bc, norm_weight, out_weight,
):
    xh, xl, ys, cs = (lax.axis_size(a) for a in PLANE)
    xs = xh * xl
    zh, zl = (lax.axis_size(a) for a in Z)
    plane = xs * ys * cs
    rows, inner = x_proj.shape
    cols = inner // plane
    tokens = rows * plane
    part = lax.axis_index("xh") * xl + lax.axis_index("xl")
    heads = dt_bias.shape[0] // xs

    def own(values, axis):
        size = values.shape[axis] // xs
        return lax.dynamic_slice_in_dim(values, part * size, size, axis)

    mine = out_weight.T
    other = shift(mine, "xl", 1)
    pair = call(
        join,
        shape((2 * mine.shape[0], mine.shape[1]), BF16),
        (mine, other, norm_weight[None]),
    )
    weights = lax.all_gather(pair, Z, axis=0, tiled=True)
    out = call(
        pack,
        shape((plane, rows, 2 * cols + 3 * LANES), BF16),
        (x_proj, z_proj, b_proj, c_proj, dt_raw),
        [pltpu.VMEM(a.shape, BF16) for a in (x_proj, z_proj, b_proj, c_proj, dt_raw)]
        + [
            pltpu.VMEM((plane, rows, 2 * cols + 3 * LANES), BF16),
            pltpu.SemaphoreType.DMA((5,)),
            pltpu.SemaphoreType.DMA((plane,)),
        ],
        limit=60,
        far=range(5),
        far_out=True,
    )
    per_head = jnp.stack([own(dt_bias, 0), own(-jnp.exp(a_log), 0)], axis=1)
    per_head = jnp.pad(per_head, ((0, 8 - heads), (0, LANES - 2)))
    skip = jnp.pad(own(d_skip, 0), (0, LANES - heads))[None]
    taps = jnp.pad(jnp.concatenate([own(conv_x, 1), own(conv_bias_x, 0)[None]]), ((0, 3), (0, 0)))
    group_taps = jnp.pad(
        jnp.concatenate([jnp.moveaxis(conv_bc, 0, 1), conv_bias_bc[:, None]], axis=1),
        ((0, 0), (0, 3), (0, 0)),
    ).reshape(16, LANES)
    packed, per_head, skip, taps, group_taps = lax.optimization_barrier(
        (sent(out, PLANE), per_head, skip, taps, group_taps)
    )
    packed = packed.reshape(tokens, 2 * cols + 3 * LANES)
    halo = call(tail, shape((8, cols + 2 * LANES), BF16), (packed,), (), 1 << 16, 4)
    halo = shift(halo, Z, 1, wrap=False)
    by_token = shape((8, tokens), F32)
    dt, cum, sums, c_raw, z_raw = call(
        steps,
        (by_token, by_token, by_token, shape((tokens, LANES), BF16), shape((tokens, cols), BF16)),
        (packed, per_head),
    )
    x_conv, b_conv, held, states_out = call(
        scan_in,
        (
            shape((tokens, cols), BF16),
            shape((tokens, LANES), BF16),
            shape((tokens // SPAN, cols, STATE), BF16),
            shape((zl, cols // zl + 8, STATE), BF16),
        ),
        (packed, halo, taps, group_taps, dt, cum, sums),
        [pltpu.VMEM((tokens + 8, cols + LANES), F32)],
        1 << 25,
    )
    c_conv, y = call(
        local,
        (shape((tokens, LANES), BF16), shape((tokens, cols), BF16)),
        (x_conv, b_conv, c_raw, halo, group_taps, dt, cum, held, skip),
        [pltpu.VMEM((tokens + 8, LANES), F32)],
        1 << 27,
    )
    near_in, c_conv, y = lax.optimization_barrier((sent(states_out, "zl"), c_conv, y))
    near = zl, cols // zl, STATE
    inner, before, group, ahead = call(
        scan_near,
        (
            shape(near, F32),
            shape((8 * zl + 8, LANES), F32),
            shape(near[1:], F32),
            shape(near[1:], BF16),
        ),
        (near_in,),
    )
    inboxes = []
    for hop in range(zh - 1):
        if hop:
            ahead = call(extend, shape(near[1:], BF16), (inboxes[-1], before, group))
        inboxes.append(lax.ppermute(ahead, "zh", [(hop, hop + 1)]))
    starts = call(scan_far, shape(near, BF16), (inner, before, *inboxes))
    start = sent(starts, "zl").reshape(cols, STATE)

    def finish_all(*refs):
        finish(*refs, ys=ys)

    def collect_all(*refs):
        collect(*refs, ys=ys)

    copies = call(
        finish_all,
        shape((xs, tokens // xl, cols), BF16),
        (start, c_conv, sums, y, z_raw),
        (),
        1 << 25,
    )
    gated = sent(copies, X)
    count = tokens // (2 * xl)
    product = shape((count, weights.shape[0]), BF16)
    room = [
        pltpu.VMEM(weights.shape, BF16),
        pltpu.VMEM((2 * count, weights.shape[1]), BF16),
        pltpu.SemaphoreType.DMA((4,)),
    ]
    theirs, ours = call(project, (product, product), (gated, weights), room, 1 << 30, 50, (1,))
    both = call(add, product, (ours, shift(theirs, "c", 1)))
    shares = sent(both.reshape(xh * ys, rows, weights.shape[0]), ("xh", "y"))
    return call(collect_all, shape((rows, xh * weights.shape[0]), BF16), (shares,))


def solution(mesh):
    split = Mesh(mesh.devices.reshape(4, 4, 2, 2, 4, 2), ALL)
    return jax.shard_map(
        per_device,
        mesh=split,
        in_specs=(
            P(ALL, None),
            P(ALL, None),
            P(ALL, None),
            P(ALL, None),
            P(ALL, None),
            P(HEAD),
            P(HEAD),
            P(HEAD),
            P(None, HEAD),
            P(HEAD),
            P(None, None, HEAD),
            P(None, HEAD),
            P(HEAD),
            P(HEAD, SEQ),
        ),
        out_specs=P(ALL, None),
        check_vma=False,
    )
```

```python
import jax
import jax.numpy as jnp
from jax import lax
from jax.experimental import pallas as pl
from jax.experimental.pallas import tpu as pltpu
from jax.sharding import Mesh
from jax.sharding import PartitionSpec as P

HEAD_DIM = 64
STATE = 128
SPAN = 128
LANES = 128
F32 = jnp.float32
BF16 = jnp.bfloat16
Z = ("zh", "zl")
X = ("xh", "xl")
SEQ = ("zh", "zl", "xh", "xl")
HEAD = ("y", "c")
PLANE = ("xh", "xl", "y", "c")
ALL = ("zh", "zl", "xh", "xl", "y", "c")
VMEM = pl.BlockSpec(memory_space=pltpu.VMEM)
HBM = pl.BlockSpec(memory_space=pltpu.HBM)


def call(kernel, outs, inputs, scratch=(), flops=1 << 22, limit=16, far=(), far_out=False):
    return pl.pallas_call(
        kernel,
        out_shape=outs,
        in_specs=[HBM if i in far else VMEM for i in range(len(inputs))],
        out_specs=jax.tree.map(lambda _: HBM if far_out else VMEM, outs),
        scratch_shapes=list(scratch),
        compiler_params=pltpu.CompilerParams(vmem_limit_bytes=limit << 20),
        cost_estimate=pl.CostEstimate(flops=flops, bytes_accessed=1 << 20, transcendentals=0),
    )(*inputs)


def shape(dims, dtype):
    return jax.ShapeDtypeStruct(dims, dtype)


def silu(v):
    return v * (1.0 / (1.0 + jnp.exp(-v)))


def nt(a, b):
    return lax.dot_general(a, b, (((1,), (1,)), ((), ())), preferred_element_type=F32)


def tn(a, b):
    return lax.dot_general(a, b, (((0,), (0,)), ((), ())), preferred_element_type=F32)


def by_head(values, chunk, first):
    return jnp.where(first, values[:, 2 * chunk : 2 * chunk + 1], values[:, 2 * chunk + 1 : 2 * chunk + 2])


def left_half():
    return lax.broadcasted_iota(jnp.int32, (1, LANES), 1) < HEAD_DIM


def top_half():
    return lax.broadcasted_iota(jnp.int32, (LANES, 1), 0) < HEAD_DIM


def pack(
    x_far, z_far, b_far, c_far, dt_far, out_far,
    x_ref, z_ref, b_ref, c_ref, dt_ref, out_ref, in_sems, out_sems,
):
    pairs = ((dt_far, dt_ref), (b_far, b_ref), (c_far, c_ref), (x_far, x_ref), (z_far, z_ref))
    loads = [pltpu.make_async_copy(*pair, in_sems.at[i]) for i, pair in enumerate(pairs)]
    for load in loads:
        load.start()
    for load in loads:
        load.wait()
    count, _, width = out_ref.shape
    groups = b_ref.shape[1] // LANES
    parts = count // groups
    cols = x_ref.shape[1] // count
    heads = dt_ref.shape[1] // count
    dt = dt_ref[...].astype(F32)
    stores = [
        pltpu.make_async_copy(out_ref.at[d], out_far.at[d], out_sems.at[d]) for d in range(count)
    ]
    for d in range(count):
        part, group = divmod(d, groups)
        at = group * parts + part
        mine = dt if at == 0 else pltpu.roll(dt, LANES - at * heads, 1)
        side = slice(group * LANES, (group + 1) * LANES)
        out_ref[d, :, :cols] = x_ref[:, at * cols : (at + 1) * cols]
        out_ref[d, :, cols : cols + LANES] = b_ref[:, side]
        out_ref[d, :, cols + LANES : cols + 2 * LANES] = c_ref[:, side]
        out_ref[d, :, cols + 2 * LANES : width - LANES] = z_ref[:, at * cols : (at + 1) * cols]
        out_ref[d, :, width - LANES :] = mine.astype(BF16)
        if d > 0:
            stores[d - 1].start()
    stores[-1].start()
    for store in stores:
        store.wait()


def steps(packed_ref, heads_ref, dt_ref, cum_ref, sum_ref, c_ref, z_ref):
    rows, tokens = dt_ref.shape
    last = packed_ref.shape[1] - LANES
    first = last - z_ref.shape[1]
    c_ref[...] = packed_ref[:, first - LANES : first]
    z_ref[...] = packed_ref[:, first:last]
    before = lax.broadcasted_iota(jnp.int32, (SPAN, SPAN), 0)
    after = lax.broadcasted_iota(jnp.int32, (SPAN, SPAN), 1)
    ones = (before <= after).astype(F32)
    bias, coeff = heads_ref[:, 0:1], heads_ref[:, 1:2]
    total = jnp.zeros((rows, 1), F32)
    for k in range(tokens // SPAN):
        part = slice(k * SPAN, (k + 1) * SPAN)
        raw = packed_ref[part, packed_ref.shape[1] - LANES :].astype(F32).T[:rows] + bias
        dt = jnp.maximum(raw, 0.0) + jnp.log1p(jnp.exp(-jnp.abs(raw)))
        dt_ref[:, part] = dt
        cum = lax.dot(
            coeff * dt, ones, precision=lax.Precision.HIGHEST, preferred_element_type=F32
        )
        cum_ref[:, part] = cum
        sum_ref[:, part] = cum + total
        total = total + cum[:, SPAN - 1 :]


def columns(rows):
    filled = jnp.concatenate([rows, jnp.zeros((SPAN - rows.shape[0], SPAN), F32)])
    return filled.T


def fill_padded(padded, halo_ref, packed_ref, width):
    padded[:8] = halo_ref[:, :width].astype(F32)
    padded[8:] = packed_ref[:, :width].astype(F32)


def conv(padded, taps, bias, k, lo):
    first = 8 + k * SPAN - 3
    total = bias + taps[0] * padded[first : first + SPAN, lo : lo + LANES]
    for j in range(1, 4):
        total = total + taps[j] * padded[first + j : first + j + SPAN, lo : lo + LANES]
    return silu(total).astype(BF16)


def scan_in(
    packed_ref, halo_ref, taps_ref, group_taps_ref, dt_ref, cum_ref, sum_ref,
    xs_ref, b_ref, held_ref, sent_ref, padded,
):
    tokens, cols = xs_ref.shape
    blocks = tokens // SPAN
    fill_padded(padded, halo_ref, packed_ref, cols + LANES)
    left, top = left_half(), top_half()
    group_taps = [group_taps_ref[j : j + 1] for j in range(4)]
    states = [jnp.zeros((LANES, STATE), F32) for _ in range(cols // LANES)]
    for k in range(blocks):
        part = slice(k * SPAN, (k + 1) * SPAN)
        b = conv(padded, group_taps, group_taps_ref[4:5], k, cols)
        b_ref[part] = b
        cum = cum_ref[:, part]
        scale = columns(dt_ref[:, part] * jnp.exp(cum[:, SPAN - 1 :] - cum))
        decay = columns(jnp.broadcast_to(jnp.exp(cum[:, SPAN - 1 :]), cum.shape))
        for chunk in range(cols // LANES):
            lo = chunk * LANES
            taps = [taps_ref[j : j + 1, lo : lo + LANES] for j in range(4)]
            xs = conv(padded, taps, taps_ref[4:5, lo : lo + LANES], k, lo)
            xs_ref[part, lo : lo + LANES] = xs
            weighted = (xs.astype(F32) * by_head(scale, chunk, left)).astype(BF16)
            held_ref[k, lo : lo + LANES] = states[chunk].astype(BF16)
            states[chunk] = by_head(decay, chunk, top) * states[chunk] + tn(weighted, b)
    count = sent_ref.shape[0]
    rows = cols // count
    total = columns(jnp.broadcast_to(sum_ref[:, tokens - 1 :], (sum_ref.shape[0], SPAN)))[:1]
    for d in range(count):
        chunk, lo = divmod(d * rows, LANES)
        sent_ref[d, :rows] = states[chunk][lo : lo + rows].astype(BF16)
        sent_ref[d, rows:] = in_terms(total[:, d : d + 1])


def in_terms(value):
    high = value.astype(BF16).astype(F32)
    middle = (value - high).astype(BF16).astype(F32)
    low = value - high - middle
    at = lax.broadcasted_iota(jnp.int32, (8, LANES), 0)
    terms = jnp.where(at == 0, high, jnp.where(at == 1, middle, jnp.where(at == 2, low, 0.0)))
    return terms.astype(BF16)


def from_terms(terms):
    terms = terms.astype(F32)
    return terms[0:1] + terms[1:2] + terms[2:3]


def scan_near(inbox_ref, inner_ref, before_ref, group_ref, sent_ref):
    count, rows, _ = inner_ref.shape
    state = jnp.zeros((rows, STATE), F32)
    log = jnp.zeros((1, LANES), F32)
    for i in range(count):
        inner_ref[i] = state
        before_ref[8 * i : 8 * i + 8] = jnp.broadcast_to(log, (8, LANES))
        mine = from_terms(inbox_ref[i, rows:])
        state = jnp.exp(mine) * state + inbox_ref[i, :rows].astype(F32)
        log = log + mine
    before_ref[8 * count :] = jnp.broadcast_to(log, (8, LANES))
    group_ref[...] = state
    sent_ref[:rows] = state.astype(BF16)
    sent_ref[rows:] = in_terms(log)


def extend(inbox_ref, before_ref, group_ref, sent_ref):
    grown = jnp.exp(before_ref[before_ref.shape[0] - 1 :])
    last = inbox_ref[: sent_ref.shape[0]].astype(F32)
    sent_ref[...] = (grown * last + group_ref[...]).astype(BF16)


def scan_far(last_ref, earlier_ref, inner_ref, before_ref, starts_ref):
    rows = earlier_ref.shape[0]
    grown = jnp.exp(from_terms(last_ref[rows:]))
    state = last_ref[:rows].astype(F32) + grown * earlier_ref[...].astype(F32)
    for i in range(inner_ref.shape[0]):
        grown = jnp.exp(before_ref[8 * i : 8 * i + 1])
        starts_ref[i] = (grown * state + inner_ref[i]).astype(BF16)


def local(
    xs_ref, b_ref, raw_ref, halo_ref, group_taps_ref, dt_ref, cum_ref, held_ref, skip_ref,
    c_ref, y_ref, padded,
):
    tokens, cols = xs_ref.shape
    padded[:8] = halo_ref[:, cols + LANES : cols + 2 * LANES].astype(F32)
    padded[8:] = raw_ref[...].astype(F32)
    rows = lax.broadcasted_iota(jnp.int32, (SPAN, SPAN), 0)
    lanes = lax.broadcasted_iota(jnp.int32, (SPAN, SPAN), 1)
    causal = rows >= lanes
    left = left_half()
    taps = [group_taps_ref[8 + j : 9 + j] for j in range(4)]
    for k in range(tokens // SPAN):
        part = slice(k * SPAN, (k + 1) * SPAN)
        c = conv(padded, taps, group_taps_ref[12:13], k, 0)
        c_ref[part] = c
        scores = nt(c, b_ref[part])
        cum_t = cum_ref[:, part]
        dt_t = dt_ref[:, part]
        cum = columns(cum_t)
        grown = jnp.exp(cum)

        def mix(h):
            spread = cum[:, h : h + 1] - cum_t[h : h + 1]
            decays = jnp.exp(jnp.where(causal, spread, -jnp.inf))
            return (decays * dt_t[h : h + 1] * scores).astype(BF16)

        for chunk in range(cols // LANES):
            lo = chunk * LANES
            xs = xs_ref[part, lo : lo + LANES]
            y0 = jnp.dot(mix(2 * chunk), xs, preferred_element_type=F32)
            y1 = jnp.dot(mix(2 * chunk + 1), xs, preferred_element_type=F32)
            y = jnp.where(left, y0, y1) + by_head(skip_ref[...], chunk, left) * xs.astype(F32)
            if k > 0:
                y = y + nt(c, held_ref[k, lo : lo + LANES]) * by_head(grown, chunk, left)
            y_ref[part, lo : lo + LANES] = y.astype(BF16)


def finish(start_ref, c_ref, sum_ref, y_ref, z_ref, out_ref, *, ys):
    tokens, cols = y_ref.shape
    rows = tokens // 32
    half = out_ref.shape[1] // 2
    left = left_half()
    first = lax.axis_index("c") == 0
    for k in range(tokens // SPAN):
        part = slice(k * SPAN, (k + 1) * SPAN)
        grown = jnp.exp(columns(sum_ref[:, part]))
        for chunk in range(cols // LANES):
            lo = chunk * LANES
            carry = nt(c_ref[part], start_ref[lo : lo + LANES]) * by_head(grown, chunk, left)
            z = z_ref[part, lo : lo + LANES].astype(F32)
            gated = ((y_ref[part, lo : lo + LANES].astype(F32) + carry) * silu(z)).astype(BF16)
            for i in range(SPAN // (2 * rows)):
                even = gated[2 * i * rows : (2 * i + 1) * rows]
                odd = gated[(2 * i + 1) * rows : (2 * i + 2) * rows]
                theirs = jnp.where(first, odd, even)
                ours = jnp.where(first, even, odd)
                x, y = divmod(k * (SPAN // (2 * rows)) + i, ys)
                at = (x // 2 * ys + y) * rows
                for d in range(x % 2, out_ref.shape[0], 2):
                    out_ref[d, at : at + rows, lo : lo + LANES] = theirs
                    out_ref[d, half + at : half + at + rows, lo : lo + LANES] = ours


def join(mine_ref, other_ref, gain_ref, out_ref):
    rows = mine_ref.shape[0]
    mine = mine_ref[...].astype(F32) * gain_ref[...]
    other = other_ref[...].astype(F32) * gain_ref[...]
    even = lax.axis_index("xl") == 0
    out_ref[:rows] = jnp.where(even, mine, other).astype(BF16)
    out_ref[rows:] = jnp.where(even, other, mine).astype(BF16)


def project(gated_ref, weights_far, theirs_ref, ours_ref, weights_ref, wide_ref, sems):
    parts, rows, cols = gated_ref.shape
    half, width = ours_ref.shape
    step = width // sems.shape[0]
    loads = []
    for j in range(sems.shape[0]):
        span = pl.ds(j * step, step)
        loads.append(pltpu.make_async_copy(weights_far.at[span], weights_ref.at[span], sems.at[j]))
        loads[-1].start()
    squares = jnp.zeros((rows, 1), F32)
    for i in range(parts):
        wide_ref[:, i * cols : (i + 1) * cols] = gated_ref[i]
        value = gated_ref[i].astype(F32)
        squares = squares + jnp.sum(value * value, axis=1, keepdims=True)
    scale = 1.0 / jnp.sqrt(squares / weights_ref.shape[1] + 1.0)
    for j, load in enumerate(loads):
        lo = j * step
        load.wait()
        total = (nt(wide_ref[...], weights_ref[lo : lo + step]) * scale).astype(BF16)
        theirs_ref[:, lo : lo + step] = total[:half]
        ours_ref[:, lo : lo + step] = total[half:]


def add(ours_ref, other_ref, out_ref):
    out_ref[...] = (ours_ref[...].astype(F32) + other_ref[...].astype(F32)).astype(BF16)


def tail(array_ref, out_ref):
    out_ref[...] = array_ref[array_ref.shape[0] - out_ref.shape[0] :, : out_ref.shape[1]]


def collect(shares_ref, out_ref, *, ys):
    count, _, width = shares_ref.shape
    halves = count // ys
    for k in range(width // LANES):
        for i in range(halves):
            total = shares_ref[i * ys, :, k * LANES : (k + 1) * LANES].astype(F32)
            for j in range(1, ys):
                total = total + shares_ref[i * ys + j, :, k * LANES : (k + 1) * LANES].astype(F32)
            at = (k * halves + i) * LANES
            out_ref[:, at : at + LANES] = total.astype(BF16)


def shift(array, axis, by, wrap=True):
    count = lax.axis_size(axis)
    pairs = [(i, (i + by) % count) for i in range(count) if wrap or 0 <= i + by < count]
    return lax.ppermute(array, axis, pairs)


def sent(array, axes):
    return lax.all_to_all(array, axes, 0, 0, tiled=True)


def per_device(
    x_proj, z_proj, b_proj, c_proj, dt_raw, dt_bias, a_log, d_skip,
    conv_x, conv_bias_x, conv_bc, conv_bias_bc, norm_weight, out_weight,
):
    xh, xl, ys, cs = (lax.axis_size(a) for a in PLANE)
    xs = xh * xl
    _, zl = (lax.axis_size(a) for a in Z)
    plane = xs * ys * cs
    rows, inner = x_proj.shape
    cols = inner // plane
    tokens = rows * plane
    part = lax.axis_index("xh") * xl + lax.axis_index("xl")
    heads = dt_bias.shape[0] // xs

    def own(values, axis):
        size = values.shape[axis] // xs
        return lax.dynamic_slice_in_dim(values, part * size, size, axis)

    mine = out_weight.T
    other = shift(mine, "xl", 1)
    pair = call(
        join,
        shape((2 * mine.shape[0], mine.shape[1]), BF16),
        (mine, other, norm_weight[None]),
    )
    weights = lax.all_gather(pair, Z, axis=0, tiled=True)
    out = call(
        pack,
        shape((plane, rows, 2 * cols + 3 * LANES), BF16),
        (x_proj, z_proj, b_proj, c_proj, dt_raw),
        [pltpu.VMEM(a.shape, BF16) for a in (x_proj, z_proj, b_proj, c_proj, dt_raw)]
        + [
            pltpu.VMEM((plane, rows, 2 * cols + 3 * LANES), BF16),
            pltpu.SemaphoreType.DMA((5,)),
            pltpu.SemaphoreType.DMA((plane,)),
        ],
        limit=60,
        far=range(5),
        far_out=True,
    )
    per_head = jnp.stack([own(dt_bias, 0), own(-jnp.exp(a_log), 0)], axis=1)
    per_head = jnp.pad(per_head, ((0, 8 - heads), (0, LANES - 2)))
    skip = jnp.pad(own(d_skip, 0), (0, LANES - heads))[None]
    taps = jnp.pad(jnp.concatenate([own(conv_x, 1), own(conv_bias_x, 0)[None]]), ((0, 3), (0, 0)))
    group_taps = jnp.pad(
        jnp.concatenate([jnp.moveaxis(conv_bc, 0, 1), conv_bias_bc[:, None]], axis=1),
        ((0, 0), (0, 3), (0, 0)),
    ).reshape(16, LANES)
    packed, per_head, skip, taps, group_taps = lax.optimization_barrier(
        (sent(out, PLANE), per_head, skip, taps, group_taps)
    )
    packed = packed.reshape(tokens, 2 * cols + 3 * LANES)
    halo = call(tail, shape((8, cols + 2 * LANES), BF16), (packed,), (), 1 << 16, 4)
    halo = shift(halo, Z, 1, wrap=False)
    by_token = shape((8, tokens), F32)
    dt, cum, sums, c_raw, z_raw = call(
        steps,
        (by_token, by_token, by_token, shape((tokens, LANES), BF16), shape((tokens, cols), BF16)),
        (packed, per_head),
    )
    x_conv, b_conv, held, states_out = call(
        scan_in,
        (
            shape((tokens, cols), BF16),
            shape((tokens, LANES), BF16),
            shape((tokens // SPAN, cols, STATE), BF16),
            shape((zl, cols // zl + 8, STATE), BF16),
        ),
        (packed, halo, taps, group_taps, dt, cum, sums),
        [pltpu.VMEM((tokens + 8, cols + LANES), F32)],
        1 << 25,
    )
    c_conv, y = call(
        local,
        (shape((tokens, LANES), BF16), shape((tokens, cols), BF16)),
        (x_conv, b_conv, c_raw, halo, group_taps, dt, cum, held, skip),
        [pltpu.VMEM((tokens + 8, LANES), F32)],
        1 << 27,
    )
    near_in, c_conv, y = lax.optimization_barrier((sent(states_out, "zl"), c_conv, y))
    near = zl, cols // zl, STATE
    inner, before, group, ahead = call(
        scan_near,
        (
            shape(near, F32),
            shape((8 * zl + 8, LANES), F32),
            shape(near[1:], F32),
            shape((near[1] + 8, STATE), BF16),
        ),
        (near_in,),
    )
    last = shift(ahead, "zh", 1, wrap=False)
    two = call(extend, shape(near[1:], BF16), (last, before, group))
    earlier = shift(two, "zh", 2, wrap=False)
    starts = call(scan_far, shape(near, BF16), (last, earlier, inner, before))
    start = sent(starts, "zl").reshape(cols, STATE)

    def finish_all(*refs):
        finish(*refs, ys=ys)

    def collect_all(*refs):
        collect(*refs, ys=ys)

    copies = call(
        finish_all,
        shape((xs, tokens // xl, cols), BF16),
        (start, c_conv, sums, y, z_raw),
        (),
        1 << 25,
    )
    gated = sent(copies, X)
    count = tokens // (2 * xl)
    product = shape((count, weights.shape[0]), BF16)
    room = [
        pltpu.VMEM(weights.shape, BF16),
        pltpu.VMEM((2 * count, weights.shape[1]), BF16),
        pltpu.SemaphoreType.DMA((4,)),
    ]
    theirs, ours = call(project, (product, product), (gated, weights), room, 1 << 30, 50, (1,))
    both = call(add, product, (ours, shift(theirs, "c", 1)))
    shares = sent(both.reshape(xh * ys, rows, weights.shape[0]), ("xh", "y"))
    return call(collect_all, shape((rows, xh * weights.shape[0]), BF16), (shares,))


def solution(mesh):
    split = Mesh(mesh.devices.reshape(4, 4, 2, 2, 4, 2), ALL)
    return jax.shard_map(
        per_device,
        mesh=split,
        in_specs=(
            P(ALL, None),
            P(ALL, None),
            P(ALL, None),
            P(ALL, None),
            P(ALL, None),
            P(HEAD),
            P(HEAD),
            P(HEAD),
            P(None, HEAD),
            P(HEAD),
            P(None, None, HEAD),
            P(None, HEAD),
            P(HEAD),
            P(HEAD, SEQ),
        ),
        out_specs=P(ALL, None),
        check_vma=False,
    )
```

```python
import jax
import jax.numpy as jnp
from jax import lax
from jax.experimental import pallas as pl
from jax.experimental.pallas import tpu as pltpu
from jax.sharding import Mesh
from jax.sharding import PartitionSpec as P

HEAD_DIM = 64
STATE = 128
SPAN = 128
LANES = 128
F32 = jnp.float32
BF16 = jnp.bfloat16
Z = ("zh", "zl")
X = ("xh", "xl")
SEQ = ("zh", "zl", "xh", "xl")
HEAD = ("y", "c")
PLANE = ("xh", "xl", "y", "c")
ALL = ("zh", "zl", "xh", "xl", "y", "c")
VMEM = pl.BlockSpec(memory_space=pltpu.VMEM)
HBM = pl.BlockSpec(memory_space=pltpu.HBM)


def call(kernel, outs, inputs, scratch=(), flops=1 << 22, limit=16, far=(), far_out=False):
    return pl.pallas_call(
        kernel,
        out_shape=outs,
        in_specs=[HBM if i in far else VMEM for i in range(len(inputs))],
        out_specs=jax.tree.map(lambda _: HBM if far_out else VMEM, outs),
        scratch_shapes=list(scratch),
        compiler_params=pltpu.CompilerParams(vmem_limit_bytes=limit << 20),
        cost_estimate=pl.CostEstimate(flops=flops, bytes_accessed=1 << 20, transcendentals=0),
    )(*inputs)


def shape(dims, dtype):
    return jax.ShapeDtypeStruct(dims, dtype)


def silu(v):
    return v * (1.0 / (1.0 + jnp.exp(-v)))


def nt(a, b):
    return lax.dot_general(a, b, (((1,), (1,)), ((), ())), preferred_element_type=F32)


def tn(a, b):
    return lax.dot_general(a, b, (((0,), (0,)), ((), ())), preferred_element_type=F32)


def by_head(values, chunk, first):
    return jnp.where(first, values[:, 2 * chunk : 2 * chunk + 1], values[:, 2 * chunk + 1 : 2 * chunk + 2])


def left_half():
    return lax.broadcasted_iota(jnp.int32, (1, LANES), 1) < HEAD_DIM


def top_half():
    return lax.broadcasted_iota(jnp.int32, (LANES, 1), 0) < HEAD_DIM


def pack(
    x_far, z_far, b_far, c_far, dt_far, out_far,
    x_ref, z_ref, b_ref, c_ref, dt_ref, out_ref, in_sems, out_sems,
):
    pairs = ((dt_far, dt_ref), (b_far, b_ref), (c_far, c_ref), (x_far, x_ref), (z_far, z_ref))
    loads = [pltpu.make_async_copy(*pair, in_sems.at[i]) for i, pair in enumerate(pairs)]
    for load in loads:
        load.start()
    for load in loads:
        load.wait()
    count = out_ref.shape[0]
    groups = b_ref.shape[1] // LANES
    parts = count // groups
    cols = x_ref.shape[1] // count
    heads = dt_ref.shape[1] // count
    tokens = dt_ref.shape[0]
    dt = jnp.concatenate([dt_ref[...].astype(F32), jnp.zeros((LANES - tokens, LANES), F32)]).T
    stores = [
        pltpu.make_async_copy(out_ref.at[d], out_far.at[d], out_sems.at[d]) for d in range(count)
    ]
    for d in range(count):
        part, group = divmod(d, groups)
        at = group * parts + part
        side = slice(group * LANES, (group + 1) * LANES)
        spans = [slice(at * cols + lo, at * cols + lo + LANES) for lo in range(0, cols, LANES)]
        pieces = [x_ref[:, span] for span in spans] + [b_ref[:, side], c_ref[:, side]]
        pieces += [z_ref[:, span] for span in spans]
        for i, piece in enumerate(pieces):
            out_ref[d, i * tokens : (i + 1) * tokens] = piece
        mine = dt[at * heads : (at + 1) * heads]
        mine = jnp.concatenate([mine, jnp.zeros((8 - heads, LANES), F32)])
        out_ref[d, len(pieces) * tokens :] = mine.astype(BF16)
        if d > 0:
            stores[d - 1].start()
    stores[-1].start()
    for store in stores:
        store.wait()


def piece_of(packed_ref, i, first, last):
    tokens = (packed_ref.shape[1] - 8) // 6
    sources = packed_ref[first // tokens : last // tokens, i * tokens : (i + 1) * tokens]
    return sources.reshape(last - first, LANES)


def steps(packed_ref, heads_ref, dt_ref, cum_ref, sum_ref, c_ref, z_ref):
    rows, tokens = dt_ref.shape
    own = (packed_ref.shape[1] - 8) // 6
    before = lax.broadcasted_iota(jnp.int32, (SPAN, SPAN), 0)
    after = lax.broadcasted_iota(jnp.int32, (SPAN, SPAN), 1)
    ones = (before <= after).astype(F32)
    bias, coeff = heads_ref[:, 0:1], heads_ref[:, 1:2]
    total = jnp.zeros((rows, 1), F32)
    for k in range(tokens // SPAN):
        part = slice(k * SPAN, (k + 1) * SPAN)
        c_ref[part] = piece_of(packed_ref, 3, k * SPAN, (k + 1) * SPAN)
        for i in range(2):
            z = piece_of(packed_ref, 4 + i, k * SPAN, (k + 1) * SPAN)
            z_ref[part, i * LANES : (i + 1) * LANES] = z
        first = k * SPAN // own
        raw = [packed_ref[first + i, 6 * own :, :own].astype(F32) for i in range(SPAN // own)]
        raw = jnp.concatenate(raw, axis=1) + bias
        dt = jnp.maximum(raw, 0.0) + jnp.log1p(jnp.exp(-jnp.abs(raw)))
        dt_ref[:, part] = dt
        cum = lax.dot(
            coeff * dt, ones, precision=lax.Precision.HIGHEST, preferred_element_type=F32
        )
        cum_ref[:, part] = cum
        sum_ref[:, part] = cum + total
        total = total + cum[:, SPAN - 1 :]


def columns(rows):
    filled = jnp.concatenate([rows, jnp.zeros((SPAN - rows.shape[0], SPAN), F32)])
    return filled.T


def conv(padded, taps, bias, k, lo):
    first = 8 + k * SPAN - 3
    total = bias + taps[0] * padded[first : first + SPAN, lo : lo + LANES]
    for j in range(1, 4):
        total = total + taps[j] * padded[first + j : first + j + SPAN, lo : lo + LANES]
    return silu(total).astype(BF16)


def scan_in(
    packed_ref, halo_ref, taps_ref, group_taps_ref, dt_ref, cum_ref, sum_ref,
    xs_ref, b_ref, held_ref, sent_ref, padded,
):
    tokens, cols = xs_ref.shape
    blocks = tokens // SPAN
    padded[:8] = halo_ref[:, : cols + LANES].astype(F32)
    for i in range(3):
        side = slice(i * LANES, (i + 1) * LANES)
        padded[8:, side] = piece_of(packed_ref, i, 0, tokens).astype(F32)
    left, top = left_half(), top_half()
    group_taps = [group_taps_ref[j : j + 1] for j in range(4)]
    states = [jnp.zeros((LANES, STATE), F32) for _ in range(cols // LANES)]
    for k in range(blocks):
        part = slice(k * SPAN, (k + 1) * SPAN)
        b = conv(padded, group_taps, group_taps_ref[4:5], k, cols)
        b_ref[part] = b
        cum = cum_ref[:, part]
        scale = columns(dt_ref[:, part] * jnp.exp(cum[:, SPAN - 1 :] - cum))
        decay = columns(jnp.broadcast_to(jnp.exp(cum[:, SPAN - 1 :]), cum.shape))
        for chunk in range(cols // LANES):
            lo = chunk * LANES
            taps = [taps_ref[j : j + 1, lo : lo + LANES] for j in range(4)]
            xs = conv(padded, taps, taps_ref[4:5, lo : lo + LANES], k, lo)
            xs_ref[part, lo : lo + LANES] = xs
            weighted = (xs.astype(F32) * by_head(scale, chunk, left)).astype(BF16)
            held_ref[k, lo : lo + LANES] = states[chunk].astype(BF16)
            states[chunk] = by_head(decay, chunk, top) * states[chunk] + tn(weighted, b)
    count = sent_ref.shape[0]
    rows = cols // count
    total = columns(jnp.broadcast_to(sum_ref[:, tokens - 1 :], (sum_ref.shape[0], SPAN)))[:1]
    for d in range(count):
        chunk, lo = divmod(d * rows, LANES)
        sent_ref[d, :rows] = states[chunk][lo : lo + rows].astype(BF16)
        sent_ref[d, rows:] = in_terms(total[:, d : d + 1])


def in_terms(value):
    high = value.astype(BF16).astype(F32)
    middle = (value - high).astype(BF16).astype(F32)
    low = value - high - middle
    at = lax.broadcasted_iota(jnp.int32, (8, LANES), 0)
    terms = jnp.where(at == 0, high, jnp.where(at == 1, middle, jnp.where(at == 2, low, 0.0)))
    return terms.astype(BF16)


def from_terms(terms):
    terms = terms.astype(F32)
    return terms[0:1] + terms[1:2] + terms[2:3]


def scan_near(inbox_ref, inner_ref, before_ref, group_ref, sent_ref):
    count, rows, _ = inner_ref.shape
    state = jnp.zeros((rows, STATE), F32)
    log = jnp.zeros((1, LANES), F32)
    for i in range(count):
        inner_ref[i] = state
        before_ref[8 * i : 8 * i + 8] = jnp.broadcast_to(log, (8, LANES))
        mine = from_terms(inbox_ref[i, rows:])
        state = jnp.exp(mine) * state + inbox_ref[i, :rows].astype(F32)
        log = log + mine
    before_ref[8 * count :] = jnp.broadcast_to(log, (8, LANES))
    group_ref[...] = state
    sent_ref[...] = state.astype(BF16)


def extend(inbox_ref, before_ref, group_ref, sent_ref):
    grown = jnp.exp(before_ref[before_ref.shape[0] - 1 :])
    sent_ref[...] = (grown * inbox_ref[...].astype(F32) + group_ref[...]).astype(BF16)


def scan_far(inner_ref, before_ref, *refs):
    starts_ref = refs[-1]
    state = refs[0][...].astype(F32)
    for ref in refs[1:-1]:
        state = state + ref[...].astype(F32)
    for i in range(inner_ref.shape[0]):
        grown = jnp.exp(before_ref[8 * i : 8 * i + 1])
        starts_ref[i] = (grown * state + inner_ref[i]).astype(BF16)


def local(
    xs_ref, b_ref, raw_ref, halo_ref, group_taps_ref, dt_ref, cum_ref, held_ref, skip_ref,
    c_ref, y_ref, padded,
):
    tokens, cols = xs_ref.shape
    padded[:8] = halo_ref[:, cols + LANES : cols + 2 * LANES].astype(F32)
    padded[8:] = raw_ref[...].astype(F32)
    rows = lax.broadcasted_iota(jnp.int32, (SPAN, SPAN), 0)
    lanes = lax.broadcasted_iota(jnp.int32, (SPAN, SPAN), 1)
    causal = rows >= lanes
    left = left_half()
    taps = [group_taps_ref[8 + j : 9 + j] for j in range(4)]
    for k in range(tokens // SPAN):
        part = slice(k * SPAN, (k + 1) * SPAN)
        c = conv(padded, taps, group_taps_ref[12:13], k, 0)
        c_ref[part] = c
        scores = nt(c, b_ref[part])
        cum_t = cum_ref[:, part]
        dt_t = dt_ref[:, part]
        cum = columns(cum_t)
        grown = jnp.exp(cum)

        def mix(h):
            spread = cum[:, h : h + 1] - cum_t[h : h + 1]
            decays = jnp.exp(jnp.where(causal, spread, -jnp.inf))
            return (decays * dt_t[h : h + 1] * scores).astype(BF16)

        for chunk in range(cols // LANES):
            lo = chunk * LANES
            xs = xs_ref[part, lo : lo + LANES]
            y0 = jnp.dot(mix(2 * chunk), xs, preferred_element_type=F32)
            y1 = jnp.dot(mix(2 * chunk + 1), xs, preferred_element_type=F32)
            y = jnp.where(left, y0, y1) + by_head(skip_ref[...], chunk, left) * xs.astype(F32)
            if k > 0:
                y = y + nt(c, held_ref[k, lo : lo + LANES]) * by_head(grown, chunk, left)
            y_ref[part, lo : lo + LANES] = y.astype(BF16)


def finish(start_ref, c_ref, sum_ref, y_ref, z_ref, out_ref, *, ys):
    tokens, cols = y_ref.shape
    rows = tokens // 32
    half = out_ref.shape[1] // 2
    left = left_half()
    first = lax.axis_index("c") == 0
    for k in range(tokens // SPAN):
        part = slice(k * SPAN, (k + 1) * SPAN)
        grown = jnp.exp(columns(sum_ref[:, part]))
        for chunk in range(cols // LANES):
            lo = chunk * LANES
            carry = nt(c_ref[part], start_ref[lo : lo + LANES]) * by_head(grown, chunk, left)
            z = z_ref[part, lo : lo + LANES].astype(F32)
            gated = ((y_ref[part, lo : lo + LANES].astype(F32) + carry) * silu(z)).astype(BF16)
            for i in range(SPAN // (2 * rows)):
                even = gated[2 * i * rows : (2 * i + 1) * rows]
                odd = gated[(2 * i + 1) * rows : (2 * i + 2) * rows]
                theirs = jnp.where(first, odd, even)
                ours = jnp.where(first, even, odd)
                x, y = divmod(k * (SPAN // (2 * rows)) + i, ys)
                at = (x // 2 * ys + y) * rows
                for d in range(x % 2, out_ref.shape[0], 2):
                    out_ref[d, at : at + rows, lo : lo + LANES] = theirs
                    out_ref[d, half + at : half + at + rows, lo : lo + LANES] = ours


def join(mine_ref, other_ref, gain_ref, out_ref):
    rows = mine_ref.shape[0]
    mine = mine_ref[...].astype(F32) * gain_ref[...]
    other = other_ref[...].astype(F32) * gain_ref[...]
    even = lax.axis_index("xl") == 0
    out_ref[:rows] = jnp.where(even, mine, other).astype(BF16)
    out_ref[rows:] = jnp.where(even, other, mine).astype(BF16)


def project(gated_ref, weights_far, theirs_ref, ours_ref, weights_ref, wide_ref, sems):
    parts, rows, cols = gated_ref.shape
    half, width = ours_ref.shape
    step = width // sems.shape[0]
    loads = []
    for j in range(sems.shape[0]):
        span = pl.ds(j * step, step)
        loads.append(pltpu.make_async_copy(weights_far.at[span], weights_ref.at[span], sems.at[j]))
        loads[-1].start()
    squares = jnp.zeros((rows, 1), F32)
    for i in range(parts):
        wide_ref[:, i * cols : (i + 1) * cols] = gated_ref[i]
        value = gated_ref[i].astype(F32)
        squares = squares + jnp.sum(value * value, axis=1, keepdims=True)
    scale = 1.0 / jnp.sqrt(squares / weights_ref.shape[1] + 1.0)
    for j, load in enumerate(loads):
        lo = j * step
        load.wait()
        total = (nt(wide_ref[...], weights_ref[lo : lo + step]) * scale).astype(BF16)
        theirs_ref[:, lo : lo + step] = total[:half]
        ours_ref[:, lo : lo + step] = total[half:]


def add(ours_ref, other_ref, out_ref):
    out_ref[...] = (ours_ref[...].astype(F32) + other_ref[...].astype(F32)).astype(BF16)


def tail(packed_ref, out_ref):
    own = (packed_ref.shape[1] - 8) // 6
    last = packed_ref.shape[0] - 1
    for i in range(out_ref.shape[1] // LANES):
        side = slice(i * LANES, (i + 1) * LANES)
        out_ref[:, side] = packed_ref[last, (i + 1) * own - 8 : (i + 1) * own]


def collect(shares_ref, out_ref, *, ys):
    count, _, width = shares_ref.shape
    halves = count // ys
    for k in range(width // LANES):
        for i in range(halves):
            total = shares_ref[i * ys, :, k * LANES : (k + 1) * LANES].astype(F32)
            for j in range(1, ys):
                total = total + shares_ref[i * ys + j, :, k * LANES : (k + 1) * LANES].astype(F32)
            at = (k * halves + i) * LANES
            out_ref[:, at : at + LANES] = total.astype(BF16)


def shift(array, axis, by, wrap=True):
    count = lax.axis_size(axis)
    pairs = [(i, (i + by) % count) for i in range(count) if wrap or 0 <= i + by < count]
    return lax.ppermute(array, axis, pairs)


def sent(array, axes):
    return lax.all_to_all(array, axes, 0, 0, tiled=True)


def per_device(
    x_proj, z_proj, b_proj, c_proj, dt_raw, dt_bias, a_log, d_skip,
    conv_x, conv_bias_x, conv_bc, conv_bias_bc, norm_weight, out_weight,
):
    xh, xl, ys, cs = (lax.axis_size(a) for a in PLANE)
    xs = xh * xl
    zh, zl = (lax.axis_size(a) for a in Z)
    plane = xs * ys * cs
    rows, inner = x_proj.shape
    cols = inner // plane
    tokens = rows * plane
    part = lax.axis_index("xh") * xl + lax.axis_index("xl")
    heads = dt_bias.shape[0] // xs

    def own(values, axis):
        size = values.shape[axis] // xs
        return lax.dynamic_slice_in_dim(values, part * size, size, axis)

    mine = out_weight.T
    other = shift(mine, "xl", 1)
    pair = call(
        join,
        shape((2 * mine.shape[0], mine.shape[1]), BF16),
        (mine, other, norm_weight[None]),
    )
    weights = lax.all_gather(pair, Z, axis=0, tiled=True)
    out = call(
        pack,
        shape((plane, 6 * rows + 8, LANES), BF16),
        (x_proj, z_proj, b_proj, c_proj, dt_raw),
        [pltpu.VMEM(a.shape, BF16) for a in (x_proj, z_proj, b_proj, c_proj, dt_raw)]
        + [
            pltpu.VMEM((plane, 6 * rows + 8, LANES), BF16),
            pltpu.SemaphoreType.DMA((5,)),
            pltpu.SemaphoreType.DMA((plane,)),
        ],
        limit=60,
        far=range(5),
        far_out=True,
    )
    per_head = jnp.stack([own(dt_bias, 0), own(-jnp.exp(a_log), 0)], axis=1)
    per_head = jnp.pad(per_head, ((0, 8 - heads), (0, LANES - 2)))
    skip = jnp.pad(own(d_skip, 0), (0, LANES - heads))[None]
    taps = jnp.pad(jnp.concatenate([own(conv_x, 1), own(conv_bias_x, 0)[None]]), ((0, 3), (0, 0)))
    group_taps = jnp.pad(
        jnp.concatenate([jnp.moveaxis(conv_bc, 0, 1), conv_bias_bc[:, None]], axis=1),
        ((0, 0), (0, 3), (0, 0)),
    ).reshape(16, LANES)
    packed, per_head, skip, taps, group_taps = lax.optimization_barrier(
        (sent(out, PLANE), per_head, skip, taps, group_taps)
    )
    halo = call(tail, shape((8, cols + 2 * LANES), BF16), (packed,), (), 1 << 16, 4)
    halo = shift(halo, Z, 1, wrap=False)
    by_token = shape((8, tokens), F32)
    dt, cum, sums, c_raw, z_raw = call(
        steps,
        (by_token, by_token, by_token, shape((tokens, LANES), BF16), shape((tokens, cols), BF16)),
        (packed, per_head),
    )
    x_conv, b_conv, held, states_out = call(
        scan_in,
        (
            shape((tokens, cols), BF16),
            shape((tokens, LANES), BF16),
            shape((tokens // SPAN, cols, STATE), BF16),
            shape((zl, cols // zl + 8, STATE), BF16),
        ),
        (packed, halo, taps, group_taps, dt, cum, sums),
        [pltpu.VMEM((tokens + 8, cols + LANES), F32)],
        1 << 25,
    )
    c_conv, y = call(
        local,
        (shape((tokens, LANES), BF16), shape((tokens, cols), BF16)),
        (x_conv, b_conv, c_raw, halo, group_taps, dt, cum, held, skip),
        [pltpu.VMEM((tokens + 8, LANES), F32)],
        1 << 27,
    )
    near_in, c_conv, y = lax.optimization_barrier((sent(states_out, "zl"), c_conv, y))
    near = zl, cols // zl, STATE
    inner, before, group, ahead = call(
        scan_near,
        (
            shape(near, F32),
            shape((8 * zl + 8, LANES), F32),
            shape(near[1:], F32),
            shape(near[1:], BF16),
        ),
        (near_in,),
    )
    inboxes = []
    for hop in range(zh - 1):
        if hop:
            ahead = call(extend, shape(near[1:], BF16), (inboxes[-1], before, group))
        inboxes.append(lax.ppermute(ahead, "zh", [(hop, hop + 1)]))
    starts = call(scan_far, shape(near, BF16), (inner, before, *inboxes))
    start = sent(starts, "zl").reshape(cols, STATE)

    def finish_all(*refs):
        finish(*refs, ys=ys)

    def collect_all(*refs):
        collect(*refs, ys=ys)

    copies = call(
        finish_all,
        shape((xs, tokens // xl, cols), BF16),
        (start, c_conv, sums, y, z_raw),
        (),
        1 << 25,
    )
    gated = sent(copies, X)
    count = tokens // (2 * xl)
    product = shape((count, weights.shape[0]), BF16)
    room = [
        pltpu.VMEM(weights.shape, BF16),
        pltpu.VMEM((2 * count, weights.shape[1]), BF16),
        pltpu.SemaphoreType.DMA((4,)),
    ]
    theirs, ours = call(project, (product, product), (gated, weights), room, 1 << 30, 50, (1,))
    both = call(add, product, (ours, shift(theirs, "c", 1)))
    shares = sent(both.reshape(xh * ys, rows, weights.shape[0]), ("xh", "y"))
    return call(collect_all, shape((rows, xh * weights.shape[0]), BF16), (shares,))


def solution(mesh):
    split = Mesh(mesh.devices.reshape(4, 4, 2, 2, 4, 2), ALL)
    return jax.shard_map(
        per_device,
        mesh=split,
        in_specs=(
            P(ALL, None),
            P(ALL, None),
            P(ALL, None),
            P(ALL, None),
            P(ALL, None),
            P(HEAD),
            P(HEAD),
            P(HEAD),
            P(None, HEAD),
            P(HEAD),
            P(None, None, HEAD),
            P(None, HEAD),
            P(HEAD),
            P(HEAD, SEQ),
        ),
        out_specs=P(ALL, None),
        check_vma=False,
    )
```

```python
import jax
import jax.numpy as jnp
from jax import lax
from jax.experimental import pallas as pl
from jax.experimental.pallas import tpu as pltpu
from jax.sharding import Mesh
from jax.sharding import PartitionSpec as P

HEAD_DIM = 64
STATE = 128
SPAN = 128
LANES = 128
F32 = jnp.float32
BF16 = jnp.bfloat16
Z = ("zh", "zl")
X = ("xh", "xl")
SEQ = ("zh", "zl", "xh", "xl")
HEAD = ("y", "c")
PLANE = ("xh", "xl", "y", "c")
ALL = ("zh", "zl", "xh", "xl", "y", "c")
VMEM = pl.BlockSpec(memory_space=pltpu.VMEM)
HBM = pl.BlockSpec(memory_space=pltpu.HBM)


def call(kernel, outs, inputs, scratch=(), flops=1 << 22, limit=16, far=(), far_out=False):
    return pl.pallas_call(
        kernel,
        out_shape=outs,
        in_specs=[HBM if i in far else VMEM for i in range(len(inputs))],
        out_specs=jax.tree.map(lambda _: HBM if far_out else VMEM, outs),
        scratch_shapes=list(scratch),
        compiler_params=pltpu.CompilerParams(vmem_limit_bytes=limit << 20),
        cost_estimate=pl.CostEstimate(flops=flops, bytes_accessed=1 << 20, transcendentals=0),
    )(*inputs)


def shape(dims, dtype):
    return jax.ShapeDtypeStruct(dims, dtype)


def silu(v):
    return v * (1.0 / (1.0 + jnp.exp(-v)))


def nt(a, b):
    return lax.dot_general(a, b, (((1,), (1,)), ((), ())), preferred_element_type=F32)


def tn(a, b):
    return lax.dot_general(a, b, (((0,), (0,)), ((), ())), preferred_element_type=F32)


def by_head(values, chunk, first):
    return jnp.where(first, values[:, 2 * chunk : 2 * chunk + 1], values[:, 2 * chunk + 1 : 2 * chunk + 2])


def left_half():
    return lax.broadcasted_iota(jnp.int32, (1, LANES), 1) < HEAD_DIM


def top_half():
    return lax.broadcasted_iota(jnp.int32, (LANES, 1), 0) < HEAD_DIM


def pack(
    x_far, z_far, b_far, c_far, dt_far, out_far,
    x_ref, z_ref, b_ref, c_ref, dt_ref, out_ref, in_sems, out_sems,
):
    pairs = ((dt_far, dt_ref), (b_far, b_ref), (c_far, c_ref), (x_far, x_ref), (z_far, z_ref))
    loads = [pltpu.make_async_copy(*pair, in_sems.at[i]) for i, pair in enumerate(pairs)]
    for load in loads:
        load.start()
    for load in loads:
        load.wait()
    count = out_ref.shape[0]
    groups = b_ref.shape[1] // LANES
    parts = count // groups
    cols = x_ref.shape[1] // count
    heads = dt_ref.shape[1] // count
    tokens = dt_ref.shape[0]
    dt = jnp.concatenate([dt_ref[...].astype(F32), jnp.zeros((LANES - tokens, LANES), F32)]).T
    stores = [
        pltpu.make_async_copy(out_ref.at[d], out_far.at[d], out_sems.at[d]) for d in range(count)
    ]
    for d in range(count):
        part, group = divmod(d, groups)
        at = group * parts + part
        side = slice(group * LANES, (group + 1) * LANES)
        spans = [slice(at * cols + lo, at * cols + lo + LANES) for lo in range(0, cols, LANES)]
        pieces = [x_ref[:, span] for span in spans] + [b_ref[:, side], c_ref[:, side]]
        pieces += [z_ref[:, span] for span in spans]
        for i, piece in enumerate(pieces):
            out_ref[d, i * tokens : (i + 1) * tokens] = piece
        mine = dt[at * heads : (at + 1) * heads]
        mine = jnp.concatenate([mine, jnp.zeros((8 - heads, LANES), F32)])
        out_ref[d, len(pieces) * tokens :] = mine.astype(BF16)
        if d > 0:
            stores[d - 1].start()
    stores[-1].start()
    for store in stores:
        store.wait()


def piece_of(packed_ref, i, first, last):
    tokens = (packed_ref.shape[1] - 8) // 6
    sources = packed_ref[first // tokens : last // tokens, i * tokens : (i + 1) * tokens]
    return sources.reshape(last - first, LANES)


def steps(packed_ref, heads_ref, dt_ref, cum_ref, sum_ref, c_ref, z_ref):
    rows, tokens = dt_ref.shape
    own = (packed_ref.shape[1] - 8) // 6
    before = lax.broadcasted_iota(jnp.int32, (SPAN, SPAN), 0)
    after = lax.broadcasted_iota(jnp.int32, (SPAN, SPAN), 1)
    ones = (before <= after).astype(F32)
    bias, coeff = heads_ref[:, 0:1], heads_ref[:, 1:2]
    total = jnp.zeros((rows, 1), F32)
    for k in range(tokens // SPAN):
        part = slice(k * SPAN, (k + 1) * SPAN)
        c_ref[part] = piece_of(packed_ref, 3, k * SPAN, (k + 1) * SPAN)
        for i in range(2):
            z = piece_of(packed_ref, 4 + i, k * SPAN, (k + 1) * SPAN)
            z_ref[part, i * LANES : (i + 1) * LANES] = z
        first = k * SPAN // own
        raw = [packed_ref[first + i, 6 * own :, :own].astype(F32) for i in range(SPAN // own)]
        raw = jnp.concatenate(raw, axis=1) + bias
        dt = jnp.maximum(raw, 0.0) + jnp.log1p(jnp.exp(-jnp.abs(raw)))
        dt_ref[:, part] = dt
        cum = lax.dot(
            coeff * dt, ones, precision=lax.Precision.HIGHEST, preferred_element_type=F32
        )
        cum_ref[:, part] = cum
        sum_ref[:, part] = cum + total
        total = total + cum[:, SPAN - 1 :]


def columns(rows):
    filled = jnp.concatenate([rows, jnp.zeros((SPAN - rows.shape[0], SPAN), F32)])
    return filled.T


def conv(padded, taps, bias, k, lo):
    first = 8 + k * SPAN - 3
    total = bias + taps[0] * padded[first : first + SPAN, lo : lo + LANES]
    for j in range(1, 4):
        total = total + taps[j] * padded[first + j : first + j + SPAN, lo : lo + LANES]
    return silu(total).astype(BF16)


def scan_in(
    packed_ref, halo_ref, taps_ref, group_taps_ref, dt_ref, cum_ref, sum_ref,
    xs_ref, b_ref, held_ref, sent_ref, padded,
):
    tokens, cols = xs_ref.shape
    blocks = tokens // SPAN
    padded[:8] = halo_ref[:, : cols + LANES].astype(F32)
    for i in range(3):
        side = slice(i * LANES, (i + 1) * LANES)
        padded[8:, side] = piece_of(packed_ref, i, 0, tokens).astype(F32)
    left, top = left_half(), top_half()
    group_taps = [group_taps_ref[j : j + 1] for j in range(4)]
    states = [jnp.zeros((LANES, STATE), F32) for _ in range(cols // LANES)]
    for k in range(blocks):
        part = slice(k * SPAN, (k + 1) * SPAN)
        b = conv(padded, group_taps, group_taps_ref[4:5], k, cols)
        b_ref[part] = b
        cum = cum_ref[:, part]
        scale = columns(dt_ref[:, part] * jnp.exp(cum[:, SPAN - 1 :] - cum))
        decay = columns(jnp.broadcast_to(jnp.exp(cum[:, SPAN - 1 :]), cum.shape))
        for chunk in range(cols // LANES):
            lo = chunk * LANES
            taps = [taps_ref[j : j + 1, lo : lo + LANES] for j in range(4)]
            xs = conv(padded, taps, taps_ref[4:5, lo : lo + LANES], k, lo)
            xs_ref[part, lo : lo + LANES] = xs
            weighted = (xs.astype(F32) * by_head(scale, chunk, left)).astype(BF16)
            held_ref[k, lo : lo + LANES] = states[chunk].astype(BF16)
            states[chunk] = by_head(decay, chunk, top) * states[chunk] + tn(weighted, b)
    count = sent_ref.shape[0]
    rows = cols // count
    total = columns(jnp.broadcast_to(sum_ref[:, tokens - 1 :], (sum_ref.shape[0], SPAN)))[:1]
    for d in range(count):
        chunk, lo = divmod(d * rows, LANES)
        sent_ref[d, :rows] = states[chunk][lo : lo + rows].astype(BF16)
        sent_ref[d, rows:] = in_terms(total[:, d : d + 1])


def in_terms(value):
    high = value.astype(BF16).astype(F32)
    middle = (value - high).astype(BF16).astype(F32)
    low = value - high - middle
    at = lax.broadcasted_iota(jnp.int32, (8, LANES), 0)
    terms = jnp.where(at == 0, high, jnp.where(at == 1, middle, jnp.where(at == 2, low, 0.0)))
    return terms.astype(BF16)


def from_terms(terms):
    terms = terms.astype(F32)
    return terms[0:1] + terms[1:2] + terms[2:3]


def scan_near(inbox_ref, inner_ref, before_ref, group_ref, sent_ref):
    count, rows, _ = inner_ref.shape
    state = jnp.zeros((rows, STATE), F32)
    log = jnp.zeros((1, LANES), F32)
    for i in range(count):
        inner_ref[i] = state
        before_ref[8 * i : 8 * i + 8] = jnp.broadcast_to(log, (8, LANES))
        mine = from_terms(inbox_ref[i, rows:])
        state = jnp.exp(mine) * state + inbox_ref[i, :rows].astype(F32)
        log = log + mine
    before_ref[8 * count :] = jnp.broadcast_to(log, (8, LANES))
    group_ref[...] = state
    sent_ref[:rows] = state.astype(BF16)
    sent_ref[rows:] = in_terms(log)


def extend(inbox_ref, before_ref, group_ref, sent_ref):
    grown = jnp.exp(before_ref[before_ref.shape[0] - 1 :])
    last = inbox_ref[: sent_ref.shape[0]].astype(F32)
    sent_ref[...] = (grown * last + group_ref[...]).astype(BF16)


def scan_far(last_ref, third_ref, second_ref, inner_ref, before_ref, starts_ref):
    rows = third_ref.shape[0]
    grown = jnp.exp(from_terms(last_ref[rows:]))
    earlier = third_ref[...].astype(F32) + second_ref[...].astype(F32)
    state = last_ref[:rows].astype(F32) + grown * earlier
    for i in range(inner_ref.shape[0]):
        grown = jnp.exp(before_ref[8 * i : 8 * i + 1])
        starts_ref[i] = (grown * state + inner_ref[i]).astype(BF16)


def local(
    xs_ref, b_ref, raw_ref, halo_ref, group_taps_ref, dt_ref, cum_ref, held_ref, skip_ref,
    c_ref, y_ref, padded,
):
    tokens, cols = xs_ref.shape
    padded[:8] = halo_ref[:, cols + LANES : cols + 2 * LANES].astype(F32)
    padded[8:] = raw_ref[...].astype(F32)
    rows = lax.broadcasted_iota(jnp.int32, (SPAN, SPAN), 0)
    lanes = lax.broadcasted_iota(jnp.int32, (SPAN, SPAN), 1)
    causal = rows >= lanes
    left = left_half()
    taps = [group_taps_ref[8 + j : 9 + j] for j in range(4)]
    for k in range(tokens // SPAN):
        part = slice(k * SPAN, (k + 1) * SPAN)
        c = conv(padded, taps, group_taps_ref[12:13], k, 0)
        c_ref[part] = c
        scores = nt(c, b_ref[part])
        cum_t = cum_ref[:, part]
        dt_t = dt_ref[:, part]
        cum = columns(cum_t)
        grown = jnp.exp(cum)

        def mix(h):
            spread = cum[:, h : h + 1] - cum_t[h : h + 1]
            decays = jnp.exp(jnp.where(causal, spread, -jnp.inf))
            return (decays * dt_t[h : h + 1] * scores).astype(BF16)

        for chunk in range(cols // LANES):
            lo = chunk * LANES
            xs = xs_ref[part, lo : lo + LANES]
            y0 = jnp.dot(mix(2 * chunk), xs, preferred_element_type=F32)
            y1 = jnp.dot(mix(2 * chunk + 1), xs, preferred_element_type=F32)
            y = jnp.where(left, y0, y1) + by_head(skip_ref[...], chunk, left) * xs.astype(F32)
            if k > 0:
                y = y + nt(c, held_ref[k, lo : lo + LANES]) * by_head(grown, chunk, left)
            y_ref[part, lo : lo + LANES] = y.astype(BF16)


def finish(start_ref, c_ref, sum_ref, y_ref, z_ref, out_ref, *, ys):
    tokens, cols = y_ref.shape
    rows = tokens // 32
    half = out_ref.shape[1] // 2
    left = left_half()
    first = lax.axis_index("c") == 0
    for k in range(tokens // SPAN):
        part = slice(k * SPAN, (k + 1) * SPAN)
        grown = jnp.exp(columns(sum_ref[:, part]))
        for chunk in range(cols // LANES):
            lo = chunk * LANES
            carry = nt(c_ref[part], start_ref[lo : lo + LANES]) * by_head(grown, chunk, left)
            z = z_ref[part, lo : lo + LANES].astype(F32)
            gated = ((y_ref[part, lo : lo + LANES].astype(F32) + carry) * silu(z)).astype(BF16)
            for i in range(SPAN // (2 * rows)):
                even = gated[2 * i * rows : (2 * i + 1) * rows]
                odd = gated[(2 * i + 1) * rows : (2 * i + 2) * rows]
                theirs = jnp.where(first, odd, even)
                ours = jnp.where(first, even, odd)
                x, y = divmod(k * (SPAN // (2 * rows)) + i, ys)
                at = (x // 2 * ys + y) * rows
                for d in range(x % 2, out_ref.shape[0], 2):
                    out_ref[d, at : at + rows, lo : lo + LANES] = theirs
                    out_ref[d, half + at : half + at + rows, lo : lo + LANES] = ours


def join(mine_ref, other_ref, gain_ref, out_ref):
    rows = mine_ref.shape[0]
    mine = mine_ref[...].astype(F32) * gain_ref[...]
    other = other_ref[...].astype(F32) * gain_ref[...]
    even = lax.axis_index("xl") == 0
    out_ref[:rows] = jnp.where(even, mine, other).astype(BF16)
    out_ref[rows:] = jnp.where(even, other, mine).astype(BF16)


def project(gated_ref, weights_far, theirs_ref, ours_ref, weights_ref, wide_ref, sems):
    parts, rows, cols = gated_ref.shape
    half, width = ours_ref.shape
    step = width // sems.shape[0]
    loads = []
    for j in range(sems.shape[0]):
        span = pl.ds(j * step, step)
        loads.append(pltpu.make_async_copy(weights_far.at[span], weights_ref.at[span], sems.at[j]))
        loads[-1].start()
    squares = jnp.zeros((rows, 1), F32)
    for i in range(parts):
        wide_ref[:, i * cols : (i + 1) * cols] = gated_ref[i]
        value = gated_ref[i].astype(F32)
        squares = squares + jnp.sum(value * value, axis=1, keepdims=True)
    scale = 1.0 / jnp.sqrt(squares / weights_ref.shape[1] + 1.0)
    for j, load in enumerate(loads):
        lo = j * step
        load.wait()
        total = (nt(wide_ref[...], weights_ref[lo : lo + step]) * scale).astype(BF16)
        theirs_ref[:, lo : lo + step] = total[:half]
        ours_ref[:, lo : lo + step] = total[half:]


def add(ours_ref, other_ref, out_ref):
    out_ref[...] = (ours_ref[...].astype(F32) + other_ref[...].astype(F32)).astype(BF16)


def tail(packed_ref, out_ref):
    own = (packed_ref.shape[1] - 8) // 6
    last = packed_ref.shape[0] - 1
    for i in range(out_ref.shape[1] // LANES):
        side = slice(i * LANES, (i + 1) * LANES)
        out_ref[:, side] = packed_ref[last, (i + 1) * own - 8 : (i + 1) * own]


def collect(shares_ref, out_ref, *, ys):
    count, _, width = shares_ref.shape
    halves = count // ys
    for k in range(width // LANES):
        for i in range(halves):
            total = shares_ref[i * ys, :, k * LANES : (k + 1) * LANES].astype(F32)
            for j in range(1, ys):
                total = total + shares_ref[i * ys + j, :, k * LANES : (k + 1) * LANES].astype(F32)
            at = (k * halves + i) * LANES
            out_ref[:, at : at + LANES] = total.astype(BF16)


def shift(array, axis, by, wrap=True):
    count = lax.axis_size(axis)
    pairs = [(i, (i + by) % count) for i in range(count) if wrap or 0 <= i + by < count]
    return lax.ppermute(array, axis, pairs)


def sent(array, axes):
    return lax.all_to_all(array, axes, 0, 0, tiled=True)


def per_device(
    x_proj, z_proj, b_proj, c_proj, dt_raw, dt_bias, a_log, d_skip,
    conv_x, conv_bias_x, conv_bc, conv_bias_bc, norm_weight, out_weight,
):
    xh, xl, ys, cs = (lax.axis_size(a) for a in PLANE)
    xs = xh * xl
    _, zl = (lax.axis_size(a) for a in Z)
    plane = xs * ys * cs
    rows, inner = x_proj.shape
    cols = inner // plane
    tokens = rows * plane
    part = lax.axis_index("xh") * xl + lax.axis_index("xl")
    heads = dt_bias.shape[0] // xs

    def own(values, axis):
        size = values.shape[axis] // xs
        return lax.dynamic_slice_in_dim(values, part * size, size, axis)

    mine = out_weight.T
    other = shift(mine, "xl", 1)
    pair = call(
        join,
        shape((2 * mine.shape[0], mine.shape[1]), BF16),
        (mine, other, norm_weight[None]),
    )
    weights = lax.all_gather(pair, Z, axis=0, tiled=True)
    out = call(
        pack,
        shape((plane, 6 * rows + 8, LANES), BF16),
        (x_proj, z_proj, b_proj, c_proj, dt_raw),
        [pltpu.VMEM(a.shape, BF16) for a in (x_proj, z_proj, b_proj, c_proj, dt_raw)]
        + [
            pltpu.VMEM((plane, 6 * rows + 8, LANES), BF16),
            pltpu.SemaphoreType.DMA((5,)),
            pltpu.SemaphoreType.DMA((plane,)),
        ],
        limit=60,
        far=range(5),
        far_out=True,
    )
    per_head = jnp.stack([own(dt_bias, 0), own(-jnp.exp(a_log), 0)], axis=1)
    per_head = jnp.pad(per_head, ((0, 8 - heads), (0, LANES - 2)))
    skip = jnp.pad(own(d_skip, 0), (0, LANES - heads))[None]
    taps = jnp.pad(jnp.concatenate([own(conv_x, 1), own(conv_bias_x, 0)[None]]), ((0, 3), (0, 0)))
    group_taps = jnp.pad(
        jnp.concatenate([jnp.moveaxis(conv_bc, 0, 1), conv_bias_bc[:, None]], axis=1),
        ((0, 0), (0, 3), (0, 0)),
    ).reshape(16, LANES)
    packed, per_head, skip, taps, group_taps = lax.optimization_barrier(
        (sent(out, PLANE), per_head, skip, taps, group_taps)
    )
    halo = call(tail, shape((8, cols + 2 * LANES), BF16), (packed,), (), 1 << 16, 4)
    halo = shift(halo, Z, 1, wrap=False)
    by_token = shape((8, tokens), F32)
    dt, cum, sums, c_raw, z_raw = call(
        steps,
        (by_token, by_token, by_token, shape((tokens, LANES), BF16), shape((tokens, cols), BF16)),
        (packed, per_head),
    )
    x_conv, b_conv, held, states_out = call(
        scan_in,
        (
            shape((tokens, cols), BF16),
            shape((tokens, LANES), BF16),
            shape((tokens // SPAN, cols, STATE), BF16),
            shape((zl, cols // zl + 8, STATE), BF16),
        ),
        (packed, halo, taps, group_taps, dt, cum, sums),
        [pltpu.VMEM((tokens + 8, cols + LANES), F32)],
        1 << 25,
    )
    c_conv, y = call(
        local,
        (shape((tokens, LANES), BF16), shape((tokens, cols), BF16)),
        (x_conv, b_conv, c_raw, halo, group_taps, dt, cum, held, skip),
        [pltpu.VMEM((tokens + 8, LANES), F32)],
        1 << 27,
    )
    near_in, c_conv, y = lax.optimization_barrier((sent(states_out, "zl"), c_conv, y))
    near = zl, cols // zl, STATE
    inner, before, group, ahead = call(
        scan_near,
        (
            shape(near, F32),
            shape((8 * zl + 8, LANES), F32),
            shape(near[1:], F32),
            shape((near[1] + 8, STATE), BF16),
        ),
        (near_in,),
    )
    last = lax.ppermute(ahead, "zh", [(0, 1), (2, 3)])
    two = call(extend, shape(near[1:], BF16), (last, before, group))
    third = lax.ppermute(two, "zh", [(1, 3)])
    second = lax.ppermute(two, "zh", [(1, 2)])
    starts = call(scan_far, shape(near, BF16), (last, third, second, inner, before))
    start = sent(starts, "zl").reshape(cols, STATE)

    def finish_all(*refs):
        finish(*refs, ys=ys)

    def collect_all(*refs):
        collect(*refs, ys=ys)

    copies = call(
        finish_all,
        shape((xs, tokens // xl, cols), BF16),
        (start, c_conv, sums, y, z_raw),
        (),
        1 << 25,
    )
    gated = sent(copies, X)
    count = tokens // (2 * xl)
    product = shape((count, weights.shape[0]), BF16)
    room = [
        pltpu.VMEM(weights.shape, BF16),
        pltpu.VMEM((2 * count, weights.shape[1]), BF16),
        pltpu.SemaphoreType.DMA((4,)),
    ]
    theirs, ours = call(project, (product, product), (gated, weights), room, 1 << 30, 50, (1,))
    both = call(add, product, (ours, shift(theirs, "c", 1)))
    shares = sent(both.reshape(xh * ys, rows, weights.shape[0]), ("xh", "y"))
    return call(collect_all, shape((rows, xh * weights.shape[0]), BF16), (shares,))


def solution(mesh):
    split = Mesh(mesh.devices.reshape(4, 4, 2, 2, 4, 2), ALL)
    return jax.shard_map(
        per_device,
        mesh=split,
        in_specs=(
            P(ALL, None),
            P(ALL, None),
            P(ALL, None),
            P(ALL, None),
            P(ALL, None),
            P(HEAD),
            P(HEAD),
            P(HEAD),
            P(None, HEAD),
            P(HEAD),
            P(None, None, HEAD),
            P(None, HEAD),
            P(HEAD),
            P(HEAD, SEQ),
        ),
        out_specs=P(ALL, None),
        check_vma=False,
    )
```

```python
import jax
import jax.numpy as jnp
from jax import lax
from jax.experimental import pallas as pl
from jax.experimental.pallas import tpu as pltpu
from jax.sharding import Mesh
from jax.sharding import PartitionSpec as P

HEAD_DIM = 64
STATE = 128
SPAN = 128
LANES = 128
F32 = jnp.float32
BF16 = jnp.bfloat16
Z = ("zh", "zl")
X = ("xh", "xl")
SEQ = ("zh", "zl", "xh", "xl")
HEAD = ("y", "c")
PLANE = ("xh", "xl", "y", "c")
ALL = ("zh", "zl", "xh", "xl", "y", "c")
VMEM = pl.BlockSpec(memory_space=pltpu.VMEM)
HBM = pl.BlockSpec(memory_space=pltpu.HBM)


def call(kernel, outs, inputs, scratch=(), flops=1 << 22, limit=16, far=(), far_out=False):
    return pl.pallas_call(
        kernel,
        out_shape=outs,
        in_specs=[HBM if i in far else VMEM for i in range(len(inputs))],
        out_specs=jax.tree.map(lambda _: HBM if far_out else VMEM, outs),
        scratch_shapes=list(scratch),
        compiler_params=pltpu.CompilerParams(vmem_limit_bytes=limit << 20),
        cost_estimate=pl.CostEstimate(flops=flops, bytes_accessed=1 << 20, transcendentals=0),
    )(*inputs)


def shape(dims, dtype):
    return jax.ShapeDtypeStruct(dims, dtype)


def silu(v):
    return v * (1.0 / (1.0 + jnp.exp(-v)))


def nt(a, b):
    return lax.dot_general(a, b, (((1,), (1,)), ((), ())), preferred_element_type=F32)


def tn(a, b):
    return lax.dot_general(a, b, (((0,), (0,)), ((), ())), preferred_element_type=F32)


def by_head(values, chunk, first):
    return jnp.where(first, values[:, 2 * chunk : 2 * chunk + 1], values[:, 2 * chunk + 1 : 2 * chunk + 2])


def left_half():
    return lax.broadcasted_iota(jnp.int32, (1, LANES), 1) < HEAD_DIM


def top_half():
    return lax.broadcasted_iota(jnp.int32, (LANES, 1), 0) < HEAD_DIM


def pack(
    x_far, z_far, b_far, c_far, dt_far, out_far,
    x_ref, z_ref, b_ref, c_ref, dt_ref, out_ref, in_sems, out_sems,
):
    pairs = ((dt_far, dt_ref), (b_far, b_ref), (c_far, c_ref), (x_far, x_ref), (z_far, z_ref))
    loads = [pltpu.make_async_copy(*pair, in_sems.at[i]) for i, pair in enumerate(pairs)]
    for load in loads:
        load.start()
    for load in loads:
        load.wait()
    count = out_ref.shape[0]
    groups = b_ref.shape[1] // LANES
    parts = count // groups
    cols = x_ref.shape[1] // count
    heads = dt_ref.shape[1] // count
    tokens = dt_ref.shape[0]
    dt = jnp.concatenate([dt_ref[...].astype(F32), jnp.zeros((LANES - tokens, LANES), F32)]).T
    stores = [
        pltpu.make_async_copy(out_ref.at[d], out_far.at[d], out_sems.at[d]) for d in range(count)
    ]
    for d in range(count):
        part, group = divmod(d, groups)
        at = group * parts + part
        side = slice(group * LANES, (group + 1) * LANES)
        spans = [slice(at * cols + lo, at * cols + lo + LANES) for lo in range(0, cols, LANES)]
        pieces = [x_ref[:, span] for span in spans] + [b_ref[:, side], c_ref[:, side]]
        pieces += [z_ref[:, span] for span in spans]
        for i, piece in enumerate(pieces):
            out_ref[d, i * tokens : (i + 1) * tokens] = piece
        mine = dt[at * heads : (at + 1) * heads]
        mine = jnp.concatenate([mine, jnp.zeros((8 - heads, LANES), F32)])
        out_ref[d, len(pieces) * tokens :] = mine.astype(BF16)
        if d > 0:
            stores[d - 1].start()
    stores[-1].start()
    for store in stores:
        store.wait()


def piece_of(packed_ref, i, first, last):
    tokens = (packed_ref.shape[1] - 8) // 6
    sources = packed_ref[first // tokens : last // tokens, i * tokens : (i + 1) * tokens]
    return sources.reshape(last - first, LANES)


def steps(packed_ref, heads_ref, dt_ref, cum_ref, sum_ref, c_ref, z_ref):
    rows, tokens = dt_ref.shape
    own = (packed_ref.shape[1] - 8) // 6
    before = lax.broadcasted_iota(jnp.int32, (SPAN, SPAN), 0)
    after = lax.broadcasted_iota(jnp.int32, (SPAN, SPAN), 1)
    ones = (before <= after).astype(F32)
    bias, coeff = heads_ref[:, 0:1], heads_ref[:, 1:2]
    total = jnp.zeros((rows, 1), F32)
    for k in range(tokens // SPAN):
        part = slice(k * SPAN, (k + 1) * SPAN)
        c_ref[part] = piece_of(packed_ref, 3, k * SPAN, (k + 1) * SPAN)
        for i in range(2):
            z = piece_of(packed_ref, 4 + i, k * SPAN, (k + 1) * SPAN)
            z_ref[part, i * LANES : (i + 1) * LANES] = z
        first = k * SPAN // own
        raw = [packed_ref[first + i, 6 * own :, :own].astype(F32) for i in range(SPAN // own)]
        raw = jnp.concatenate(raw, axis=1) + bias
        dt = jnp.maximum(raw, 0.0) + jnp.log1p(jnp.exp(-jnp.abs(raw)))
        dt_ref[:, part] = dt
        cum = lax.dot(
            coeff * dt, ones, precision=lax.Precision.HIGHEST, preferred_element_type=F32
        )
        cum_ref[:, part] = cum
        sum_ref[:, part] = cum + total
        total = total + cum[:, SPAN - 1 :]


def columns(rows):
    filled = jnp.concatenate([rows, jnp.zeros((SPAN - rows.shape[0], SPAN), F32)])
    return filled.T


def conv(padded, taps, bias, k, lo):
    first = 8 + k * SPAN - 3
    total = bias + taps[0] * padded[first : first + SPAN, lo : lo + LANES]
    for j in range(1, 4):
        total = total + taps[j] * padded[first + j : first + j + SPAN, lo : lo + LANES]
    return silu(total).astype(BF16)


def scan_in(
    packed_ref, halo_ref, taps_ref, group_taps_ref, dt_ref, cum_ref, sum_ref,
    xs_ref, b_ref, held_ref, sent_ref, padded,
):
    tokens, cols = xs_ref.shape
    blocks = tokens // SPAN
    padded[:8] = halo_ref[:, : cols + LANES].astype(F32)
    for i in range(3):
        side = slice(i * LANES, (i + 1) * LANES)
        padded[8:, side] = piece_of(packed_ref, i, 0, tokens).astype(F32)
    left, top = left_half(), top_half()
    group_taps = [group_taps_ref[j : j + 1] for j in range(4)]
    states = [jnp.zeros((LANES, STATE), F32) for _ in range(cols // LANES)]
    for k in range(blocks):
        part = slice(k * SPAN, (k + 1) * SPAN)
        b = conv(padded, group_taps, group_taps_ref[4:5], k, cols)
        b_ref[part] = b
        cum = cum_ref[:, part]
        scale = columns(dt_ref[:, part] * jnp.exp(cum[:, SPAN - 1 :] - cum))
        decay = columns(jnp.broadcast_to(jnp.exp(cum[:, SPAN - 1 :]), cum.shape))
        for chunk in range(cols // LANES):
            lo = chunk * LANES
            taps = [taps_ref[j : j + 1, lo : lo + LANES] for j in range(4)]
            xs = conv(padded, taps, taps_ref[4:5, lo : lo + LANES], k, lo)
            xs_ref[part, lo : lo + LANES] = xs
            weighted = (xs.astype(F32) * by_head(scale, chunk, left)).astype(BF16)
            if k > 0:
                held_ref[k - 1, lo : lo + LANES] = states[chunk].astype(BF16)
            states[chunk] = by_head(decay, chunk, top) * states[chunk] + tn(weighted, b)
    count = sent_ref.shape[0]
    rows = cols // count
    total = columns(jnp.broadcast_to(sum_ref[:, tokens - 1 :], (sum_ref.shape[0], SPAN)))[:1]
    for d in range(count):
        chunk, lo = divmod(d * rows, LANES)
        sent_ref[d, :rows] = states[chunk][lo : lo + rows].astype(BF16)
        sent_ref[d, rows:] = in_terms(total[:, d : d + 1])


def in_terms(value):
    high = value.astype(BF16).astype(F32)
    middle = (value - high).astype(BF16).astype(F32)
    low = value - high - middle
    at = lax.broadcasted_iota(jnp.int32, (8, LANES), 0)
    terms = jnp.where(at == 0, high, jnp.where(at == 1, middle, jnp.where(at == 2, low, 0.0)))
    return terms.astype(BF16)


def from_terms(terms):
    terms = terms.astype(F32)
    return terms[0:1] + terms[1:2] + terms[2:3]


def scan_near(inbox_ref, inner_ref, before_ref, group_ref, sent_ref):
    count, rows, _ = inner_ref.shape
    state = jnp.zeros((rows, STATE), F32)
    log = jnp.zeros((1, LANES), F32)
    for i in range(count):
        inner_ref[i] = state
        before_ref[8 * i : 8 * i + 8] = jnp.broadcast_to(log, (8, LANES))
        mine = from_terms(inbox_ref[i, rows:])
        state = jnp.exp(mine) * state + inbox_ref[i, :rows].astype(F32)
        log = log + mine
    before_ref[8 * count :] = jnp.broadcast_to(log, (8, LANES))
    group_ref[...] = state
    sent_ref[...] = state.astype(BF16)


def extend(inbox_ref, before_ref, group_ref, sent_ref):
    grown = jnp.exp(before_ref[before_ref.shape[0] - 1 :])
    sent_ref[...] = (grown * inbox_ref[...].astype(F32) + group_ref[...]).astype(BF16)


def scan_far(inner_ref, before_ref, *refs):
    starts_ref = refs[-1]
    state = refs[0][...].astype(F32)
    for ref in refs[1:-1]:
        state = state + ref[...].astype(F32)
    for i in range(inner_ref.shape[0]):
        grown = jnp.exp(before_ref[8 * i : 8 * i + 1])
        starts_ref[i] = (grown * state + inner_ref[i]).astype(BF16)


def local(
    xs_ref, b_ref, raw_ref, halo_ref, group_taps_ref, dt_ref, cum_ref, held_ref, skip_ref,
    c_ref, y_ref, padded,
):
    tokens, cols = xs_ref.shape
    padded[:8] = halo_ref[:, cols + LANES : cols + 2 * LANES].astype(F32)
    padded[8:] = raw_ref[...].astype(F32)
    rows = lax.broadcasted_iota(jnp.int32, (SPAN, SPAN), 0)
    lanes = lax.broadcasted_iota(jnp.int32, (SPAN, SPAN), 1)
    causal = rows >= lanes
    left = left_half()
    taps = [group_taps_ref[8 + j : 9 + j] for j in range(4)]
    for k in range(tokens // SPAN):
        part = slice(k * SPAN, (k + 1) * SPAN)
        c = conv(padded, taps, group_taps_ref[12:13], k, 0)
        c_ref[part] = c
        scores = nt(c, b_ref[part])
        cum_t = cum_ref[:, part]
        dt_t = dt_ref[:, part]
        cum = columns(cum_t)
        grown = jnp.exp(cum)

        def mix(h):
            spread = cum[:, h : h + 1] - cum_t[h : h + 1]
            decays = jnp.exp(jnp.where(causal, spread, -jnp.inf))
            return (decays * dt_t[h : h + 1] * scores).astype(BF16)

        for chunk in range(cols // LANES):
            lo = chunk * LANES
            xs = xs_ref[part, lo : lo + LANES]
            y0 = jnp.dot(mix(2 * chunk), xs, preferred_element_type=F32)
            y1 = jnp.dot(mix(2 * chunk + 1), xs, preferred_element_type=F32)
            y = jnp.where(left, y0, y1) + by_head(skip_ref[...], chunk, left) * xs.astype(F32)
            if k > 0:
                y = y + nt(c, held_ref[k - 1, lo : lo + LANES]) * by_head(grown, chunk, left)
            y_ref[part, lo : lo + LANES] = y.astype(BF16)


def finish(start_ref, c_ref, sum_ref, y_ref, z_ref, out_ref, *, ys):
    tokens, cols = y_ref.shape
    rows = tokens // 32
    half = out_ref.shape[1] // 2
    left = left_half()
    first = lax.axis_index("c") == 0
    for k in range(tokens // SPAN):
        part = slice(k * SPAN, (k + 1) * SPAN)
        grown = jnp.exp(columns(sum_ref[:, part]))
        for chunk in range(cols // LANES):
            lo = chunk * LANES
            carry = nt(c_ref[part], start_ref[lo : lo + LANES]) * by_head(grown, chunk, left)
            z = z_ref[part, lo : lo + LANES].astype(F32)
            gated = ((y_ref[part, lo : lo + LANES].astype(F32) + carry) * silu(z)).astype(BF16)
            for i in range(SPAN // (2 * rows)):
                even = gated[2 * i * rows : (2 * i + 1) * rows]
                odd = gated[(2 * i + 1) * rows : (2 * i + 2) * rows]
                theirs = jnp.where(first, odd, even)
                ours = jnp.where(first, even, odd)
                x, y = divmod(k * (SPAN // (2 * rows)) + i, ys)
                at = (x // 2 * ys + y) * rows
                for d in range(x % 2, out_ref.shape[0], 2):
                    out_ref[d, at : at + rows, lo : lo + LANES] = theirs
                    out_ref[d, half + at : half + at + rows, lo : lo + LANES] = ours


def join(mine_ref, other_ref, gain_ref, out_ref):
    rows = mine_ref.shape[0]
    mine = mine_ref[...].astype(F32) * gain_ref[...]
    other = other_ref[...].astype(F32) * gain_ref[...]
    even = lax.axis_index("xl") == 0
    out_ref[:rows] = jnp.where(even, mine, other).astype(BF16)
    out_ref[rows:] = jnp.where(even, other, mine).astype(BF16)


def project(gated_ref, weights_far, theirs_ref, ours_ref, weights_ref, wide_ref, sems):
    parts, rows, cols = gated_ref.shape
    half, width = ours_ref.shape
    step = width // sems.shape[0]
    loads = []
    for j in range(sems.shape[0]):
        span = pl.ds(j * step, step)
        loads.append(pltpu.make_async_copy(weights_far.at[span], weights_ref.at[span], sems.at[j]))
        loads[-1].start()
    squares = jnp.zeros((rows, 1), F32)
    for i in range(parts):
        wide_ref[:, i * cols : (i + 1) * cols] = gated_ref[i]
        value = gated_ref[i].astype(F32)
        squares = squares + jnp.sum(value * value, axis=1, keepdims=True)
    scale = 1.0 / jnp.sqrt(squares / weights_ref.shape[1] + 1.0)
    for j, load in enumerate(loads):
        lo = j * step
        load.wait()
        total = (nt(wide_ref[...], weights_ref[lo : lo + step]) * scale).astype(BF16)
        theirs_ref[:, lo : lo + step] = total[:half]
        ours_ref[:, lo : lo + step] = total[half:]


def add(ours_ref, other_ref, out_ref):
    out_ref[...] = (ours_ref[...].astype(F32) + other_ref[...].astype(F32)).astype(BF16)


def tail(packed_ref, out_ref):
    own = (packed_ref.shape[1] - 8) // 6
    last = packed_ref.shape[0] - 1
    for i in range(out_ref.shape[1] // LANES):
        side = slice(i * LANES, (i + 1) * LANES)
        out_ref[:, side] = packed_ref[last, (i + 1) * own - 8 : (i + 1) * own]


def collect(shares_ref, out_ref, *, ys):
    count, _, width = shares_ref.shape
    halves = count // ys
    for k in range(width // LANES):
        for i in range(halves):
            total = shares_ref[i * ys, :, k * LANES : (k + 1) * LANES].astype(F32)
            for j in range(1, ys):
                total = total + shares_ref[i * ys + j, :, k * LANES : (k + 1) * LANES].astype(F32)
            at = (k * halves + i) * LANES
            out_ref[:, at : at + LANES] = total.astype(BF16)


def shift(array, axis, by, wrap=True):
    count = lax.axis_size(axis)
    pairs = [(i, (i + by) % count) for i in range(count) if wrap or 0 <= i + by < count]
    return lax.ppermute(array, axis, pairs)


def sent(array, axes):
    return lax.all_to_all(array, axes, 0, 0, tiled=True)


def per_device(
    x_proj, z_proj, b_proj, c_proj, dt_raw, dt_bias, a_log, d_skip,
    conv_x, conv_bias_x, conv_bc, conv_bias_bc, norm_weight, out_weight,
):
    xh, xl, ys, cs = (lax.axis_size(a) for a in PLANE)
    xs = xh * xl
    zh, zl = (lax.axis_size(a) for a in Z)
    plane = xs * ys * cs
    rows, inner = x_proj.shape
    cols = inner // plane
    tokens = rows * plane
    part = lax.axis_index("xh") * xl + lax.axis_index("xl")
    heads = dt_bias.shape[0] // xs

    def own(values, axis):
        size = values.shape[axis] // xs
        return lax.dynamic_slice_in_dim(values, part * size, size, axis)

    mine = out_weight.T
    other = shift(mine, "xl", 1)
    pair = call(
        join,
        shape((2 * mine.shape[0], mine.shape[1]), BF16),
        (mine, other, norm_weight[None]),
    )
    weights = lax.all_gather(pair, Z, axis=0, tiled=True)
    out = call(
        pack,
        shape((plane, 6 * rows + 8, LANES), BF16),
        (x_proj, z_proj, b_proj, c_proj, dt_raw),
        [pltpu.VMEM(a.shape, BF16) for a in (x_proj, z_proj, b_proj, c_proj, dt_raw)]
        + [
            pltpu.VMEM((plane, 6 * rows + 8, LANES), BF16),
            pltpu.SemaphoreType.DMA((5,)),
            pltpu.SemaphoreType.DMA((plane,)),
        ],
        limit=60,
        far=range(5),
        far_out=True,
    )
    per_head = jnp.stack([own(dt_bias, 0), own(-jnp.exp(a_log), 0)], axis=1)
    per_head = jnp.pad(per_head, ((0, 8 - heads), (0, LANES - 2)))
    skip = jnp.pad(own(d_skip, 0), (0, LANES - heads))[None]
    taps = jnp.pad(jnp.concatenate([own(conv_x, 1), own(conv_bias_x, 0)[None]]), ((0, 3), (0, 0)))
    group_taps = jnp.pad(
        jnp.concatenate([jnp.moveaxis(conv_bc, 0, 1), conv_bias_bc[:, None]], axis=1),
        ((0, 0), (0, 3), (0, 0)),
    ).reshape(16, LANES)
    packed, per_head, skip, taps, group_taps = lax.optimization_barrier(
        (sent(out, PLANE), per_head, skip, taps, group_taps)
    )
    halo = call(tail, shape((8, cols + 2 * LANES), BF16), (packed,), (), 1 << 16, 4)
    halo = shift(halo, Z, 1, wrap=False)
    by_token = shape((8, tokens), F32)
    dt, cum, sums, c_raw, z_raw = call(
        steps,
        (by_token, by_token, by_token, shape((tokens, LANES), BF16), shape((tokens, cols), BF16)),
        (packed, per_head),
    )
    x_conv, b_conv, held, states_out = call(
        scan_in,
        (
            shape((tokens, cols), BF16),
            shape((tokens, LANES), BF16),
            shape((tokens // SPAN - 1, cols, STATE), BF16),
            shape((zl, cols // zl + 8, STATE), BF16),
        ),
        (packed, halo, taps, group_taps, dt, cum, sums),
        [pltpu.VMEM((tokens + 8, cols + LANES), F32)],
        1 << 25,
    )
    c_conv, y = call(
        local,
        (shape((tokens, LANES), BF16), shape((tokens, cols), BF16)),
        (x_conv, b_conv, c_raw, halo, group_taps, dt, cum, held, skip),
        [pltpu.VMEM((tokens + 8, LANES), F32)],
        1 << 27,
    )
    near_in, c_conv, y = lax.optimization_barrier((sent(states_out, "zl"), c_conv, y))
    near = zl, cols // zl, STATE
    inner, before, group, ahead = call(
        scan_near,
        (
            shape(near, F32),
            shape((8 * zl + 8, LANES), F32),
            shape(near[1:], F32),
            shape(near[1:], BF16),
        ),
        (near_in,),
    )
    inboxes = []
    for hop in range(zh - 1):
        if hop:
            ahead = call(extend, shape(near[1:], BF16), (inboxes[-1], before, group))
        inboxes.append(lax.ppermute(ahead, "zh", [(hop, hop + 1)]))
    starts = call(scan_far, shape(near, BF16), (inner, before, *inboxes))
    start = sent(starts, "zl").reshape(cols, STATE)

    def finish_all(*refs):
        finish(*refs, ys=ys)

    def collect_all(*refs):
        collect(*refs, ys=ys)

    copies = call(
        finish_all,
        shape((xs, tokens // xl, cols), BF16),
        (start, c_conv, sums, y, z_raw),
        (),
        1 << 25,
    )
    gated = sent(copies, X)
    count = tokens // (2 * xl)
    product = shape((count, weights.shape[0]), BF16)
    room = [
        pltpu.VMEM(weights.shape, BF16),
        pltpu.VMEM((2 * count, weights.shape[1]), BF16),
        pltpu.SemaphoreType.DMA((4,)),
    ]
    theirs, ours = call(project, (product, product), (gated, weights), room, 1 << 30, 50, (1,))
    both = call(add, product, (ours, shift(theirs, "c", 1)))
    shares = sent(both.reshape(xh * ys, rows, weights.shape[0]), ("xh", "y"))
    return call(collect_all, shape((rows, xh * weights.shape[0]), BF16), (shares,))


def solution(mesh):
    split = Mesh(mesh.devices.reshape(4, 4, 2, 2, 4, 2), ALL)
    return jax.shard_map(
        per_device,
        mesh=split,
        in_specs=(
            P(ALL, None),
            P(ALL, None),
            P(ALL, None),
            P(ALL, None),
            P(ALL, None),
            P(HEAD),
            P(HEAD),
            P(HEAD),
            P(None, HEAD),
            P(HEAD),
            P(None, None, HEAD),
            P(None, HEAD),
            P(HEAD),
            P(HEAD, SEQ),
        ),
        out_specs=P(ALL, None),
        check_vma=False,
    )
```
